512 devices in a mesh: req: 16 (over x, z_lo), patch: 32 (over y, z_hi, core).
Axes of the slice: x: 4, y: 8, z: 8 (z_hi: 2, z_lo: 4; z = z_hi * 4 + z_lo), core: 2. Of those that a mesh axis runs over, the one named last changes fastest.
Arguments:
- field: float32 [1024, 16, 640], P(('req', 'patch')), parts along dimension 0
- stale_conv_in: bfloat16 [1024, 16, 640], P(('req', 'patch')), parts along dimension 0, may hold values from -6 to 6
- stale_keys: bfloat16 [16384, 320], P(('req', 'patch')), parts along dimension 0, may hold values from -6 to 6
- stale_values: bfloat16 [16384, 320], P(('req', 'patch')), parts along dimension 0, may hold values from -6 to 6
- norm1_gain: float32 [640], replicated, may hold values from 0.25 to 1.75
- norm1_bias: float32 [640], replicated, may hold values from -3 to 3
- conv_weight: bfloat16 [3, 3, 640, 640], P(None, None, None, 'patch'), may hold values from -0.078125 to 0.078125
- conv_bias: float32 [640], replicated, may hold values from -3 to 3
- time_embed: float32 [32, 640], P('req'), parts along dimension 0, may hold values from -5 to 5
- norm2_gain: float32 [640], replicated, may hold values from 0.25 to 1.75
- norm2_bias: float32 [640], replicated, may hold values from -3 to 3
- w_query: bfloat16 [640, 320], replicated
- w_keyvalue: bfloat16 [640, 640], replicated, may hold values from -0.25 to 0.25
- w_out: bfloat16 [320, 640], replicated, may hold values from -0.3125 to 0.3125
Outputs:
- outputs: float32 [2, 1024, 16, 640], P(None, ('req', 'patch')), parts along dimension 1
The draws below stay inside these ranges and needn't reach their ends.
There are 16 independent parts, one for each index of `req`. The reference program is written for one: setup_inputs(seed, part) draws one part's arguments, and reference() takes and returns one part's arrays. A program takes and returns all parts, laid end to end along the dimension named above; an argument that names none is the same for every part. Nothing has to cross between parts.
All inputs are finite; a program needn't handle non-finite values.
Results may differ from the reference program's by a relative error of at most 0.0047.
Values may be sent and summed in bfloat16 or wider, within the bound.
No kernel may reach another device: no remote copies, remote signals or barrier semaphores. Data moves between devices by JAX's collectives and lax.ppermute only.
A program may use at most 64 MiB of HBM per device.

```python
import jax
import jax.numpy as jnp
from jax import lax

CHANNELS = 640
GROUPS = 32
HEADS = 5
HEAD_DIM = 64
COLS = 16
KEY_WIDTH = 320
HEIGHT = 64
TOKENS = 1024
N_PATCH = 32


def draw_field(key, part):
    base = jax.random.normal(jax.random.fold_in(key, 11), (HEIGHT, COLS, CHANNELS), jnp.float32)
    rising = 1.0 + 2.0 * jnp.arange(HEIGHT, dtype=jnp.float32) / HEIGHT
    result = base * rising[:, None, None]
    return result.astype(jnp.float32)


def draw_w_query(key, part):
    base = jax.random.normal(jax.random.fold_in(key, 21), (CHANNELS, KEY_WIDTH), jnp.float32)
    return (base * CHANNELS ** (-0.5)).astype(jnp.bfloat16)


def block_levels(key, dims, shards, low, high):
    loudness = 1.0
    for position, shards_of in shards:
        draws = jax.random.uniform(jax.random.fold_in(jax.random.fold_in(key, 6), position), (shards_of,), jnp.float32, low / len(shards), high / len(shards))
        loudness = loudness * jnp.repeat(jnp.exp(draws), dims[position] // shards_of).reshape((-1,) + (1,) * (len(dims) - 1 - position))
    return loudness


def noise(rng, dims, spread, bound, shards=(), kind=jnp.bfloat16):
    loudness = block_levels(rng, dims, shards, -0.22, 0.18) if shards else 1.0
    drawn = jax.random.normal(rng, dims, jnp.float32) * spread * loudness
    return jnp.minimum(jnp.maximum(drawn, -bound), bound).astype(kind)


def setup_inputs(seed: int = 0, part: int = 0) -> dict:
    splits = jax.random.split(jax.random.key(seed), 15)
    part_splits = jax.random.split(jax.random.fold_in(splits[14], part), 15)
    return {
        "field": draw_field(jax.random.fold_in(jax.random.fold_in(splits[14], part), 71), part),
        "stale_conv_in": noise(part_splits[1], (HEIGHT, COLS, CHANNELS), 1.0, 6.0, ((0, 32),)),
        "stale_keys": noise(part_splits[2], (TOKENS, KEY_WIDTH), 1.0, 6.0, ((0, 32),)),
        "stale_values": noise(part_splits[3], (TOKENS, KEY_WIDTH), 1.0, 6.0, ((0, 32),)),
        "norm1_gain": jnp.clip(1.0 + 0.15 * jax.random.normal(splits[4], (CHANNELS,), jnp.float32), 0.25, 1.75),
        "norm1_bias": noise(splits[5], (CHANNELS,), 0.5, 3.0, (), jnp.float32),
        "conv_weight": noise(splits[6], (3, 3, CHANNELS, CHANNELS), (9 * CHANNELS) ** -0.5, 0.078125, ((3, 32),)),
        "conv_bias": noise(splits[7], (CHANNELS,), 0.5, 3.0, (), jnp.float32),
        "time_embed": noise(part_splits[8], (2, CHANNELS), 1.0, 5.0, (), jnp.float32),
        "norm2_gain": jnp.clip(1.0 + 0.15 * jax.random.normal(splits[9], (CHANNELS,), jnp.float32), 0.25, 1.75),
        "norm2_bias": noise(splits[10], (CHANNELS,), 0.5, 3.0, (), jnp.float32),
        "w_query": draw_w_query(jax.random.fold_in(splits[14], 71), part),
        "w_keyvalue": noise(splits[12], (CHANNELS, 2 * KEY_WIDTH), CHANNELS ** -0.5, 0.25),
        "w_out": noise(splits[13], (KEY_WIDTH, CHANNELS), KEY_WIDTH ** -0.5, 0.3125),
    }


epsilon = 1e-05

def group_norm(values_in, gain, bias):
    members = CHANNELS // GROUPS
    grouped = values_in.reshape(-1, GROUPS, members)
    number = grouped.shape[0] * members
    totals = lax.optimization_barrier(jnp.sum(grouped, axis=(0, 2)))
    squares = lax.optimization_barrier(jnp.sum(grouped * grouped, axis=(0, 2)))
    average = totals / number
    variance = squares / number - average * average
    scaled = (grouped - average[None, :, None]) * lax.rsqrt(variance + epsilon)[None, :, None]
    return scaled.reshape(values_in.shape) * gain + bias

def build_blocks(current_all, previous_all, parts):
    blocks = current_all.reshape(parts, -1, current_all.shape[1], current_all.shape[2])
    prior_blocks = previous_all.reshape(blocks.shape)
    zero_row = jnp.zeros_like(blocks[:1, :1])
    above = jnp.concatenate([zero_row, prior_blocks[:-1, -1:]], axis=0)
    below = jnp.concatenate([prior_blocks[1:, :1], zero_row], axis=0)
    stacked = jnp.concatenate([above, blocks, below], axis=1)
    return jnp.pad(stacked, ((0, 0), (0, 0), (1, 1), (0, 0)))

def conv_rows(padded, kernel):
    inner = padded.shape[1] - 2
    across = padded.shape[2] - 2
    result = None
    for offset_row in range(3):
        for offset_col in range(3):
            window = padded[:, offset_row:offset_row + inner, offset_col:offset_col + across, :]
            window = window.reshape(-1, padded.shape[3])
            term = jnp.dot(window, kernel[offset_row, offset_col], preferred_element_type=jnp.float32)
            result = term if result is None else result + term
    return result

def attention(query_block, key_set, value_set):
    count_rows = query_block.shape[0]
    query_heads = query_block.astype(jnp.float32).reshape(count_rows, HEADS, HEAD_DIM)
    key_heads = key_set.astype(jnp.float32).reshape(-1, HEADS, HEAD_DIM)
    value_heads = value_set.astype(jnp.float32).reshape(-1, HEADS, HEAD_DIM)
    scores = jnp.einsum('qhd,khd->hqk', query_heads, key_heads) * HEAD_DIM ** (-0.5)
    peak = lax.optimization_barrier(jnp.max(scores, axis=-1, keepdims=True))
    expo = jnp.exp(scores - peak)
    totals = lax.optimization_barrier(jnp.sum(expo, axis=-1, keepdims=True))
    weights = expo.astype(jnp.bfloat16).astype(jnp.float32)
    summed = jnp.einsum('hqk,khd->hqd', weights, value_heads) / totals
    return summed.transpose(1, 0, 2).reshape(count_rows, KEY_WIDTH).astype(jnp.bfloat16)

def attend_all(query, keys, values, prior_keys, prior_values):
    per_patch = TOKENS // N_PATCH
    owner = jnp.arange(TOKENS, dtype=jnp.int32) // per_patch

    def one_patch(index):
        chosen = (owner == index)[:, None]
        mixed_keys = jnp.where(chosen, keys, prior_keys)
        mixed_values = jnp.where(chosen, values, prior_values)
        block = lax.dynamic_slice_in_dim(query, (index * per_patch).astype(jnp.int32), per_patch, 0)
        return attention(block, mixed_keys, mixed_values)
    result = lax.map(one_patch, jnp.arange(N_PATCH, dtype=jnp.int32))
    return result.reshape(TOKENS, KEY_WIDTH)

def reference(field, stale_conv_in, stale_keys, stale_values, norm1_gain, norm1_bias, conv_weight, conv_bias, time_embed, norm2_gain, norm2_bias, w_query, w_keyvalue, w_out):
    state = field
    prior_conv = stale_conv_in
    prior_keys = stale_keys
    prior_values = stale_values
    results = []
    for which_step in range(2):
        activated = jax.nn.silu(group_norm(state, norm1_gain, norm1_bias)).astype(jnp.bfloat16)
        padded = build_blocks(activated, prior_conv, N_PATCH)
        conv_out = conv_rows(padded, conv_weight).reshape(state.shape)
        hidden = state + (conv_out + conv_bias + time_embed[which_step])
        normed = group_norm(hidden, norm2_gain, norm2_bias).astype(jnp.bfloat16).reshape(TOKENS, CHANNELS)
        query = jnp.dot(normed, w_query, preferred_element_type=jnp.float32).astype(jnp.bfloat16)
        keyvalue = jnp.dot(normed, w_keyvalue, preferred_element_type=jnp.float32).astype(jnp.bfloat16)
        keys = keyvalue[:, :KEY_WIDTH]
        values = keyvalue[:, KEY_WIDTH:]
        attended = attend_all(query, keys, values, prior_keys, prior_values)
        mixed = jnp.dot(attended, w_out, preferred_element_type=jnp.float32)
        result = hidden + mixed.reshape(hidden.shape)
        results.append(result)
        state = result
        prior_conv = activated
        prior_keys = keys
        prior_values = values
    return jnp.stack(results)
```

```python
import functools

import jax
import jax.numpy as jnp
from jax import lax
from jax.experimental import pallas as pl
from jax.experimental.pallas import tpu as pltpu
from jax.sharding import Mesh
from jax.sharding import PartitionSpec as P

GROUPS = 32
HEADS = 5
HEAD_DIM = 64
WIDTH = HEADS * HEAD_DIM
CHANNELS = 640
MEMBERS = CHANNELS // GROUPS
COLS = 16
ROWS = 32
LANES = 128
POSITIONS = 1024
EPS = 1e-05

PATCH = ("y", "zh", "core")
QUAD = ("zh", "core")
REQ_PATCH = ("req", "y", "zh", "core")

F32 = jnp.float32
BF16 = jnp.bfloat16

NN = (((1,), (0,)), ((), ()))
NT = (((1,), (1,)), ((), ()))


def dot(a, b, dims=NN):
    return lax.dot_general(a, b, dims, preferred_element_type=F32)


def thirds(x):
    high = x.astype(BF16)
    rest = x - high.astype(F32)
    middle = rest.astype(BF16)
    low = (rest - middle.astype(F32)).astype(BF16)
    return high, middle, low


def picked(x, zero_one, dims=NN):
    rows = x.shape[0]
    stacked = jnp.concatenate([t.astype(F32) for t in thirds(x)], axis=0).astype(BF16)
    out = dot(stacked, zero_one, dims)
    return out[:rows] + out[rows : 2 * rows] + out[2 * rows :]


def group_matrix():
    channel = lax.broadcasted_iota(jnp.int32, (CHANNELS, LANES), 0)
    first = lax.broadcasted_iota(jnp.int32, (CHANNELS, LANES), 1) * MEMBERS
    return jnp.where((channel >= first) & (channel < first + MEMBERS), 1.0, 0.0).astype(BF16)


def eight(rows, lanes):
    have = sum(r.shape[0] for r in rows)
    return jnp.concatenate([*rows, jnp.zeros((8 - have, lanes), F32)], axis=0)


def local_sums(x, groups):
    sums = eight(
        [jnp.sum(x, axis=0, keepdims=True), jnp.sum(x * x, axis=0, keepdims=True)], CHANNELS
    )
    return picked(sums, groups)


def tell_state(x, groups, stats_ref, diff_ref):
    sums = local_sums(x, groups)
    own_mean = (sums[0:1] * (1.0 / (ROWS * MEMBERS))).astype(BF16)
    spread = dot(eight([own_mean.astype(F32)], LANES).astype(BF16), groups, NT)
    diff_ref[...] = (x - spread[0:1]).astype(BF16)
    told = jnp.concatenate(
        [sums[0:2], own_mean.astype(F32), jnp.zeros((1, LANES), F32)], axis=0
    )
    stats_ref[...] = jnp.broadcast_to(told[None], stats_ref.shape)


def mean_and_scale(total, squares):
    number = POSITIONS * MEMBERS
    mean = total * (1.0 / number)
    variance = squares * (1.0 / number) - mean * mean
    return mean, lax.rsqrt(variance + EPS)


def first_kernel(field_ref, keys_ref, values_ref, stats_ref, diff_ref, kv_ref, select_ref):
    tell_state(field_ref[...], group_matrix(), stats_ref, diff_ref)
    both = jnp.concatenate(
        [keys_ref[...].astype(F32), values_ref[...].astype(F32)], axis=1
    ).astype(BF16)
    kv_ref[...] = jnp.broadcast_to(both[None], kv_ref.shape)
    channel = lax.broadcasted_iota(jnp.int32, (CHANNELS, 256), 0)
    lane = lax.broadcasted_iota(jnp.int32, (CHANNELS, 256), 1)
    within = lane & 31
    for turn in range(4):
        meant = (lane >> 5) * (4 * MEMBERS) + turn * MEMBERS + within
        chosen = (channel == meant) & (within < MEMBERS)
        select_ref[turn] = jnp.where(chosen, 1.0, 0.0).astype(BF16)


def rows_kernel(place_ref, own_ref, one_ref, two_ref, three_ref, four_ref, first_ref, last_ref):
    a = place_ref[1]
    for k, ref in enumerate((own_ref, one_ref, two_ref, three_ref)):
        four_ref[a ^ k] = ref[...]
    first_ref[...] = four_ref[0, :COLS]
    last_ref[...] = four_ref[3, COLS:]


def conv_kernel(
    place_ref,
    stats_ref,
    d0_ref,
    d1_ref,
    d2_ref,
    d3_ref,
    prior_ref,
    above_ref,
    below_ref,
    weight_ref,
    gain_ref,
    bias_ref,
    shift_ref,
    select_ref,
    told_ref,
    o0_ref,
    o1_ref,
    o2_ref,
    o3_ref,
    act_ref,
    first_ref,
    last_ref,
    diff,
    rows,
    wide,
    outs,
):
    y = place_ref[0]
    a = place_ref[1]
    groups = group_matrix()
    for k, ref in enumerate((d0_ref, d1_ref, d2_ref, d3_ref)):
        diff[a ^ k] = ref[...]

    sums = jnp.sum(stats_ref[...], axis=0)
    mean, scale = mean_and_scale(sums[0:1], sums[1:2])
    own_means = [stats_ref[4 * y + t][2:3] for t in range(4)]
    spread = picked(eight([(m - mean) * scale for m in own_means] + [scale], LANES), groups, NT)
    gain = gain_ref[...]
    bias = bias_ref[...]
    factor = spread[4:5] * gain
    for t in range(4):
        offset = spread[t : t + 1] * gain + bias
        value = diff[t].astype(F32) * factor + offset
        act_ref[t] = (value * (1.0 / (1.0 + jnp.exp(-value)))).astype(BF16)
    first_ref[...] = act_ref[0, :COLS]
    last_ref[...] = act_ref[3, COLS:]
    for t in range(4):
        rows[t, 0:COLS] = above_ref[...] if t == 0 else prior_ref[t - 1, COLS:]
        rows[t, COLS : 3 * COLS] = act_ref[t]
        rows[t, 3 * COLS :] = below_ref[...] if t == 3 else prior_ref[t + 1, :COLS]
    window = rows[...].reshape(4 * 64, CHANNELS)

    wide[...] = jnp.zeros(wide.shape, F32)
    col = lax.broadcasted_iota(jnp.int32, (LANES, LANES), 0) & (COLS - 1)
    lane = lax.broadcasted_iota(jnp.int32, (LANES, LANES), 1)
    within = lane & 31
    halves = [jnp.zeros((LANES, LANES), F32), jnp.zeros((LANES, LANES), F32)]
    for part in range(8):
        wide[:, 0 : 9 * MEMBERS] = dot(window, weight_ref[part], NT)
        whole = wide[...].reshape(4, 64, 256)
        lines = [
            whole[:, COLS * r : COLS * r + 2 * COLS].reshape(LANES, 256) for r in range(3)
        ]
        total = (
            lines[0][:, :LANES]
            + pltpu.roll(lines[1][:, :LANES], LANES - 3 * MEMBERS, 1)
            + pltpu.roll(lines[2], 256 - 6 * MEMBERS, 1)[:, :LANES]
        )
        left = jnp.where(col > 0, pltpu.roll(total, 1, 0), 0.0)
        centre = pltpu.roll(total, LANES - MEMBERS, 1)
        right = pltpu.roll(total, LANES - 2 * MEMBERS, 1)
        right = jnp.where(col < COLS - 1, pltpu.roll(right, LANES - 1, 0), 0.0)
        made = left + centre + right
        at = 32 * (part % 4)
        if at:
            made = pltpu.roll(made, at, 1)
        kept = (lane >= at) & (lane < at + MEMBERS)
        halves[part // 4] = jnp.where(kept, made, halves[part // 4])
    made = jnp.concatenate(halves, axis=1)
    outs[...] = made.reshape(4, ROWS, 256)
    for k, ref in enumerate((o0_ref, o1_ref, o2_ref, o3_ref)):
        ref[...] = outs[a ^ k]

    select = select_ref[a]
    group = lax.broadcasted_iota(jnp.int32, (LANES, 256), 0)
    wide_lane = lax.broadcasted_iota(jnp.int32, (LANES, 256), 1)
    holds = (group == (wide_lane >> 5) * 4 + a) & ((wide_lane & 31) < MEMBERS)
    holds = jnp.where(holds, 1.0, 0.0).astype(BF16)
    state = dot(diff[...].reshape(LANES, CHANNELS), select).reshape(4, ROWS, 256)
    means = dot(eight(own_means, LANES).astype(BF16), holds)
    added = picked(eight([shift_ref[...]], CHANNELS), select)[0:1]
    total = jnp.zeros((1, 256), F32)
    squares = jnp.zeros((1, 256), F32)
    for t in range(4):
        hidden = state[t] + means[t : t + 1] + added + outs[t]
        total += jnp.sum(hidden, axis=0, keepdims=True)
        squares += jnp.sum(hidden * hidden, axis=0, keepdims=True)
    sums = picked(eight([total, squares], 256), holds, NT)
    told_ref[...] = jnp.broadcast_to(sums[None, 0:4], told_ref.shape)


def attend_kernel(
    last_step,
    n_kv,
    place_ref,
    own_ref,
    stats_ref,
    state_ref,
    c0_ref,
    c1_ref,
    c2_ref,
    c3_ref,
    select_ref,
    gain_ref,
    bias_ref,
    shift_ref,
    query_ref,
    keyvalue_ref,
    out_ref,
    *refs,
):
    kv_refs, result_ref, more = refs[:n_kv], refs[n_kv], refs[n_kv + 1 :]
    a = place_ref[1]
    own_start = own_ref[0]
    groups = group_matrix()
    conv = jnp.zeros((ROWS, CHANNELS), F32)
    for k, ref in enumerate((c0_ref, c1_ref, c2_ref, c3_ref)):
        conv += picked(ref[...], select_ref[a ^ k], NT)
    hidden = state_ref[...] + (conv + shift_ref[...])
    sums = jnp.sum(stats_ref[...], axis=0)
    mean, scale = mean_and_scale(sums[0:1], sums[1:2])
    spread = picked(eight([mean, scale], LANES), groups, NT)
    normed = (hidden - spread[0:1]) * spread[1:2] * gain_ref[...] + bias_ref[...]
    normed = normed.astype(BF16)
    query = dot(normed, query_ref[...])
    fresh = dot(normed, keyvalue_ref[...]).astype(BF16)

    lane = lax.broadcasted_iota(jnp.int32, (ROWS, CHANNELS), 1)
    padded = jnp.concatenate([query, jnp.zeros((ROWS, CHANNELS - WIDTH), F32)], axis=1)
    heads = jnp.concatenate(
        [
            jnp.where((lane >= h * HEAD_DIM) & (lane < (h + 1) * HEAD_DIM), padded, 0.0)
            for h in range(HEADS)
        ],
        axis=0,
    ).astype(BF16)
    blocks = [ref[...].reshape(-1, CHANNELS) for ref in kv_refs] + [fresh]
    scores = [dot(heads, b, NT) * HEAD_DIM ** (-0.5) for b in blocks]
    column = lax.broadcasted_iota(jnp.int32, scores[0].shape, 1)
    outside = (column < own_start) | (column >= own_start + ROWS)
    scores[0] = jnp.where(outside, scores[0], -jnp.inf)
    peak = functools.reduce(
        jnp.maximum, [jnp.max(s, axis=1, keepdims=True) for s in scores]
    )
    expo = [jnp.exp(s - peak) for s in scores]
    total = sum(jnp.sum(e, axis=1, keepdims=True) for e in expo)
    summed = sum(dot(e.astype(BF16), b) for e, b in zip(expo, blocks)) / total
    attended = jnp.zeros((ROWS, CHANNELS), F32)
    for h in range(HEADS):
        start = WIDTH + h * HEAD_DIM
        kept = (lane >= start) & (lane < start + HEAD_DIM)
        attended = jnp.where(kept, summed[h * ROWS : (h + 1) * ROWS], attended)
    attended = attended[:, WIDTH:].astype(BF16)
    result = hidden + dot(attended, out_ref[...])
    if last_step:
        result_ref[0] = state_ref[...]
        result_ref[1] = result
    else:
        stats_out, diff_out, kv_out = more
        result_ref[...] = result
        kv_out[...] = fresh
        tell_state(result, groups, stats_out, diff_out)


VMEM = pl.BlockSpec(memory_space=pltpu.VMEM)
SMEM = pl.BlockSpec(memory_space=pltpu.SMEM)


def call(kernel, name, out_shapes, args, scalars=0, scratch=(), flops=0):
    return pl.pallas_call(
        kernel,
        name=name,
        out_shape=[jax.ShapeDtypeStruct(s, t) for s, t in out_shapes],
        in_specs=[SMEM] * scalars + [VMEM] * (len(args) - scalars),
        out_specs=[VMEM] * len(out_shapes),
        scratch_shapes=list(scratch),
        cost_estimate=pl.CostEstimate(flops=flops, bytes_accessed=1 << 20, transcendentals=0),
        compiler_params=pltpu.CompilerParams(vmem_limit_bytes=48 << 20),
    )(*args)


def flipped(value, k):
    return lax.ppermute(value, QUAD, [(i, i ^ k) for i in range(4)])


def to_all(value, axes):
    return lax.all_to_all(value, axes, 0, 0, tiled=True)


def per_device(
    field,
    stale_conv_in,
    stale_keys,
    stale_values,
    norm1_gain,
    norm1_bias,
    conv_weight,
    conv_bias,
    time_embed,
    norm2_gain,
    norm2_bias,
    w_query,
    w_keyvalue,
    w_out,
):
    y = lax.axis_index("y")
    zh = lax.axis_index("zh")
    a = 2 * zh + lax.axis_index("core")
    place = jnp.stack([y, a]).astype(jnp.int32)
    owns = (((2 * y + zh) * ROWS).reshape(1).astype(jnp.int32), (y * 4 * ROWS).reshape(1).astype(jnp.int32))
    up = [(i, i + 1) for i in range(7)]
    down = [(i + 1, i) for i in range(7)]

    slices = conv_weight.transpose(0, 1, 3, 2).reshape(9 * MEMBERS, CHANNELS)
    weights = lax.all_gather(slices, "y", axis=0, tiled=False)

    state = field.reshape(ROWS, CHANNELS)
    stats, diff, kv, select = call(
        first_kernel,
        "first",
        [
            ((32, 4, LANES), F32),
            ((ROWS, CHANNELS), BF16),
            ((16, ROWS, CHANNELS), BF16),
            ((4, CHANNELS, 256), BF16),
        ],
        (state, stale_keys, stale_values),
    )
    stats = to_all(stats, PATCH)
    diffs = (diff, *(flipped(diff, k) for k in (1, 2, 3)))
    kv_same = to_all(kv, ("y", "zh"))
    kvs = (kv_same, flipped(kv_same, 1))

    stale = stale_conv_in.reshape(ROWS, CHANNELS)
    prior, first, last = call(
        rows_kernel,
        "rows",
        [((4, ROWS, CHANNELS), BF16), ((COLS, CHANNELS), BF16), ((COLS, CHANNELS), BF16)],
        (place, stale, *(flipped(stale, k) for k in (1, 2, 3))),
        scalars=1,
    )
    row = lambda v: v.reshape(1, CHANNELS)
    for step in range(2):
        above = lax.ppermute(last, "y", up)
        below = lax.ppermute(first, "y", down)
        shift = row(conv_bias + time_embed[step])
        told, o0, o1, o2, o3, prior, first, last = call(
            conv_kernel,
            f"conv{step}",
            [((32, 4, LANES), F32)]
            + [((ROWS, 256), F32)] * 4
            + [((4, ROWS, CHANNELS), BF16), ((COLS, CHANNELS), BF16), ((COLS, CHANNELS), BF16)],
            (
                place,
                stats,
                *diffs,
                prior,
                above,
                below,
                weights,
                row(norm1_gain),
                row(norm1_bias),
                shift,
                select,
            ),
            scalars=1,
            scratch=[
                pltpu.VMEM((4, ROWS, CHANNELS), BF16),
                pltpu.VMEM((4, 64, CHANNELS), BF16),
                pltpu.VMEM((256, 256), F32),
                pltpu.VMEM((4, ROWS, 256), F32),
            ],
            flops=1 << 30,
        )
        told = to_all(told, PATCH)
        parts = (o0, flipped(o1, 1), flipped(o2, 2), flipped(o3, 3))
        final = step == 1
        shapes = (
            [((2, ROWS, CHANNELS), F32)]
            if final
            else [
                ((ROWS, CHANNELS), F32),
                ((32, 4, LANES), F32),
                ((ROWS, CHANNELS), BF16),
                ((ROWS, CHANNELS), BF16),
            ]
        )
        made = call(
            functools.partial(attend_kernel, final, len(kvs)),
            f"attend{step}",
            shapes,
            (
                place,
                owns[step],
                told,
                state,
                *parts,
                select,
                row(norm2_gain),
                row(norm2_bias),
                shift,
                w_query,
                w_keyvalue,
                w_out,
                *kvs,
            ),
            scalars=2,
            flops=1 << 30,
        )
        if final:
            return made[0].reshape(2, 2, COLS, CHANNELS)
        state, stats, diff, kv = made
        stats = to_all(stats, PATCH)
        diffs = (diff, *(flipped(diff, k) for k in (1, 2, 3)))
        four = jnp.concatenate([kv, *(flipped(kv, k) for k in (1, 2, 3))], axis=0)
        kvs = (lax.all_gather(four, "y", axis=0, tiled=False),)


def solution(mesh):
    torus = Mesh(
        mesh.devices.reshape(mesh.shape["req"], 8, 2, 2), ("req", "y", "zh", "core")
    )
    placed = (
        P(REQ_PATCH, None, None),
        P(REQ_PATCH, None, None),
        P(REQ_PATCH, None),
        P(REQ_PATCH, None),
        P(),
        P(),
        P(None, None, None, PATCH),
        P(),
        P("req", None),
        P(),
        P(),
        P(),
        P(),
        P(),
    )
    return jax.shard_map(
        per_device,
        mesh=torus,
        in_specs=placed,
        out_specs=P(None, REQ_PATCH, None, None),
        check_vma=False,
    )
```

```python
import functools

import jax
import jax.numpy as jnp
from jax import lax
from jax.experimental import pallas as pl
from jax.experimental.pallas import tpu as pltpu
from jax.sharding import Mesh
from jax.sharding import PartitionSpec as P

GROUPS = 32
HEADS = 5
HEAD_DIM = 64
WIDTH = HEADS * HEAD_DIM
CHANNELS = 640
MEMBERS = CHANNELS // GROUPS
COLS = 16
ROWS = 32
LANES = 128
QUAD_ROWS = 4 * ROWS
POSITIONS = 1024
EPS = 1e-05

PATCH = ("y", "zh", "core")
QUAD = ("zh", "core")
REQ_PATCH = ("req", "y", "zh", "core")

F32 = jnp.float32
BF16 = jnp.bfloat16

NN = (((1,), (0,)), ((), ()))
NT = (((1,), (1,)), ((), ()))


def dot(a, b, dims=NN):
    return lax.dot_general(a, b, dims, preferred_element_type=F32)


def thirds(x):
    high = x.astype(BF16)
    rest = x - high.astype(F32)
    middle = rest.astype(BF16)
    low = (rest - middle.astype(F32)).astype(BF16)
    return high, middle, low


def picked(x, zero_one, dims=NN):
    rows = x.shape[0]
    stacked = jnp.concatenate([t.astype(F32) for t in thirds(x)], axis=0).astype(BF16)
    out = dot(stacked, zero_one, dims)
    return out[:rows] + out[rows : 2 * rows] + out[2 * rows :]


def group_matrix():
    channel = lax.broadcasted_iota(jnp.int32, (CHANNELS, LANES), 0)
    first = lax.broadcasted_iota(jnp.int32, (CHANNELS, LANES), 1) * MEMBERS
    return jnp.where((channel >= first) & (channel < first + MEMBERS), 1.0, 0.0).astype(BF16)


def eight(rows, lanes):
    have = sum(r.shape[0] for r in rows)
    return jnp.concatenate([*rows, jnp.zeros((8 - have, lanes), F32)], axis=0)


def tell_sums(x, groups, stats_ref):
    sums = eight(
        [jnp.sum(x, axis=0, keepdims=True), jnp.sum(x * x, axis=0, keepdims=True)], CHANNELS
    )
    told = picked(sums, groups)[0:4]
    stats_ref[...] = jnp.broadcast_to(told[None], stats_ref.shape)


def mean_and_scale(stats_ref, groups):
    sums = jnp.sum(stats_ref[...], axis=0)
    number = POSITIONS * MEMBERS
    mean = sums[0:1] * (1.0 / number)
    variance = sums[1:2] * (1.0 / number) - mean * mean
    spread = picked(eight([mean, lax.rsqrt(variance + EPS)], LANES), groups, NT)
    return spread[0:1], spread[1:2]


def pack_kernel(field_ref, stale_ref, keys_ref, values_ref, packed_ref):
    high, middle, _ = thirds(field_ref[...])
    both = jnp.concatenate(
        [keys_ref[...].astype(F32), values_ref[...].astype(F32)], axis=1
    ).astype(BF16)
    for to in range(4):
        packed_ref[to, 0:ROWS] = high
        packed_ref[to, ROWS : 2 * ROWS] = middle
        packed_ref[to, 2 * ROWS : 3 * ROWS] = stale_ref[...]
        packed_ref[to, 3 * ROWS :] = both


def unpack_kernel(
    place_ref,
    packed_ref,
    field_ref,
    state_ref,
    stats_ref,
    kv_ref,
    prior_ref,
    first_ref,
    last_ref,
):
    a = place_ref[1]
    for t in range(4):
        state_ref[t] = packed_ref[t, 0:ROWS].astype(F32) + packed_ref[t, ROWS : 2 * ROWS].astype(F32)
        prior_ref[t] = packed_ref[t, 2 * ROWS : 3 * ROWS]
        kv_ref[t] = packed_ref[t, 3 * ROWS :]
    state_ref[a] = field_ref[...]
    first_ref[...] = prior_ref[0, :COLS]
    last_ref[...] = prior_ref[3, COLS:]
    tell_sums(state_ref[...].reshape(QUAD_ROWS, CHANNELS), group_matrix(), stats_ref)


def conv_kernel(
    stats_ref,
    state_ref,
    prior_ref,
    above_ref,
    below_ref,
    weight_ref,
    gain_ref,
    bias_ref,
    out_ref,
    act_ref,
    first_ref,
    last_ref,
    rows,
    wide,
):
    mean, scale = mean_and_scale(stats_ref, group_matrix())
    for t in range(4):
        value = (state_ref[t] - mean) * scale * gain_ref[...] + bias_ref[...]
        act_ref[t] = (value * (1.0 / (1.0 + jnp.exp(-value)))).astype(BF16)
    first_ref[...] = act_ref[0, :COLS]
    last_ref[...] = act_ref[3, COLS:]
    for t in range(4):
        rows[t, 0:COLS] = above_ref[...] if t == 0 else prior_ref[t - 1, COLS:]
        rows[t, COLS : 3 * COLS] = act_ref[t]
        rows[t, 3 * COLS :] = below_ref[...] if t == 3 else prior_ref[t + 1, :COLS]
    window = rows[...].reshape(4 * 64, CHANNELS)

    wide[...] = jnp.zeros(wide.shape, F32)
    col = lax.broadcasted_iota(jnp.int32, (LANES, LANES), 0) & (COLS - 1)
    lane = lax.broadcasted_iota(jnp.int32, (LANES, LANES), 1)
    tiles = [jnp.zeros((LANES, LANES), F32), jnp.zeros((LANES, LANES), F32)]
    for part in range(8):
        wide[:, 0 : 9 * MEMBERS] = dot(window, weight_ref[part], NT)
        whole = wide[...].reshape(4, 64, 256)
        lines = [
            whole[:, COLS * r : COLS * r + 2 * COLS].reshape(LANES, 256) for r in range(3)
        ]
        total = (
            lines[0][:, :LANES]
            + pltpu.roll(lines[1][:, :LANES], LANES - 3 * MEMBERS, 1)
            + pltpu.roll(lines[2], 256 - 6 * MEMBERS, 1)[:, :LANES]
        )
        left = jnp.where(col > 0, pltpu.roll(total, 1, 0), 0.0)
        centre = pltpu.roll(total, LANES - MEMBERS, 1)
        right = pltpu.roll(total, LANES - 2 * MEMBERS, 1)
        right = jnp.where(col < COLS - 1, pltpu.roll(right, LANES - 1, 0), 0.0)
        made = left + centre + right
        tile, at = divmod(part, 6)
        at *= MEMBERS
        if at:
            made = pltpu.roll(made, at, 1)
        kept = (lane >= at) & (lane < at + MEMBERS)
        tiles[tile] = jnp.where(kept, made, tiles[tile])
    rest = jnp.where(
        lane[:64] < 64, tiles[1][:64], pltpu.roll(tiles[1][64:], 64, 1)
    )
    for to in range(4):
        out_ref[to, 0:LANES] = tiles[0]
        out_ref[to, LANES:] = rest


def hidden_kernel(conv_ref, state_ref, shift_ref, hidden_ref, stats_ref):
    lane = lax.broadcasted_iota(jnp.int32, (LANES, LANES), 1)
    tiles = [jnp.zeros((LANES, LANES), F32) for _ in range(5)]
    for t in range(4):
        rest = conv_ref[t, LANES:]
        sources = (
            conv_ref[t, 0:LANES],
            jnp.concatenate([rest, pltpu.roll(rest, 64, 1)], axis=0),
        )
        for part in range(8):
            source, at = divmod(part, 6)
            at *= MEMBERS
            tile, to = divmod(4 * MEMBERS * part + MEMBERS * t, LANES)
            turn = (to - at) % LANES
            block = sources[source]
            if turn:
                block = pltpu.roll(block, turn, 1)
            kept = (lane >= to) & (lane < to + MEMBERS)
            tiles[tile] = jnp.where(kept, block, tiles[tile])
            if to + MEMBERS > LANES:
                kept = lane < to + MEMBERS - LANES
                tiles[tile + 1] = jnp.where(kept, block, tiles[tile + 1])
    state = state_ref[...].reshape(QUAD_ROWS, CHANNELS)
    hidden = state + (jnp.concatenate(tiles, axis=1) + shift_ref[...])
    hidden_ref[...] = hidden.reshape(hidden_ref.shape)
    tell_sums(hidden, group_matrix(), stats_ref)


def attend(hidden, patch, y, mean, scale, gain, bias, w_query, w_keyvalue, w_out, kv_ref):
    count = hidden.shape[0]
    normed = ((hidden - mean) * scale * gain + bias).astype(BF16)
    query = dot(normed, w_query)
    fresh = dot(normed, w_keyvalue).astype(BF16)
    query = jnp.concatenate([query, jnp.zeros((count, 3 * LANES - WIDTH), F32)], axis=1)
    lane = lax.broadcasted_iota(jnp.int32, (count, LANES), 1)
    low = lane < HEAD_DIM

    column = lax.broadcasted_iota(jnp.int32, (count, POSITIONS), 1) >> 5
    replaced = column == 4 * y + patch
    if count == ROWS:
        theirs = None
    else:
        theirs = (lax.broadcasted_iota(jnp.int32, (count, count), 1) >> 5) == patch
    tiles = [jnp.zeros((count, LANES), F32) for _ in range(3)]
    for h in range(HEADS):
        at = LANES * (h // 2)
        own = low if h % 2 == 0 else ~low
        asked = jnp.where(own, query[:, at : at + LANES], 0.0).astype(BF16)
        old = dot(asked, kv_ref[:, at : at + LANES], NT) * HEAD_DIM ** (-0.5)
        old = jnp.where(replaced, -jnp.inf, old)
        new = dot(asked, fresh[:, at : at + LANES], NT) * HEAD_DIM ** (-0.5)
        if theirs is not None:
            new = jnp.where(theirs, new, -jnp.inf)
        peak = jnp.maximum(
            jnp.max(old, axis=1, keepdims=True), jnp.max(new, axis=1, keepdims=True)
        )
        old = jnp.exp(old - peak)
        new = jnp.exp(new - peak)
        total = jnp.sum(old, axis=1, keepdims=True) + jnp.sum(new, axis=1, keepdims=True)
        at = LANES * ((HEADS + h) // 2)
        summed = dot(old.astype(BF16), kv_ref[:, at : at + LANES])
        summed += dot(new.astype(BF16), fresh[:, at : at + LANES])
        summed = pltpu.roll(summed / total, HEAD_DIM, 1)
        tiles[h // 2] = jnp.where(own, summed, tiles[h // 2])
    attended = jnp.concatenate(tiles, axis=1)[:, :WIDTH].astype(BF16)
    return hidden + dot(attended, w_out), fresh


def attend_quad_kernel(
    place_ref,
    stats_ref,
    hidden_ref,
    gain_ref,
    bias_ref,
    query_ref,
    keyvalue_ref,
    out_ref,
    kv_ref,
    state_ref,
    result_ref,
    told_ref,
    fresh_ref,
):
    groups = group_matrix()
    mean, scale = mean_and_scale(stats_ref, groups)
    patch = lax.broadcasted_iota(jnp.int32, (QUAD_ROWS, 1), 0) >> 5
    result, fresh = attend(
        hidden_ref[...].reshape(QUAD_ROWS, CHANNELS),
        patch,
        place_ref[0],
        mean,
        scale,
        gain_ref[...],
        bias_ref[...],
        query_ref[...],
        keyvalue_ref[...],
        out_ref[...],
        kv_ref,
    )
    state_ref[...] = result.reshape(state_ref.shape)
    result_ref[...] = state_ref[place_ref[1]]
    fresh_ref[...] = fresh
    tell_sums(result, groups, told_ref)


def attend_own_kernel(
    place_ref,
    stats_ref,
    hidden_ref,
    gain_ref,
    bias_ref,
    query_ref,
    keyvalue_ref,
    out_ref,
    kv_ref,
    earlier_ref,
    result_ref,
):
    mean, scale = mean_and_scale(stats_ref, group_matrix())
    a = place_ref[1]
    result, _ = attend(
        hidden_ref[a],
        a,
        place_ref[0],
        mean,
        scale,
        gain_ref[...],
        bias_ref[...],
        query_ref[...],
        keyvalue_ref[...],
        out_ref[...],
        kv_ref,
    )
    result_ref[0] = earlier_ref[...]
    result_ref[1] = result


VMEM = pl.BlockSpec(memory_space=pltpu.VMEM)
SMEM = pl.BlockSpec(memory_space=pltpu.SMEM)


def call(kernel, name, out_shapes, args, scalars=0, scratch=(), flops=0):
    return pl.pallas_call(
        kernel,
        name=name,
        out_shape=[jax.ShapeDtypeStruct(s, t) for s, t in out_shapes],
        in_specs=[SMEM] * scalars + [VMEM] * (len(args) - scalars),
        out_specs=[VMEM] * len(out_shapes),
        scratch_shapes=list(scratch),
        cost_estimate=pl.CostEstimate(flops=flops, bytes_accessed=1 << 20, transcendentals=0),
        compiler_params=pltpu.CompilerParams(vmem_limit_bytes=48 << 20),
    )(*args)


def to_all(value, axes):
    return lax.all_to_all(value, axes, 0, 0, tiled=True)


def per_device(
    field,
    stale_conv_in,
    stale_keys,
    stale_values,
    norm1_gain,
    norm1_bias,
    conv_weight,
    conv_bias,
    time_embed,
    norm2_gain,
    norm2_bias,
    w_query,
    w_keyvalue,
    w_out,
):
    quad = (4, ROWS, CHANNELS)
    line = (COLS, CHANNELS)
    stats8 = ((8, 4, LANES), F32)
    y = lax.axis_index("y")
    a = 2 * lax.axis_index("zh") + lax.axis_index("core")
    place = jnp.stack([y, a]).astype(jnp.int32)
    up = [(i, i + 1) for i in range(7)]
    down = [(i + 1, i) for i in range(7)]
    row = lambda v: v.reshape(1, CHANNELS)

    slices = conv_weight.transpose(0, 1, 3, 2).reshape(9 * MEMBERS, CHANNELS)
    weights = lax.all_gather(slices, "y", axis=0, tiled=False)

    own = field.reshape(ROWS, CHANNELS)
    (packed,) = call(
        pack_kernel,
        "pack",
        [((4, 4 * ROWS, CHANNELS), BF16)],
        (own, stale_conv_in.reshape(ROWS, CHANNELS), stale_keys, stale_values),
    )
    state, stats, kv, prior, first, last = call(
        unpack_kernel,
        "unpack",
        [(quad, F32), stats8, (quad, BF16), (quad, BF16), (line, BF16), (line, BF16)],
        (place, to_all(packed, QUAD), own),
        scalars=1,
    )
    for step in range(2):
        stats = to_all(stats, "y")
        above = lax.ppermute(last, "y", up)
        below = lax.ppermute(first, "y", down)
        kv = lax.all_gather(kv.reshape(QUAD_ROWS, CHANNELS), "y", axis=0, tiled=True)
        conv, prior, first, last = call(
            conv_kernel,
            f"conv{step}",
            [((4, LANES + 64, LANES), F32), (quad, BF16), (line, BF16), (line, BF16)],
            (stats, state, prior, above, below, weights, row(norm1_gain), row(norm1_bias)),
            scratch=[pltpu.VMEM((4, 64, CHANNELS), BF16), pltpu.VMEM((256, 256), F32)],
            flops=1 << 30,
        )
        hidden, stats = call(
            hidden_kernel,
            f"hidden{step}",
            [(quad, F32), stats8],
            (to_all(conv, QUAD), state, row(conv_bias + time_embed[step])),
            flops=1 << 28,
        )
        common = (
            place,
            to_all(stats, "y"),
            hidden,
            row(norm2_gain),
            row(norm2_bias),
            w_query,
            w_keyvalue,
            w_out,
            kv,
        )
        if step == 1:
            (out,) = call(
                attend_own_kernel,
                "attend1",
                [((2, ROWS, CHANNELS), F32)],
                (*common, earlier),
                scalars=1,
                flops=1 << 30,
            )
            return out.reshape(2, 2, COLS, CHANNELS)
        state, earlier, stats, kv = call(
            attend_quad_kernel,
            "attend0",
            [(quad, F32), ((ROWS, CHANNELS), F32), stats8, ((QUAD_ROWS, CHANNELS), BF16)],
            common,
            scalars=1,
            flops=1 << 30,
        )


def solution(mesh):
    torus = Mesh(
        mesh.devices.reshape(mesh.shape["req"], 8, 2, 2), ("req", "y", "zh", "core")
    )
    placed = (
        P(REQ_PATCH, None, None),
        P(REQ_PATCH, None, None),
        P(REQ_PATCH, None),
        P(REQ_PATCH, None),
        P(),
        P(),
        P(None, None, None, PATCH),
        P(),
        P("req", None),
        P(),
        P(),
        P(),
        P(),
        P(),
    )
    return jax.shard_map(
        per_device,
        mesh=torus,
        in_specs=placed,
        out_specs=P(None, REQ_PATCH, None, None),
        check_vma=False,
    )
```

```python
import functools

import jax
import jax.numpy as jnp
from jax import lax
from jax.experimental import pallas as pl
from jax.experimental.pallas import tpu as pltpu
from jax.sharding import Mesh
from jax.sharding import PartitionSpec as P

GROUPS = 32
HEADS = 5
HEAD_DIM = 64
WIDTH = HEADS * HEAD_DIM
CHANNELS = 640
MEMBERS = CHANNELS // GROUPS
COLS = 16
ROWS = 32
LANES = 128
QUAD_ROWS = 4 * ROWS
POSITIONS = 1024
EPS = 1e-05

PATCH = ("y", "zh", "core")
QUAD = ("zh", "core")
REQ_PATCH = ("req", "y", "zh", "core")

F32 = jnp.float32
BF16 = jnp.bfloat16

NN = (((1,), (0,)), ((), ()))
NT = (((1,), (1,)), ((), ()))


def dot(a, b, dims=NN):
    return lax.dot_general(a, b, dims, preferred_element_type=F32)


def thirds(x):
    high = x.astype(BF16)
    rest = x - high.astype(F32)
    middle = rest.astype(BF16)
    low = (rest - middle.astype(F32)).astype(BF16)
    return high, middle, low


def picked(x, zero_one, dims=NN):
    rows = x.shape[0]
    stacked = jnp.concatenate([t.astype(F32) for t in thirds(x)], axis=0).astype(BF16)
    out = dot(stacked, zero_one, dims)
    return out[:rows] + out[rows : 2 * rows] + out[2 * rows :]


def group_matrix():
    channel = lax.broadcasted_iota(jnp.int32, (CHANNELS, LANES), 0)
    first = lax.broadcasted_iota(jnp.int32, (CHANNELS, LANES), 1) * MEMBERS
    return jnp.where((channel >= first) & (channel < first + MEMBERS), 1.0, 0.0).astype(BF16)


def eight(rows, lanes):
    have = sum(r.shape[0] for r in rows)
    return jnp.concatenate([*rows, jnp.zeros((8 - have, lanes), F32)], axis=0)


def tell_sums(x, groups, stats_ref):
    sums = eight(
        [jnp.sum(x, axis=0, keepdims=True), jnp.sum(x * x, axis=0, keepdims=True)], CHANNELS
    )
    told = picked(sums, groups)[0:4]
    stats_ref[...] = jnp.broadcast_to(told[None], stats_ref.shape)


def mean_and_scale(stats_ref, groups):
    return spread_sums(jnp.sum(stats_ref[...], axis=0), groups)


def spread_sums(sums, groups):
    number = POSITIONS * MEMBERS
    mean = sums[0:1] * (1.0 / number)
    variance = sums[1:2] * (1.0 / number) - mean * mean
    spread = picked(eight([mean, lax.rsqrt(variance + EPS)], LANES), groups, NT)
    return spread[0:1], spread[1:2]


def pack_kernel(field_ref, stale_ref, keys_ref, values_ref, packed_ref):
    high, middle, _ = thirds(field_ref[...])
    both = jnp.concatenate(
        [keys_ref[...].astype(F32), values_ref[...].astype(F32)], axis=1
    ).astype(BF16)
    for to in range(4):
        packed_ref[to, 0:ROWS] = high
        packed_ref[to, ROWS : 2 * ROWS] = middle
        packed_ref[to, 2 * ROWS : 3 * ROWS] = stale_ref[...]
        packed_ref[to, 3 * ROWS :] = both


def unpack_kernel(
    place_ref,
    packed_ref,
    field_ref,
    state_ref,
    stats_ref,
    kv_ref,
    prior_ref,
    first_ref,
    last_ref,
):
    a = place_ref[1]
    for t in range(4):
        state_ref[t] = packed_ref[t, 0:ROWS].astype(F32) + packed_ref[t, ROWS : 2 * ROWS].astype(F32)
        prior_ref[t] = packed_ref[t, 2 * ROWS : 3 * ROWS]
        kv_ref[t] = packed_ref[t, 3 * ROWS :]
    state_ref[a] = field_ref[...]
    first_ref[...] = prior_ref[0, :COLS]
    last_ref[...] = prior_ref[3, COLS:]
    tell_sums(state_ref[...].reshape(QUAD_ROWS, CHANNELS), group_matrix(), stats_ref)


def activate(stats_ref, state_ref, prior_ref, above_ref, below_ref, gain_ref, bias_ref, keep, rows):
    mean, scale = mean_and_scale(stats_ref, group_matrix())
    for t in range(4):
        value = (state_ref[t] - mean) * scale * gain_ref[...] + bias_ref[...]
        act = (value * (1.0 / (1.0 + jnp.exp(-value)))).astype(BF16)
        rows[t, COLS : 3 * COLS] = act
        keep(t, act)
        rows[t, 0:COLS] = above_ref[...] if t == 0 else prior_ref[t - 1, COLS:]
        rows[t, 3 * COLS :] = below_ref[...] if t == 3 else prior_ref[t + 1, :COLS]


def convolve(rows, weight_ref, wide):
    window = rows[...].reshape(4 * 64, CHANNELS)
    wide[...] = jnp.zeros(wide.shape, F32)
    col = lax.broadcasted_iota(jnp.int32, (LANES, LANES), 0) & (COLS - 1)
    lane = lax.broadcasted_iota(jnp.int32, (LANES, LANES), 1)
    tiles = [jnp.zeros((LANES, LANES), F32), jnp.zeros((LANES, LANES), F32)]
    for part in range(8):
        wide[:, 0 : 9 * MEMBERS] = dot(window, weight_ref[part], NT)
        whole = wide[...].reshape(4, 64, 256)
        lines = [
            whole[:, COLS * r : COLS * r + 2 * COLS].reshape(LANES, 256) for r in range(3)
        ]
        total = (
            lines[0][:, :LANES]
            + pltpu.roll(lines[1][:, :LANES], LANES - 3 * MEMBERS, 1)
            + pltpu.roll(lines[2], 256 - 6 * MEMBERS, 1)[:, :LANES]
        )
        left = jnp.where(col > 0, pltpu.roll(total, 1, 0), 0.0)
        centre = pltpu.roll(total, LANES - MEMBERS, 1)
        right = pltpu.roll(total, LANES - 2 * MEMBERS, 1)
        right = jnp.where(col < COLS - 1, pltpu.roll(right, LANES - 1, 0), 0.0)
        made = left + centre + right
        tile, at = divmod(part, 6)
        at *= MEMBERS
        if at:
            made = pltpu.roll(made, at, 1)
        kept = (lane >= at) & (lane < at + MEMBERS)
        tiles[tile] = jnp.where(kept, made, tiles[tile])
    return tiles


def folded(tile):
    half = tile.shape[0] // 2
    lane = lax.broadcasted_iota(jnp.int32, (half, LANES), 1)
    return jnp.where(lane < 64, tile[:half], pltpu.roll(tile[half:], 64, 1))


def conv_quad_kernel(
    stats_ref,
    state_ref,
    prior_ref,
    above_ref,
    below_ref,
    weight_ref,
    gain_ref,
    bias_ref,
    out_ref,
    act_ref,
    first_ref,
    last_ref,
    rows,
    wide,
):
    def keep(t, act):
        act_ref[t] = act
        if t == 0:
            first_ref[...] = act[:COLS]
        if t == 3:
            last_ref[...] = act[COLS:]

    activate(stats_ref, state_ref, prior_ref, above_ref, below_ref, gain_ref, bias_ref, keep, rows)
    tiles = convolve(rows, weight_ref, wide)
    rest = folded(tiles[1])
    for to in range(4):
        out_ref[to, 0:LANES] = tiles[0]
        out_ref[to, LANES:] = rest


def shard_lanes(shape, dim):
    lane = lax.broadcasted_iota(jnp.int32, shape, dim)
    inner = lane & (LANES - 1)
    part = (inner * 3277) >> 16
    within = inner - MEMBERS * part
    second = lane >= LANES
    used = part < jnp.where(second, 2, 6)
    return part + jnp.where(second, 6, 0), within, used


def conv_own_kernel(
    place_ref,
    stats_ref,
    state_ref,
    prior_ref,
    above_ref,
    below_ref,
    weight_ref,
    gain_ref,
    bias_ref,
    shift_ref,
    out_ref,
    told_ref,
    rows,
    wide,
):
    a = place_ref[1]
    activate(
        stats_ref, state_ref, prior_ref, above_ref, below_ref, gain_ref, bias_ref, lambda t, act: None, rows
    )
    tiles = convolve(rows, weight_ref, wide)
    for t in range(4):
        mine = slice(t * ROWS, (t + 1) * ROWS)
        out_ref[t, 0:ROWS] = tiles[0][mine]
        out_ref[t, ROWS:] = folded(tiles[1][mine])
    part, within, used = shard_lanes((CHANNELS, 256), 1)
    channel = lax.broadcasted_iota(jnp.int32, (CHANNELS, 256), 0)
    select = used & (channel == 4 * MEMBERS * part + MEMBERS * a + within)
    select = jnp.where(select, 1.0, 0.0).astype(BF16)
    part, _, used = shard_lanes((LANES, 256), 1)
    group = lax.broadcasted_iota(jnp.int32, (LANES, 256), 0)
    holds = jnp.where(used & (group == 4 * part + a), 1.0, 0.0).astype(BF16)
    state = state_ref[...].reshape(QUAD_ROWS, CHANNELS)
    hidden = picked(state, select) + (
        jnp.concatenate(tiles, axis=1) + picked(eight([shift_ref[...]], CHANNELS), select)[0:1]
    )
    sums = eight(
        [jnp.sum(hidden, axis=0, keepdims=True), jnp.sum(hidden * hidden, axis=0, keepdims=True)],
        256,
    )
    told = picked(sums, holds, NT)[0:4]
    told_ref[...] = jnp.broadcast_to(told[None], told_ref.shape)


def insert_kernel(conv_ref, stats_ref, out_ref):
    sums = jnp.sum(stats_ref[...], axis=0)
    for to in range(4):
        out_ref[to, 0:48] = conv_ref[to]
        out_ref[to, 48:] = eight([sums], LANES)


def assembled(conv_ref, count):
    lane = lax.broadcasted_iota(jnp.int32, (count, LANES), 1)
    tiles = [jnp.zeros((count, LANES), F32) for _ in range(5)]
    for t in range(4):
        rest = conv_ref[t, count : count + count // 2]
        sources = (
            conv_ref[t, 0:count],
            jnp.concatenate([rest, pltpu.roll(rest, 64, 1)], axis=0),
        )
        for part in range(8):
            source, at = divmod(part, 6)
            at *= MEMBERS
            tile, to = divmod(4 * MEMBERS * part + MEMBERS * t, LANES)
            turn = (to - at) % LANES
            block = sources[source]
            if turn:
                block = pltpu.roll(block, turn, 1)
            kept = (lane >= to) & (lane < to + MEMBERS)
            tiles[tile] = jnp.where(kept, block, tiles[tile])
            if to + MEMBERS > LANES:
                kept = lane < to + MEMBERS - LANES
                tiles[tile + 1] = jnp.where(kept, block, tiles[tile + 1])
    return jnp.concatenate(tiles, axis=1)


def hidden_kernel(conv_ref, state_ref, shift_ref, hidden_ref, stats_ref):
    state = state_ref[...].reshape(QUAD_ROWS, CHANNELS)
    hidden = state + (assembled(conv_ref, QUAD_ROWS) + shift_ref[...])
    hidden_ref[...] = hidden.reshape(hidden_ref.shape)
    tell_sums(hidden, group_matrix(), stats_ref)


def project(hidden, mean, scale, gain_ref, bias_ref, query_ref, keyvalue_ref):
    normed = ((hidden - mean) * scale * gain_ref[...] + bias_ref[...]).astype(BF16)
    query = dot(normed, query_ref[...]).astype(BF16).astype(F32)
    query = jnp.concatenate(
        [query, jnp.zeros((hidden.shape[0], 3 * LANES - WIDTH), F32)], axis=1
    )
    return query.astype(BF16), dot(normed, keyvalue_ref[...]).astype(BF16)


def project_kernel(
    stats_ref, hidden_ref, gain_ref, bias_ref, query_ref, keyvalue_ref, asked_ref, fresh_ref
):
    mean, scale = mean_and_scale(stats_ref, group_matrix())
    hidden = hidden_ref[...].reshape(QUAD_ROWS, CHANNELS)
    asked, fresh = project(hidden, mean, scale, gain_ref, bias_ref, query_ref, keyvalue_ref)
    asked_ref[...] = asked
    fresh_ref[...] = fresh


def attend(query, fresh, patch, y, kv_ref):
    count = query.shape[0]
    lane = lax.broadcasted_iota(jnp.int32, (count, LANES), 1)
    low = lane < HEAD_DIM

    column = lax.broadcasted_iota(jnp.int32, (count, POSITIONS), 1) >> 5
    replaced = column == 4 * y + patch
    if count == ROWS:
        theirs = None
    else:
        theirs = (lax.broadcasted_iota(jnp.int32, (count, count), 1) >> 5) == patch
    tiles = [jnp.zeros((count, LANES), F32) for _ in range(3)]
    for h in range(HEADS):
        at = LANES * (h // 2)
        own = low if h % 2 == 0 else ~low
        asked = jnp.where(own, query[:, at : at + LANES].astype(F32), 0.0).astype(BF16)
        old = dot(asked, kv_ref[:, at : at + LANES], NT) * HEAD_DIM ** (-0.5)
        old = jnp.where(replaced, -jnp.inf, old)
        new = dot(asked, fresh[:, at : at + LANES], NT) * HEAD_DIM ** (-0.5)
        if theirs is not None:
            new = jnp.where(theirs, new, -jnp.inf)
        peak = jnp.maximum(
            jnp.max(old, axis=1, keepdims=True), jnp.max(new, axis=1, keepdims=True)
        )
        old = jnp.exp(old - peak)
        new = jnp.exp(new - peak)
        total = jnp.sum(old, axis=1, keepdims=True) + jnp.sum(new, axis=1, keepdims=True)
        at = LANES * ((HEADS + h) // 2)
        summed = dot(old.astype(BF16), kv_ref[:, at : at + LANES])
        summed += dot(new.astype(BF16), fresh[:, at : at + LANES])
        summed = pltpu.roll(summed / total, HEAD_DIM, 1)
        tiles[h // 2] = jnp.where(own, summed, tiles[h // 2])
    return jnp.concatenate(tiles, axis=1)[:, :WIDTH].astype(BF16)


def attend_quad_kernel(
    place_ref, asked_ref, fresh_ref, hidden_ref, out_ref, kv_ref, state_ref, told_ref
):
    patch = lax.broadcasted_iota(jnp.int32, (QUAD_ROWS, 1), 0) >> 5
    attended = attend(asked_ref[...], fresh_ref[...], patch, place_ref[0], kv_ref)
    result = hidden_ref[...].reshape(QUAD_ROWS, CHANNELS) + dot(attended, out_ref[...])
    state_ref[...] = result.reshape(state_ref.shape)
    tell_sums(result, group_matrix(), told_ref)


def attend_own_kernel(
    place_ref,
    conv_ref,
    state_ref,
    shift_ref,
    gain_ref,
    bias_ref,
    query_ref,
    keyvalue_ref,
    out_ref,
    kv_ref,
    result_ref,
):
    a = place_ref[1]
    earlier = state_ref[a]
    hidden = earlier + (assembled(conv_ref, ROWS) + shift_ref[...])
    sums = jnp.zeros((8, LANES), F32)
    for t in range(4):
        sums += conv_ref[t, 48:56]
    mean, scale = spread_sums(sums, group_matrix())
    query, fresh = project(hidden, mean, scale, gain_ref, bias_ref, query_ref, keyvalue_ref)
    attended = attend(query, fresh, a, place_ref[0], kv_ref)
    result_ref[0] = earlier
    result_ref[1] = hidden + dot(attended, out_ref[...])


VMEM = pl.BlockSpec(memory_space=pltpu.VMEM)
SMEM = pl.BlockSpec(memory_space=pltpu.SMEM)


def call(kernel, name, out_shapes, args, scalars=0, scratch=(), flops=0):
    return pl.pallas_call(
        kernel,
        name=name,
        out_shape=[jax.ShapeDtypeStruct(s, t) for s, t in out_shapes],
        in_specs=[SMEM] * scalars + [VMEM] * (len(args) - scalars),
        out_specs=[VMEM] * len(out_shapes),
        scratch_shapes=list(scratch),
        cost_estimate=pl.CostEstimate(flops=flops, bytes_accessed=1 << 20, transcendentals=0),
        compiler_params=pltpu.CompilerParams(vmem_limit_bytes=20 << 20),
    )(*args)


def to_all(value, axes):
    return lax.all_to_all(value, axes, 0, 0, tiled=True)


def per_device(
    field,
    stale_conv_in,
    stale_keys,
    stale_values,
    norm1_gain,
    norm1_bias,
    conv_weight,
    conv_bias,
    time_embed,
    norm2_gain,
    norm2_bias,
    w_query,
    w_keyvalue,
    w_out,
):
    quad = (4, ROWS, CHANNELS)
    line = (COLS, CHANNELS)
    stats8 = ((8, 4, LANES), F32)
    y = lax.axis_index("y")
    a = 2 * lax.axis_index("zh") + lax.axis_index("core")
    place = jnp.stack([y, a]).astype(jnp.int32)
    up = [(i, i + 1) for i in range(7)]
    down = [(i + 1, i) for i in range(7)]
    row = lambda v: v.reshape(1, CHANNELS)

    slices = conv_weight.transpose(0, 1, 3, 2).reshape(9 * MEMBERS, CHANNELS)
    weights = lax.all_gather(slices, "y", axis=0, tiled=False)

    own = field.reshape(ROWS, CHANNELS)
    (packed,) = call(
        pack_kernel,
        "pack",
        [((4, 4 * ROWS, CHANNELS), BF16)],
        (own, stale_conv_in.reshape(ROWS, CHANNELS), stale_keys, stale_values),
    )
    state, stats, kv, prior, first, last = call(
        unpack_kernel,
        "unpack",
        [(quad, F32), stats8, (quad, BF16), (quad, BF16), (line, BF16), (line, BF16)],
        (place, to_all(packed, QUAD), own),
        scalars=1,
    )
    norm1 = (row(norm1_gain), row(norm1_bias))
    norm2 = (row(norm2_gain), row(norm2_bias))
    buffers = [pltpu.VMEM((4, 64, CHANNELS), BF16), pltpu.VMEM((256, 256), F32)]
    gathered = lambda v: lax.all_gather(
        v.reshape(QUAD_ROWS, CHANNELS), "y", axis=0, tiled=True
    )
    above = lax.ppermute(last, "y", up)
    below = lax.ppermute(first, "y", down)
    old = gathered(kv)

    conv, prior, first, last = call(
        conv_quad_kernel,
        "conv0",
        [((4, LANES + 64, LANES), F32), (quad, BF16), (line, BF16), (line, BF16)],
        (to_all(stats, "y"), state, prior, above, below, weights, *norm1),
        scratch=buffers,
        flops=1 << 30,
    )
    conv, above, below = lax.optimization_barrier(
        (to_all(conv, QUAD), lax.ppermute(last, "y", up), lax.ppermute(first, "y", down))
    )
    hidden, stats = call(
        hidden_kernel,
        "hidden0",
        [(quad, F32), stats8],
        (conv, state, row(conv_bias + time_embed[0])),
        flops=1 << 28,
    )
    asked, fresh = call(
        project_kernel,
        "project0",
        [((QUAD_ROWS, 3 * LANES), BF16), ((QUAD_ROWS, CHANNELS), BF16)],
        (to_all(stats, "y"), hidden, *norm2, w_query, w_keyvalue),
        flops=1 << 28,
    )
    kv = gathered(fresh)
    state, stats = call(
        attend_quad_kernel,
        "attend0",
        [(quad, F32), stats8],
        (place, asked, fresh, hidden, w_out, old),
        scalars=1,
        flops=1 << 30,
    )
    shift = row(conv_bias + time_embed[1])
    conv, stats = call(
        conv_own_kernel,
        "conv1",
        [((4, ROWS + ROWS // 2, LANES), F32), stats8],
        (place, to_all(stats, "y"), state, prior, above, below, weights, *norm1, shift),
        scalars=1,
        scratch=buffers,
        flops=1 << 30,
    )
    (conv,) = call(
        insert_kernel,
        "insert1",
        [((4, 56, LANES), F32)],
        (conv, to_all(stats, "y")),
        flops=1 << 24,
    )
    (out,) = call(
        attend_own_kernel,
        "attend1",
        [((2, ROWS, CHANNELS), F32)],
        (place, to_all(conv, QUAD), state, shift, *norm2, w_query, w_keyvalue, w_out, kv),
        scalars=1,
        flops=1 << 30,
    )
    return out.reshape(2, 2, COLS, CHANNELS)


def solution(mesh):
    torus = Mesh(
        mesh.devices.reshape(mesh.shape["req"], 8, 2, 2), ("req", "y", "zh", "core")
    )
    placed = (
        P(REQ_PATCH, None, None),
        P(REQ_PATCH, None, None),
        P(REQ_PATCH, None),
        P(REQ_PATCH, None),
        P(),
        P(),
        P(None, None, None, PATCH),
        P(),
        P("req", None),
        P(),
        P(),
        P(),
        P(),
        P(),
    )
    return jax.shard_map(
        per_device,
        mesh=torus,
        in_specs=placed,
        out_specs=P(None, REQ_PATCH, None, None),
        check_vma=False,
    )
```

```python
import functools

import jax
import jax.numpy as jnp
from jax import lax
from jax.experimental import pallas as pl
from jax.experimental.pallas import tpu as pltpu
from jax.sharding import Mesh
from jax.sharding import PartitionSpec as P

GROUPS = 32
HEADS = 5
HEAD_DIM = 64
WIDTH = HEADS * HEAD_DIM
CHANNELS = 640
MEMBERS = CHANNELS // GROUPS
COLS = 16
ROWS = 32
LANES = 128
QUAD_ROWS = 4 * ROWS
POSITIONS = 1024
EPS = 1e-05

PATCH = ("y", "zh", "core")
QUAD = ("zh", "core")
REQ_PATCH = ("req", "y", "zh", "core")

F32 = jnp.float32
BF16 = jnp.bfloat16

NN = (((1,), (0,)), ((), ()))
NT = (((1,), (1,)), ((), ()))


def dot(a, b, dims=NN):
    return lax.dot_general(a, b, dims, preferred_element_type=F32)


def thirds(x):
    high = x.astype(BF16)
    rest = x - high.astype(F32)
    middle = rest.astype(BF16)
    low = (rest - middle.astype(F32)).astype(BF16)
    return high, middle, low


def picked(x, zero_one, dims=NN):
    rows = x.shape[0]
    stacked = jnp.concatenate([t.astype(F32) for t in thirds(x)], axis=0).astype(BF16)
    out = dot(stacked, zero_one, dims)
    return out[:rows] + out[rows : 2 * rows] + out[2 * rows :]


def group_matrix():
    channel = lax.broadcasted_iota(jnp.int32, (CHANNELS, LANES), 0)
    first = lax.broadcasted_iota(jnp.int32, (CHANNELS, LANES), 1) * MEMBERS
    return jnp.where((channel >= first) & (channel < first + MEMBERS), 1.0, 0.0).astype(BF16)


def eight(rows, lanes):
    have = sum(r.shape[0] for r in rows)
    return jnp.concatenate([*rows, jnp.zeros((8 - have, lanes), F32)], axis=0)


def tell_sums(x, groups, stats_ref):
    sums = eight(
        [jnp.sum(x, axis=0, keepdims=True), jnp.sum(x * x, axis=0, keepdims=True)], CHANNELS
    )
    told = picked(sums, groups)[0:4]
    stats_ref[...] = jnp.broadcast_to(told[None], stats_ref.shape)


def mean_and_scale(stats_ref, groups):
    return spread_sums(jnp.sum(stats_ref[...], axis=0), groups)


def spread_sums(sums, groups):
    number = POSITIONS * MEMBERS
    mean = sums[0:1] * (1.0 / number)
    variance = sums[1:2] * (1.0 / number) - mean * mean
    spread = picked(eight([mean, lax.rsqrt(variance + EPS)], LANES), groups, NT)
    return spread[0:1], spread[1:2]


def pack_kernel(field_ref, stale_ref, keys_ref, values_ref, packed_ref):
    high, middle, _ = thirds(field_ref[...])
    both = jnp.concatenate(
        [keys_ref[...].astype(F32), values_ref[...].astype(F32)], axis=1
    ).astype(BF16)
    for to in range(4):
        packed_ref[to, 0:ROWS] = high
        packed_ref[to, ROWS : 2 * ROWS] = middle
        packed_ref[to, 2 * ROWS : 3 * ROWS] = stale_ref[...]
        packed_ref[to, 3 * ROWS :] = both


def unpack_kernel(
    place_ref,
    packed_ref,
    field_ref,
    state_ref,
    stats_ref,
    kv_ref,
    prior_ref,
    first_ref,
    last_ref,
):
    a = place_ref[1]
    for t in range(4):
        state_ref[t] = packed_ref[t, 0:ROWS].astype(F32) + packed_ref[t, ROWS : 2 * ROWS].astype(F32)
        prior_ref[t] = packed_ref[t, 2 * ROWS : 3 * ROWS]
        kv_ref[t] = packed_ref[t, 3 * ROWS :]
    state_ref[a] = field_ref[...]
    first_ref[...] = prior_ref[0, :COLS]
    last_ref[...] = prior_ref[3, COLS:]
    tell_sums(state_ref[...].reshape(QUAD_ROWS, CHANNELS), group_matrix(), stats_ref)


def activate(stats_ref, state_ref, prior_ref, above_ref, below_ref, gain_ref, bias_ref, keep, rows):
    mean, scale = mean_and_scale(stats_ref, group_matrix())
    for t in range(4):
        value = (state_ref[t] - mean) * scale * gain_ref[...] + bias_ref[...]
        act = (value * (1.0 / (1.0 + jnp.exp(-value)))).astype(BF16)
        rows[t, COLS : 3 * COLS] = act
        keep(t, act)
        rows[t, 0:COLS] = above_ref[...] if t == 0 else prior_ref[t - 1, COLS:]
        rows[t, 3 * COLS :] = below_ref[...] if t == 3 else prior_ref[t + 1, :COLS]


def convolve(rows, weight_refs, y, wide):
    window = rows[...].reshape(4 * 64, CHANNELS)
    wide[...] = jnp.zeros(wide.shape, F32)
    col = lax.broadcasted_iota(jnp.int32, (LANES, LANES), 0) & (COLS - 1)
    lane = lax.broadcasted_iota(jnp.int32, (LANES, LANES), 1)
    tiles = [jnp.zeros((LANES, LANES), F32), jnp.zeros((LANES, LANES), F32)]
    for turn, weight_ref in enumerate(weight_refs):
        part = (y - turn) & 7
        wide[:, 0 : 9 * MEMBERS] = dot(window, weight_ref[...], NT)
        whole = wide[...].reshape(4, 64, 256)
        lines = [
            whole[:, COLS * r : COLS * r + 2 * COLS].reshape(LANES, 256) for r in range(3)
        ]
        total = (
            lines[0][:, :LANES]
            + pltpu.roll(lines[1][:, :LANES], LANES - 3 * MEMBERS, 1)
            + pltpu.roll(lines[2], 256 - 6 * MEMBERS, 1)[:, :LANES]
        )
        left = jnp.where(col > 0, pltpu.roll(total, 1, 0), 0.0)
        centre = pltpu.roll(total, LANES - MEMBERS, 1)
        right = pltpu.roll(total, LANES - 2 * MEMBERS, 1)
        right = jnp.where(col < COLS - 1, pltpu.roll(right, LANES - 1, 0), 0.0)
        made = left + centre + right
        at = MEMBERS * jnp.where(part < 6, part, part - 6)
        made = pltpu.roll(made, at, 1)
        kept = (lane >= at) & (lane < at + MEMBERS)
        tiles[0] = jnp.where(kept & (part < 6), made, tiles[0])
        tiles[1] = jnp.where(kept & (part >= 6), made, tiles[1])
    return tiles


def folded(tile):
    half = tile.shape[0] // 2
    lane = lax.broadcasted_iota(jnp.int32, (half, LANES), 1)
    return jnp.where(lane < 64, tile[:half], pltpu.roll(tile[half:], 64, 1))


def conv_quad_kernel(
    place_ref,
    stats_ref,
    state_ref,
    prior_ref,
    above_ref,
    below_ref,
    gain_ref,
    bias_ref,
    *refs,
):
    weight_refs = refs[:8]
    out_ref, act_ref, first_ref, last_ref, rows, wide = refs[8:]

    def keep(t, act):
        act_ref[t] = act
        if t == 0:
            first_ref[...] = act[:COLS]
        if t == 3:
            last_ref[...] = act[COLS:]

    activate(stats_ref, state_ref, prior_ref, above_ref, below_ref, gain_ref, bias_ref, keep, rows)
    tiles = convolve(rows, weight_refs, place_ref[0], wide)
    rest = folded(tiles[1])
    for to in range(4):
        out_ref[to, 0:LANES] = tiles[0]
        out_ref[to, LANES:] = rest


def shard_lanes(shape, dim):
    lane = lax.broadcasted_iota(jnp.int32, shape, dim)
    inner = lane & (LANES - 1)
    part = (inner * 3277) >> 16
    within = inner - MEMBERS * part
    second = lane >= LANES
    used = part < jnp.where(second, 2, 6)
    return part + jnp.where(second, 6, 0), within, used


def conv_own_kernel(
    place_ref,
    stats_ref,
    state_ref,
    prior_ref,
    above_ref,
    below_ref,
    gain_ref,
    bias_ref,
    shift_ref,
    *refs,
):
    weight_refs = refs[:8]
    out_ref, told_ref, rows, wide = refs[8:]
    a = place_ref[1]
    activate(
        stats_ref, state_ref, prior_ref, above_ref, below_ref, gain_ref, bias_ref, lambda t, act: None, rows
    )
    tiles = convolve(rows, weight_refs, place_ref[0], wide)
    for t in range(4):
        mine = slice(t * ROWS, (t + 1) * ROWS)
        out_ref[t, 0:ROWS] = tiles[0][mine]
        out_ref[t, ROWS:] = folded(tiles[1][mine])
    part, within, used = shard_lanes((CHANNELS, 256), 1)
    channel = lax.broadcasted_iota(jnp.int32, (CHANNELS, 256), 0)
    select = used & (channel == 4 * MEMBERS * part + MEMBERS * a + within)
    select = jnp.where(select, 1.0, 0.0).astype(BF16)
    part, _, used = shard_lanes((LANES, 256), 1)
    group = lax.broadcasted_iota(jnp.int32, (LANES, 256), 0)
    holds = jnp.where(used & (group == 4 * part + a), 1.0, 0.0).astype(BF16)
    state = state_ref[...].reshape(QUAD_ROWS, CHANNELS)
    hidden = picked(state, select) + (
        jnp.concatenate(tiles, axis=1) + picked(eight([shift_ref[...]], CHANNELS), select)[0:1]
    )
    sums = eight(
        [jnp.sum(hidden, axis=0, keepdims=True), jnp.sum(hidden * hidden, axis=0, keepdims=True)],
        256,
    )
    told = picked(sums, holds, NT)[0:4]
    told_ref[...] = jnp.broadcast_to(told[None], told_ref.shape)


def insert_kernel(conv_ref, stats_ref, out_ref):
    sums = jnp.sum(stats_ref[...], axis=0)
    for to in range(4):
        out_ref[to, 0:48] = conv_ref[to]
        out_ref[to, 48:] = eight([sums], LANES)


def assembled(conv_ref, count):
    lane = lax.broadcasted_iota(jnp.int32, (count, LANES), 1)
    tiles = [jnp.zeros((count, LANES), F32) for _ in range(5)]
    for t in range(4):
        rest = conv_ref[t, count : count + count // 2]
        sources = (
            conv_ref[t, 0:count],
            jnp.concatenate([rest, pltpu.roll(rest, 64, 1)], axis=0),
        )
        for part in range(8):
            source, at = divmod(part, 6)
            at *= MEMBERS
            tile, to = divmod(4 * MEMBERS * part + MEMBERS * t, LANES)
            turn = (to - at) % LANES
            block = sources[source]
            if turn:
                block = pltpu.roll(block, turn, 1)
            kept = (lane >= to) & (lane < to + MEMBERS)
            tiles[tile] = jnp.where(kept, block, tiles[tile])
            if to + MEMBERS > LANES:
                kept = lane < to + MEMBERS - LANES
                tiles[tile + 1] = jnp.where(kept, block, tiles[tile + 1])
    return jnp.concatenate(tiles, axis=1)


def hidden_kernel(conv_ref, state_ref, shift_ref, hidden_ref, stats_ref):
    state = state_ref[...].reshape(QUAD_ROWS, CHANNELS)
    hidden = state + (assembled(conv_ref, QUAD_ROWS) + shift_ref[...])
    hidden_ref[...] = hidden.reshape(hidden_ref.shape)
    tell_sums(hidden, group_matrix(), stats_ref)


def project(hidden, mean, scale, gain_ref, bias_ref, query_ref, keyvalue_ref):
    normed = ((hidden - mean) * scale * gain_ref[...] + bias_ref[...]).astype(BF16)
    query = dot(normed, query_ref[...]).astype(BF16).astype(F32)
    query = jnp.concatenate(
        [query, jnp.zeros((hidden.shape[0], 3 * LANES - WIDTH), F32)], axis=1
    )
    return query.astype(BF16), dot(normed, keyvalue_ref[...]).astype(BF16)


def project_kernel(
    stats_ref, hidden_ref, gain_ref, bias_ref, query_ref, keyvalue_ref, asked_ref, fresh_ref
):
    mean, scale = mean_and_scale(stats_ref, group_matrix())
    hidden = hidden_ref[...].reshape(QUAD_ROWS, CHANNELS)
    asked, fresh = project(hidden, mean, scale, gain_ref, bias_ref, query_ref, keyvalue_ref)
    asked_ref[...] = asked
    fresh_ref[...] = fresh


def attend(query, fresh, patch, y, kv_ref):
    count = query.shape[0]
    lane = lax.broadcasted_iota(jnp.int32, (count, LANES), 1)
    low = lane < HEAD_DIM

    column = lax.broadcasted_iota(jnp.int32, (count, POSITIONS), 1) >> 5
    replaced = column == 4 * y + patch
    if count == ROWS:
        theirs = None
    else:
        theirs = (lax.broadcasted_iota(jnp.int32, (count, count), 1) >> 5) == patch
    tiles = [jnp.zeros((count, LANES), F32) for _ in range(3)]
    for h in range(HEADS):
        at = LANES * (h // 2)
        own = low if h % 2 == 0 else ~low
        asked = jnp.where(own, query[:, at : at + LANES].astype(F32), 0.0).astype(BF16)
        old = dot(asked, kv_ref[:, at : at + LANES], NT) * HEAD_DIM ** (-0.5)
        old = jnp.where(replaced, -jnp.inf, old)
        new = dot(asked, fresh[:, at : at + LANES], NT) * HEAD_DIM ** (-0.5)
        if theirs is not None:
            new = jnp.where(theirs, new, -jnp.inf)
        peak = jnp.maximum(
            jnp.max(old, axis=1, keepdims=True), jnp.max(new, axis=1, keepdims=True)
        )
        old = jnp.exp(old - peak)
        new = jnp.exp(new - peak)
        total = jnp.sum(old, axis=1, keepdims=True) + jnp.sum(new, axis=1, keepdims=True)
        at = LANES * ((HEADS + h) // 2)
        summed = dot(old.astype(BF16), kv_ref[:, at : at + LANES])
        summed += dot(new.astype(BF16), fresh[:, at : at + LANES])
        summed = pltpu.roll(summed / total, HEAD_DIM, 1)
        tiles[h // 2] = jnp.where(own, summed, tiles[h // 2])
    return jnp.concatenate(tiles, axis=1)[:, :WIDTH].astype(BF16)


def attend_quad_kernel(
    place_ref, asked_ref, fresh_ref, hidden_ref, out_ref, kv_ref, state_ref, told_ref
):
    patch = lax.broadcasted_iota(jnp.int32, (QUAD_ROWS, 1), 0) >> 5
    attended = attend(asked_ref[...], fresh_ref[...], patch, place_ref[0], kv_ref)
    result = hidden_ref[...].reshape(QUAD_ROWS, CHANNELS) + dot(attended, out_ref[...])
    state_ref[...] = result.reshape(state_ref.shape)
    tell_sums(result, group_matrix(), told_ref)


def attend_own_kernel(
    place_ref,
    conv_ref,
    state_ref,
    shift_ref,
    gain_ref,
    bias_ref,
    query_ref,
    keyvalue_ref,
    out_ref,
    kv_ref,
    result_ref,
):
    a = place_ref[1]
    earlier = state_ref[a]
    hidden = earlier + (assembled(conv_ref, ROWS) + shift_ref[...])
    sums = jnp.zeros((8, LANES), F32)
    for t in range(4):
        sums += conv_ref[t, 48:56]
    mean, scale = spread_sums(sums, group_matrix())
    query, fresh = project(hidden, mean, scale, gain_ref, bias_ref, query_ref, keyvalue_ref)
    attended = attend(query, fresh, a, place_ref[0], kv_ref)
    result_ref[0] = earlier
    result_ref[1] = hidden + dot(attended, out_ref[...])


VMEM = pl.BlockSpec(memory_space=pltpu.VMEM)
SMEM = pl.BlockSpec(memory_space=pltpu.SMEM)


def call(kernel, name, out_shapes, args, scalars=0, scratch=(), flops=0):
    return pl.pallas_call(
        kernel,
        name=name,
        out_shape=[jax.ShapeDtypeStruct(s, t) for s, t in out_shapes],
        in_specs=[SMEM] * scalars + [VMEM] * (len(args) - scalars),
        out_specs=[VMEM] * len(out_shapes),
        scratch_shapes=list(scratch),
        cost_estimate=pl.CostEstimate(flops=flops, bytes_accessed=1 << 20, transcendentals=0),
        compiler_params=pltpu.CompilerParams(vmem_limit_bytes=20 << 20),
    )(*args)


def to_all(value, axes):
    return lax.all_to_all(value, axes, 0, 0, tiled=True)


def per_device(
    field,
    stale_conv_in,
    stale_keys,
    stale_values,
    norm1_gain,
    norm1_bias,
    conv_weight,
    conv_bias,
    time_embed,
    norm2_gain,
    norm2_bias,
    w_query,
    w_keyvalue,
    w_out,
):
    quad = (4, ROWS, CHANNELS)
    line = (COLS, CHANNELS)
    stats8 = ((8, 4, LANES), F32)
    y = lax.axis_index("y")
    a = 2 * lax.axis_index("zh") + lax.axis_index("core")
    place = jnp.stack([y, a]).astype(jnp.int32)
    up = [(i, i + 1) for i in range(7)]
    down = [(i + 1, i) for i in range(7)]
    row = lambda v: v.reshape(1, CHANNELS)

    slices = conv_weight.transpose(0, 1, 3, 2).reshape(9 * MEMBERS, CHANNELS)
    onward = [(i, (i + 1) % 8) for i in range(8)]
    back = [((i + 1) % 8, i) for i in range(8)]
    weights = [slices] + [None] * 7

    def pass_on(hop):
        weights[hop] = lax.ppermute(weights[hop - 1], "y", onward)
        if hop < 4:
            weights[-hop] = lax.ppermute(weights[(1 - hop) % 8], "y", back)

    pass_on(1)
    pass_on(2)

    own = field.reshape(ROWS, CHANNELS)
    (packed,) = call(
        pack_kernel,
        "pack",
        [((4, 4 * ROWS, CHANNELS), BF16)],
        (own, stale_conv_in.reshape(ROWS, CHANNELS), stale_keys, stale_values),
    )
    packed, weights[1], weights[7], weights[2], weights[6] = lax.optimization_barrier(
        (to_all(packed, QUAD), weights[1], weights[7], weights[2], weights[6])
    )
    state, stats, kv, prior, first, last = call(
        unpack_kernel,
        "unpack",
        [(quad, F32), stats8, (quad, BF16), (quad, BF16), (line, BF16), (line, BF16)],
        (place, packed, own),
        scalars=1,
    )
    pass_on(3)
    pass_on(4)
    norm1 = (row(norm1_gain), row(norm1_bias))
    norm2 = (row(norm2_gain), row(norm2_bias))
    buffers = [pltpu.VMEM((4, 64, CHANNELS), BF16), pltpu.VMEM((256, 256), F32)]
    gathered = lambda v: lax.all_gather(
        v.reshape(QUAD_ROWS, CHANNELS), "y", axis=0, tiled=True
    )
    above = lax.ppermute(last, "y", up)
    below = lax.ppermute(first, "y", down)
    old = gathered(kv)

    conv, prior, first, last = call(
        conv_quad_kernel,
        "conv0",
        [((4, LANES + 64, LANES), F32), (quad, BF16), (line, BF16), (line, BF16)],
        (place, to_all(stats, "y"), state, prior, above, below, *norm1, *weights),
        scalars=1,
        scratch=buffers,
        flops=1 << 30,
    )
    conv, above, below = lax.optimization_barrier(
        (to_all(conv, QUAD), lax.ppermute(last, "y", up), lax.ppermute(first, "y", down))
    )
    hidden, stats = call(
        hidden_kernel,
        "hidden0",
        [(quad, F32), stats8],
        (conv, state, row(conv_bias + time_embed[0])),
        flops=1 << 28,
    )
    asked, fresh = call(
        project_kernel,
        "project0",
        [((QUAD_ROWS, 3 * LANES), BF16), ((QUAD_ROWS, CHANNELS), BF16)],
        (to_all(stats, "y"), hidden, *norm2, w_query, w_keyvalue),
        flops=1 << 28,
    )
    kv = gathered(fresh)
    state, stats = call(
        attend_quad_kernel,
        "attend0",
        [(quad, F32), stats8],
        (place, asked, fresh, hidden, w_out, old),
        scalars=1,
        flops=1 << 30,
    )
    shift = row(conv_bias + time_embed[1])
    conv, stats = call(
        conv_own_kernel,
        "conv1",
        [((4, ROWS + ROWS // 2, LANES), F32), stats8],
        (place, to_all(stats, "y"), state, prior, above, below, *norm1, shift, *weights),
        scalars=1,
        scratch=buffers,
        flops=1 << 30,
    )
    (conv,) = call(
        insert_kernel,
        "insert1",
        [((4, 56, LANES), F32)],
        (conv, to_all(stats, "y")),
        flops=1 << 24,
    )
    (out,) = call(
        attend_own_kernel,
        "attend1",
        [((2, ROWS, CHANNELS), F32)],
        (place, to_all(conv, QUAD), state, shift, *norm2, w_query, w_keyvalue, w_out, kv),
        scalars=1,
        flops=1 << 30,
    )
    return out.reshape(2, 2, COLS, CHANNELS)


def solution(mesh):
    torus = Mesh(
        mesh.devices.reshape(mesh.shape["req"], 8, 2, 2), ("req", "y", "zh", "core")
    )
    placed = (
        P(REQ_PATCH, None, None),
        P(REQ_PATCH, None, None),
        P(REQ_PATCH, None),
        P(REQ_PATCH, None),
        P(),
        P(),
        P(None, None, None, PATCH),
        P(),
        P("req", None),
        P(),
        P(),
        P(),
        P(),
        P(),
    )
    return jax.shard_map(
        per_device,
        mesh=torus,
        in_specs=placed,
        out_specs=P(None, REQ_PATCH, None, None),
        check_vma=False,
    )
```

```python
import functools

import jax
import jax.numpy as jnp
from jax import lax
from jax.experimental import pallas as pl
from jax.experimental.pallas import tpu as pltpu
from jax.sharding import Mesh
from jax.sharding import PartitionSpec as P

GROUPS = 32
HEADS = 5
HEAD_DIM = 64
WIDTH = HEADS * HEAD_DIM
CHANNELS = 640
MEMBERS = CHANNELS // GROUPS
COLS = 16
ROWS = 32
LANES = 128
QUAD_ROWS = 4 * ROWS
POSITIONS = 1024
EPS = 1e-05

PATCH = ("y", "zh", "core")
QUAD = ("zh", "core")
REQ_PATCH = ("req", "y", "zh", "core")

F32 = jnp.float32
BF16 = jnp.bfloat16

NN = (((1,), (0,)), ((), ()))
NT = (((1,), (1,)), ((), ()))


def dot(a, b, dims=NN):
    return lax.dot_general(a, b, dims, preferred_element_type=F32)


def thirds(x):
    high = x.astype(BF16)
    rest = x - high.astype(F32)
    middle = rest.astype(BF16)
    low = (rest - middle.astype(F32)).astype(BF16)
    return high, middle, low


def picked(x, zero_one, dims=NN):
    rows = x.shape[0]
    stacked = jnp.concatenate([t.astype(F32) for t in thirds(x)], axis=0).astype(BF16)
    out = dot(stacked, zero_one, dims)
    return out[:rows] + out[rows : 2 * rows] + out[2 * rows :]


def group_matrix():
    channel = lax.broadcasted_iota(jnp.int32, (CHANNELS, LANES), 0)
    first = lax.broadcasted_iota(jnp.int32, (CHANNELS, LANES), 1) * MEMBERS
    return jnp.where((channel >= first) & (channel < first + MEMBERS), 1.0, 0.0).astype(BF16)


def eight(rows, lanes):
    have = sum(r.shape[0] for r in rows)
    return jnp.concatenate([*rows, jnp.zeros((8 - have, lanes), F32)], axis=0)


def tell_sums(x, groups, stats_ref):
    sums = eight(
        [jnp.sum(x, axis=0, keepdims=True), jnp.sum(x * x, axis=0, keepdims=True)], CHANNELS
    )
    told = picked(sums, groups)[0:4]
    stats_ref[...] = jnp.broadcast_to(told[None], stats_ref.shape)


def mean_and_scale(stats_ref, groups):
    return spread_sums(jnp.sum(stats_ref[...], axis=0), groups)


def spread_sums(sums, groups):
    number = POSITIONS * MEMBERS
    mean = sums[0:1] * (1.0 / number)
    variance = sums[1:2] * (1.0 / number) - mean * mean
    spread = picked(eight([mean, lax.rsqrt(variance + EPS)], LANES), groups, NT)
    return spread[0:1], spread[1:2]


def tell_sums_and_edges(x, y, first, last, out_ref):
    sums = eight(
        [jnp.sum(x, axis=0, keepdims=True), jnp.sum(x * x, axis=0, keepdims=True)], CHANNELS
    )
    terms = [t.astype(F32)[0:2] for t in thirds(picked(sums, group_matrix()))]
    told = jnp.concatenate([*terms, jnp.zeros((10, LANES), F32)], axis=0).astype(BF16)
    for to in range(8):
        out_ref[to, 0:COLS] = told
        edge = jnp.where(y + 1 == to, last.astype(F32), first.astype(F32)).astype(BF16)
        for k in range(5):
            out_ref[to, COLS * (k + 1) : COLS * (k + 2)] = edge[:, LANES * k : LANES * (k + 1)]


def heard_sums(heard_ref):
    terms = jnp.sum(heard_ref[:, 0:COLS].astype(F32), axis=0)
    return terms[0:2] + terms[2:4] + terms[4:6]


def heard_edge(heard_ref, sender, exists):
    row = jnp.concatenate(
        [heard_ref[sender, COLS * (k + 1) : COLS * (k + 2)] for k in range(5)], axis=1
    )
    return jnp.where(exists, row.astype(F32), 0.0).astype(BF16)


def heard_edges(heard_ref, y):
    return heard_edge(heard_ref, (y - 1) & 7, y > 0), heard_edge(heard_ref, (y + 1) & 7, y < 7)


def pack_kernel(field_ref, stale_ref, keys_ref, values_ref, packed_ref, kv_ref):
    high, middle, _ = thirds(field_ref[...])
    packed_ref[0:ROWS] = high
    packed_ref[ROWS : 2 * ROWS] = middle
    packed_ref[2 * ROWS :] = stale_ref[...]
    both = jnp.concatenate(
        [keys_ref[...].astype(F32), values_ref[...].astype(F32)], axis=1
    ).astype(BF16)
    kv_ref[...] = jnp.broadcast_to(both[None], kv_ref.shape)


def unpack_kernel(
    place_ref, field_ref, stale_ref, one_ref, two_ref, three_ref, state_ref, prior_ref, told_ref
):
    a = place_ref[1]
    state_ref[a] = field_ref[...]
    prior_ref[a] = stale_ref[...]
    for k, ref in enumerate((one_ref, two_ref, three_ref), 1):
        state_ref[a ^ k] = ref[0:ROWS].astype(F32) + ref[ROWS : 2 * ROWS].astype(F32)
        prior_ref[a ^ k] = ref[2 * ROWS :]
    tell_sums_and_edges(
        state_ref[...].reshape(QUAD_ROWS, CHANNELS),
        place_ref[0],
        prior_ref[0, :COLS],
        prior_ref[3, COLS:],
        told_ref,
    )


def activate(sums, edges, state_ref, prior_ref, gain_ref, bias_ref, keep, rows):
    mean, scale = spread_sums(sums, group_matrix())
    above, below = edges
    for t in range(4):
        value = (state_ref[t] - mean) * scale * gain_ref[...] + bias_ref[...]
        act = (value * (1.0 / (1.0 + jnp.exp(-value)))).astype(BF16)
        rows[t, COLS : 3 * COLS] = act
        keep(t, act)
        rows[t, 0:COLS] = above if t == 0 else prior_ref[t - 1, COLS:]
        rows[t, 3 * COLS :] = below if t == 3 else prior_ref[t + 1, :COLS]


def convolve(rows, weight_ref, wide):
    window = rows[...].reshape(4 * 64, CHANNELS)
    wide[...] = jnp.zeros(wide.shape, F32)
    col = lax.broadcasted_iota(jnp.int32, (LANES, LANES), 0) & (COLS - 1)
    lane = lax.broadcasted_iota(jnp.int32, (LANES, LANES), 1)
    tiles = [jnp.zeros((LANES, LANES), F32), jnp.zeros((LANES, LANES), F32)]
    for part in range(8):
        wide[:, 0 : 9 * MEMBERS] = dot(window, weight_ref[part], NT)
        whole = wide[...].reshape(4, 64, 256)
        lines = [
            whole[:, COLS * r : COLS * r + 2 * COLS].reshape(LANES, 256) for r in range(3)
        ]
        total = (
            lines[0][:, :LANES]
            + pltpu.roll(lines[1][:, :LANES], LANES - 3 * MEMBERS, 1)
            + pltpu.roll(lines[2], 256 - 6 * MEMBERS, 1)[:, :LANES]
        )
        left = jnp.where(col > 0, pltpu.roll(total, 1, 0), 0.0)
        centre = pltpu.roll(total, LANES - MEMBERS, 1)
        right = pltpu.roll(total, LANES - 2 * MEMBERS, 1)
        right = jnp.where(col < COLS - 1, pltpu.roll(right, LANES - 1, 0), 0.0)
        made = left + centre + right
        tile, at = divmod(part, 6)
        at *= MEMBERS
        if at:
            made = pltpu.roll(made, at, 1)
        kept = (lane >= at) & (lane < at + MEMBERS)
        tiles[tile] = jnp.where(kept, made, tiles[tile])
    return tiles


def folded(tile):
    half = tile.shape[0] // 2
    lane = lax.broadcasted_iota(jnp.int32, (half, LANES), 1)
    return jnp.where(lane < 64, tile[:half], pltpu.roll(tile[half:], 64, 1))


def conv_quad_kernel(
    place_ref,
    heard_ref,
    state_ref,
    prior_ref,
    weight_ref,
    gain_ref,
    bias_ref,
    out_ref,
    act_ref,
    first_ref,
    last_ref,
    rows,
    wide,
):
    def keep(t, act):
        act_ref[t] = act
        if t == 0:
            first_ref[...] = act[:COLS]
        if t == 3:
            last_ref[...] = act[COLS:]

    edges = heard_edges(heard_ref, place_ref[0])
    activate(heard_sums(heard_ref), edges, state_ref, prior_ref, gain_ref, bias_ref, keep, rows)
    tiles = convolve(rows, weight_ref, wide)
    rest = folded(tiles[1])
    for to in range(4):
        out_ref[to, 0:LANES] = tiles[0]
        out_ref[to, LANES:] = rest


def shard_lanes(shape, dim):
    lane = lax.broadcasted_iota(jnp.int32, shape, dim)
    inner = lane & (LANES - 1)
    part = (inner * 3277) >> 16
    within = inner - MEMBERS * part
    second = lane >= LANES
    used = part < jnp.where(second, 2, 6)
    return part + jnp.where(second, 6, 0), within, used


def conv_own_kernel(
    place_ref,
    stats_ref,
    heard_ref,
    state_ref,
    prior_ref,
    weight_ref,
    gain_ref,
    bias_ref,
    shift_ref,
    out_ref,
    told_ref,
    rows,
    wide,
):
    a = place_ref[1]
    activate(
        jnp.sum(stats_ref[...], axis=0),
        heard_edges(heard_ref, place_ref[0]),
        state_ref,
        prior_ref,
        gain_ref,
        bias_ref,
        lambda t, act: None,
        rows,
    )
    tiles = convolve(rows, weight_ref, wide)
    for t in range(4):
        mine = slice(t * ROWS, (t + 1) * ROWS)
        out_ref[t, 0:ROWS] = tiles[0][mine]
        out_ref[t, ROWS:] = folded(tiles[1][mine])
    part, within, used = shard_lanes((CHANNELS, 256), 1)
    channel = lax.broadcasted_iota(jnp.int32, (CHANNELS, 256), 0)
    select = used & (channel == 4 * MEMBERS * part + MEMBERS * a + within)
    select = jnp.where(select, 1.0, 0.0).astype(BF16)
    part, _, used = shard_lanes((LANES, 256), 1)
    group = lax.broadcasted_iota(jnp.int32, (LANES, 256), 0)
    holds = jnp.where(used & (group == 4 * part + a), 1.0, 0.0).astype(BF16)
    state = state_ref[...].reshape(QUAD_ROWS, CHANNELS)
    hidden = picked(state, select) + (
        jnp.concatenate(tiles, axis=1) + picked(eight([shift_ref[...]], CHANNELS), select)[0:1]
    )
    sums = eight(
        [jnp.sum(hidden, axis=0, keepdims=True), jnp.sum(hidden * hidden, axis=0, keepdims=True)],
        256,
    )
    told = picked(sums, holds, NT)[0:4]
    told_ref[...] = jnp.broadcast_to(told[None], told_ref.shape)


def insert_kernel(conv_ref, stats_ref, out_ref):
    sums = jnp.sum(stats_ref[...], axis=0)
    for to in range(4):
        out_ref[to, 0:48] = conv_ref[to]
        out_ref[to, 48:] = eight([sums], LANES)


def assembled(conv_ref, count):
    lane = lax.broadcasted_iota(jnp.int32, (count, LANES), 1)
    tiles = [jnp.zeros((count, LANES), F32) for _ in range(5)]
    for t in range(4):
        rest = conv_ref[t, count : count + count // 2]
        sources = (
            conv_ref[t, 0:count],
            jnp.concatenate([rest, pltpu.roll(rest, 64, 1)], axis=0),
        )
        for part in range(8):
            source, at = divmod(part, 6)
            at *= MEMBERS
            tile, to = divmod(4 * MEMBERS * part + MEMBERS * t, LANES)
            turn = (to - at) % LANES
            block = sources[source]
            if turn:
                block = pltpu.roll(block, turn, 1)
            kept = (lane >= to) & (lane < to + MEMBERS)
            tiles[tile] = jnp.where(kept, block, tiles[tile])
            if to + MEMBERS > LANES:
                kept = lane < to + MEMBERS - LANES
                tiles[tile + 1] = jnp.where(kept, block, tiles[tile + 1])
    return jnp.concatenate(tiles, axis=1)


def hidden_kernel(
    place_ref, conv_ref, state_ref, shift_ref, first_ref, last_ref, hidden_ref, told_ref
):
    state = state_ref[...].reshape(QUAD_ROWS, CHANNELS)
    hidden = state + (assembled(conv_ref, QUAD_ROWS) + shift_ref[...])
    hidden_ref[...] = hidden.reshape(hidden_ref.shape)
    tell_sums_and_edges(hidden, place_ref[0], first_ref[...], last_ref[...], told_ref)


def project(hidden, mean, scale, gain_ref, bias_ref, query_ref, keyvalue_ref):
    normed = ((hidden - mean) * scale * gain_ref[...] + bias_ref[...]).astype(BF16)
    query = dot(normed, query_ref[...]).astype(BF16).astype(F32)
    query = jnp.concatenate(
        [query, jnp.zeros((hidden.shape[0], 3 * LANES - WIDTH), F32)], axis=1
    )
    return query.astype(BF16), dot(normed, keyvalue_ref[...]).astype(BF16)


def project_kernel(
    heard_ref, hidden_ref, gain_ref, bias_ref, query_ref, keyvalue_ref, asked_ref, fresh_ref
):
    mean, scale = spread_sums(heard_sums(heard_ref), group_matrix())
    hidden = hidden_ref[...].reshape(QUAD_ROWS, CHANNELS)
    asked, fresh = project(hidden, mean, scale, gain_ref, bias_ref, query_ref, keyvalue_ref)
    asked_ref[...] = asked
    fresh_ref[...] = fresh


def attend(query, fresh, patch, y, kvs):
    count = query.shape[0]
    lane = lax.broadcasted_iota(jnp.int32, (count, LANES), 1)
    low = lane < HEAD_DIM

    replaced = []
    for kv_ref, step, first in kvs:
        block = lax.broadcasted_iota(jnp.int32, (count, kv_ref.shape[0]), 1) >> 5
        replaced.append(step * block + first == 4 * y + patch)
    if count == ROWS:
        theirs = None
    else:
        theirs = (lax.broadcasted_iota(jnp.int32, (count, count), 1) >> 5) == patch
    tiles = [jnp.zeros((count, LANES), F32) for _ in range(3)]
    for h in range(HEADS):
        at = LANES * (h // 2)
        own = low if h % 2 == 0 else ~low
        asked = jnp.where(own, query[:, at : at + LANES].astype(F32), 0.0).astype(BF16)
        olds = [
            jnp.where(own_patch, -jnp.inf, dot(asked, ref[:, at : at + LANES], NT) * HEAD_DIM ** (-0.5))
            for own_patch, (ref, _, _) in zip(replaced, kvs)
        ]
        new = dot(asked, fresh[:, at : at + LANES], NT) * HEAD_DIM ** (-0.5)
        if theirs is not None:
            new = jnp.where(theirs, new, -jnp.inf)
        peak = functools.reduce(
            jnp.maximum, [jnp.max(e, axis=1, keepdims=True) for e in (*olds, new)]
        )
        olds = [jnp.exp(old - peak) for old in olds]
        new = jnp.exp(new - peak)
        total = sum(jnp.sum(e, axis=1, keepdims=True) for e in (*olds, new))
        at = LANES * ((HEADS + h) // 2)
        summed = sum(
            dot(old.astype(BF16), ref[:, at : at + LANES]) for old, (ref, _, _) in zip(olds, kvs)
        )
        summed += dot(new.astype(BF16), fresh[:, at : at + LANES])
        summed = pltpu.roll(summed / total, HEAD_DIM, 1)
        tiles[h // 2] = jnp.where(own, summed, tiles[h // 2])
    return jnp.concatenate(tiles, axis=1)[:, :WIDTH].astype(BF16)


def attend_quad_kernel(
    place_ref, asked_ref, fresh_ref, hidden_ref, out_ref, same_ref, other_ref, state_ref, told_ref
):
    core = place_ref[1] & 1
    kvs = ((same_ref, 2, core), (other_ref, 2, 1 - core))
    patch = lax.broadcasted_iota(jnp.int32, (QUAD_ROWS, 1), 0) >> 5
    attended = attend(asked_ref[...], fresh_ref[...], patch, place_ref[0], kvs)
    result = hidden_ref[...].reshape(QUAD_ROWS, CHANNELS) + dot(attended, out_ref[...])
    state_ref[...] = result.reshape(state_ref.shape)
    tell_sums(result, group_matrix(), told_ref)


def attend_own_kernel(
    place_ref,
    conv_ref,
    state_ref,
    shift_ref,
    gain_ref,
    bias_ref,
    query_ref,
    keyvalue_ref,
    out_ref,
    kv_ref,
    result_ref,
):
    a = place_ref[1]
    earlier = state_ref[a]
    hidden = earlier + (assembled(conv_ref, ROWS) + shift_ref[...])
    sums = jnp.zeros((8, LANES), F32)
    for t in range(4):
        sums += conv_ref[t, 48:56]
    mean, scale = spread_sums(sums, group_matrix())
    query, fresh = project(hidden, mean, scale, gain_ref, bias_ref, query_ref, keyvalue_ref)
    attended = attend(query, fresh, a, place_ref[0], ((kv_ref, 1, 0),))
    result_ref[0] = earlier
    result_ref[1] = hidden + dot(attended, out_ref[...])


VMEM = pl.BlockSpec(memory_space=pltpu.VMEM)
SMEM = pl.BlockSpec(memory_space=pltpu.SMEM)


def call(kernel, name, out_shapes, args, scalars=0, scratch=(), flops=0):
    return pl.pallas_call(
        kernel,
        name=name,
        out_shape=[jax.ShapeDtypeStruct(s, t) for s, t in out_shapes],
        in_specs=[SMEM] * scalars + [VMEM] * (len(args) - scalars),
        out_specs=[VMEM] * len(out_shapes),
        scratch_shapes=list(scratch),
        cost_estimate=pl.CostEstimate(flops=flops, bytes_accessed=1 << 20, transcendentals=0),
        compiler_params=pltpu.CompilerParams(vmem_limit_bytes=20 << 20),
    )(*args)


def to_all(value, axes):
    return lax.all_to_all(value, axes, 0, 0, tiled=True)


def per_device(
    field,
    stale_conv_in,
    stale_keys,
    stale_values,
    norm1_gain,
    norm1_bias,
    conv_weight,
    conv_bias,
    time_embed,
    norm2_gain,
    norm2_bias,
    w_query,
    w_keyvalue,
    w_out,
):
    quad = (4, ROWS, CHANNELS)
    line = (COLS, CHANNELS)
    stats8 = ((8, 4, LANES), F32)
    told8 = ((8, 6 * COLS, LANES), BF16)
    y = lax.axis_index("y")
    a = 2 * lax.axis_index("zh") + lax.axis_index("core")
    place = jnp.stack([y, a]).astype(jnp.int32)
    row = lambda v: v.reshape(1, CHANNELS)
    swapped = lambda v, axis: lax.ppermute(v, axis, [(0, 1), (1, 0)])

    slices = conv_weight.transpose(0, 1, 3, 2).reshape(9 * MEMBERS, CHANNELS)
    weights = lax.all_gather(slices, "y", axis=0, tiled=False)

    own = field.reshape(ROWS, CHANNELS)
    stale = stale_conv_in.reshape(ROWS, CHANNELS)
    packed, kv = call(
        pack_kernel,
        "pack",
        [((3 * ROWS, CHANNELS), BF16), ((16, ROWS, CHANNELS), BF16)],
        (own, stale, stale_keys, stale_values),
    )
    across = swapped(packed, "zh")
    kv, beside, across, corner = lax.optimization_barrier(
        (
            to_all(kv, ("y", "zh")),
            swapped(packed, "core"),
            across,
            swapped(across, "core"),
        )
    )
    kv = kv.reshape(16 * ROWS, CHANNELS)
    state, prior, told = call(
        unpack_kernel,
        "unpack",
        [(quad, F32), (quad, BF16), told8],
        (place, own, stale, beside, across, corner),
        scalars=1,
    )
    norm1 = (row(norm1_gain), row(norm1_bias))
    norm2 = (row(norm2_gain), row(norm2_bias))
    buffers = [pltpu.VMEM((4, 64, CHANNELS), BF16), pltpu.VMEM((256, 256), F32)]

    told, other = lax.optimization_barrier((to_all(told, "y"), swapped(kv, "core")))
    olds = (kv, other)
    conv, prior, first, last = call(
        conv_quad_kernel,
        "conv0",
        [((4, LANES + 64, LANES), F32), (quad, BF16), (line, BF16), (line, BF16)],
        (place, told, state, prior, weights, *norm1),
        scalars=1,
        scratch=buffers,
        flops=1 << 30,
    )
    hidden, told = call(
        hidden_kernel,
        "hidden0",
        [(quad, F32), told8],
        (place, to_all(conv, QUAD), state, row(conv_bias + time_embed[0]), first, last),
        scalars=1,
        flops=1 << 28,
    )
    heard = to_all(told, "y")
    asked, fresh = call(
        project_kernel,
        "project0",
        [((QUAD_ROWS, 3 * LANES), BF16), ((QUAD_ROWS, CHANNELS), BF16)],
        (heard, hidden, *norm2, w_query, w_keyvalue),
        flops=1 << 28,
    )
    kv = lax.all_gather(fresh, "y", axis=0, tiled=True)
    state, stats = call(
        attend_quad_kernel,
        "attend0",
        [(quad, F32), stats8],
        (place, asked, fresh, hidden, w_out, *olds),
        scalars=1,
        flops=1 << 30,
    )
    shift = row(conv_bias + time_embed[1])
    conv, stats = call(
        conv_own_kernel,
        "conv1",
        [((4, ROWS + ROWS // 2, LANES), F32), stats8],
        (place, to_all(stats, "y"), heard, state, prior, weights, *norm1, shift),
        scalars=1,
        scratch=buffers,
        flops=1 << 30,
    )
    (conv,) = call(
        insert_kernel,
        "insert1",
        [((4, 56, LANES), F32)],
        (conv, to_all(stats, "y")),
        flops=1 << 24,
    )
    (out,) = call(
        attend_own_kernel,
        "attend1",
        [((2, ROWS, CHANNELS), F32)],
        (place, to_all(conv, QUAD), state, shift, *norm2, w_query, w_keyvalue, w_out, kv),
        scalars=1,
        flops=1 << 30,
    )
    return out.reshape(2, 2, COLS, CHANNELS)


def solution(mesh):
    torus = Mesh(
        mesh.devices.reshape(mesh.shape["req"], 8, 2, 2), ("req", "y", "zh", "core")
    )
    placed = (
        P(REQ_PATCH, None, None),
        P(REQ_PATCH, None, None),
        P(REQ_PATCH, None),
        P(REQ_PATCH, None),
        P(),
        P(),
        P(None, None, None, PATCH),
        P(),
        P("req", None),
        P(),
        P(),
        P(),
        P(),
        P(),
    )
    return jax.shard_map(
        per_device,
        mesh=torus,
        in_specs=placed,
        out_specs=P(None, REQ_PATCH, None, None),
        check_vma=False,
    )
```

```python
import functools

import jax
import jax.numpy as jnp
from jax import lax
from jax.experimental import pallas as pl
from jax.experimental.pallas import tpu as pltpu
from jax.sharding import Mesh
from jax.sharding import PartitionSpec as P

GROUPS = 32
HEADS = 5
HEAD_DIM = 64
WIDTH = HEADS * HEAD_DIM
CHANNELS = 640
MEMBERS = CHANNELS // GROUPS
COLS = 16
ROWS = 32
LANES = 128
QUAD_ROWS = 4 * ROWS
POSITIONS = 1024
EPS = 1e-05

Y = ("yh", "yl")
QUAD = ("zh", "core")
REQ_PATCH = ("req", "yh", "yl", "zh", "core")
PATCH = ("yh", "yl", "zh", "core")

F32 = jnp.float32
BF16 = jnp.bfloat16

NN = (((1,), (0,)), ((), ()))
NT = (((1,), (1,)), ((), ()))


def dot(a, b, dims=NN):
    return lax.dot_general(a, b, dims, preferred_element_type=F32)


def thirds(x):
    high = x.astype(BF16)
    rest = x - high.astype(F32)
    middle = rest.astype(BF16)
    low = (rest - middle.astype(F32)).astype(BF16)
    return high, middle, low


def picked(x, zero_one, dims=NN):
    rows = x.shape[0]
    stacked = jnp.concatenate([t.astype(F32) for t in thirds(x)], axis=0).astype(BF16)
    out = dot(stacked, zero_one, dims)
    return out[:rows] + out[rows : 2 * rows] + out[2 * rows :]


def group_matrix():
    channel = lax.broadcasted_iota(jnp.int32, (CHANNELS, LANES), 0)
    first = lax.broadcasted_iota(jnp.int32, (CHANNELS, LANES), 1) * MEMBERS
    return jnp.where((channel >= first) & (channel < first + MEMBERS), 1.0, 0.0).astype(BF16)


def eight(rows, lanes):
    have = sum(r.shape[0] for r in rows)
    return jnp.concatenate([*rows, jnp.zeros((8 - have, lanes), F32)], axis=0)


def tell_sums(x, groups, stats_ref):
    sums = eight(
        [jnp.sum(x, axis=0, keepdims=True), jnp.sum(x * x, axis=0, keepdims=True)], CHANNELS
    )
    told = picked(sums, groups)[0:4]
    stats_ref[...] = jnp.broadcast_to(told[None], stats_ref.shape)


def mean_and_scale(stats_ref, groups):
    return spread_sums(jnp.sum(stats_ref[...], axis=0), groups)


def spread_sums(sums, groups):
    number = POSITIONS * MEMBERS
    mean = sums[0:1] * (1.0 / number)
    variance = sums[1:2] * (1.0 / number) - mean * mean
    spread = picked(eight([mean, lax.rsqrt(variance + EPS)], LANES), groups, NT)
    return spread[0:1], spread[1:2]


def tell_sums_and_edges(x, y, first, last, out_ref):
    sums = eight(
        [jnp.sum(x, axis=0, keepdims=True), jnp.sum(x * x, axis=0, keepdims=True)], CHANNELS
    )
    terms = [t.astype(F32)[0:2] for t in thirds(picked(sums, group_matrix()))]
    told = jnp.concatenate([*terms, jnp.zeros((10, LANES), F32)], axis=0).astype(BF16)
    for to in range(8):
        out_ref[to, 0:COLS] = told
        edge = jnp.where(y + 1 == to, last.astype(F32), first.astype(F32)).astype(BF16)
        for k in range(5):
            out_ref[to, COLS * (k + 1) : COLS * (k + 2)] = edge[:, LANES * k : LANES * (k + 1)]


def heard_sums(heard_ref):
    terms = jnp.sum(heard_ref[:, 0:COLS].astype(F32), axis=0)
    return terms[0:2] + terms[2:4] + terms[4:6]


def heard_edge(heard_ref, sender, exists):
    row = jnp.concatenate(
        [heard_ref[sender, COLS * (k + 1) : COLS * (k + 2)] for k in range(5)], axis=1
    )
    return jnp.where(exists, row.astype(F32), 0.0).astype(BF16)


def heard_edges(heard_ref, y):
    return heard_edge(heard_ref, (y - 1) & 7, y > 0), heard_edge(heard_ref, (y + 1) & 7, y < 7)


def pack_kernel(field_ref, stale_ref, keys_ref, values_ref, packed_ref):
    high, middle, _ = thirds(field_ref[...])
    both = jnp.concatenate(
        [keys_ref[...].astype(F32), values_ref[...].astype(F32)], axis=1
    ).astype(BF16)
    for to in range(4):
        packed_ref[to, 0:ROWS] = high
        packed_ref[to, ROWS : 2 * ROWS] = middle
        packed_ref[to, 2 * ROWS : 3 * ROWS] = stale_ref[...]
        packed_ref[to, 3 * ROWS :] = both


def unpack_kernel(place_ref, packed_ref, field_ref, state_ref, kv_ref, prior_ref, told_ref):
    for t in range(4):
        state_ref[t] = packed_ref[t, 0:ROWS].astype(F32) + packed_ref[t, ROWS : 2 * ROWS].astype(F32)
        prior_ref[t] = packed_ref[t, 2 * ROWS : 3 * ROWS]
        kv_ref[t] = packed_ref[t, 3 * ROWS :]
    state_ref[place_ref[1]] = field_ref[...]
    tell_sums_and_edges(
        state_ref[...].reshape(QUAD_ROWS, CHANNELS),
        place_ref[0],
        prior_ref[0, :COLS],
        prior_ref[3, COLS:],
        told_ref,
    )


def activate(sums, edges, state_ref, prior_ref, vectors_ref, keep, rows):
    mean, scale = spread_sums(sums, group_matrix())
    above, below = edges
    for t in range(4):
        value = (state_ref[t] - mean) * scale * vectors_ref[0:1] + vectors_ref[1:2]
        act = (value * (1.0 / (1.0 + jnp.exp(-value)))).astype(BF16)
        rows[t, COLS : 3 * COLS] = act
        keep(t, act)
        rows[t, 0:COLS] = above if t == 0 else prior_ref[t - 1, COLS:]
        rows[t, 3 * COLS :] = below if t == 3 else prior_ref[t + 1, :COLS]


def convolve(rows, weight_ref, wide):
    window = rows[...].reshape(4 * 64, CHANNELS)
    wide[...] = jnp.zeros(wide.shape, F32)
    col = lax.broadcasted_iota(jnp.int32, (LANES, LANES), 0) & (COLS - 1)
    lane = lax.broadcasted_iota(jnp.int32, (LANES, LANES), 1)
    tiles = [jnp.zeros((LANES, LANES), F32), jnp.zeros((LANES, LANES), F32)]
    for part in range(8):
        wide[:, 0 : 9 * MEMBERS] = dot(window, weight_ref[part], NT)
        whole = wide[...].reshape(4, 64, 256)
        lines = [
            whole[:, COLS * r : COLS * r + 2 * COLS].reshape(LANES, 256) for r in range(3)
        ]
        total = (
            lines[0][:, :LANES]
            + pltpu.roll(lines[1][:, :LANES], LANES - 3 * MEMBERS, 1)
            + pltpu.roll(lines[2], 256 - 6 * MEMBERS, 1)[:, :LANES]
        )
        left = jnp.where(col > 0, pltpu.roll(total, 1, 0), 0.0)
        centre = pltpu.roll(total, LANES - MEMBERS, 1)
        right = pltpu.roll(total, LANES - 2 * MEMBERS, 1)
        right = jnp.where(col < COLS - 1, pltpu.roll(right, LANES - 1, 0), 0.0)
        made = left + centre + right
        tile, at = divmod(part, 6)
        at *= MEMBERS
        if at:
            made = pltpu.roll(made, at, 1)
        kept = (lane >= at) & (lane < at + MEMBERS)
        tiles[tile] = jnp.where(kept, made, tiles[tile])
    return tiles


def folded(tile):
    half = tile.shape[0] // 2
    lane = lax.broadcasted_iota(jnp.int32, (half, LANES), 1)
    return jnp.where(lane < 64, tile[:half], pltpu.roll(tile[half:], 64, 1))


def conv_quad_kernel(
    place_ref,
    heard_ref,
    state_ref,
    prior_ref,
    weight_ref,
    vectors_ref,
    out_ref,
    act_ref,
    first_ref,
    last_ref,
    rows,
    wide,
):
    def keep(t, act):
        act_ref[t] = act
        if t == 0:
            first_ref[...] = act[:COLS]
        if t == 3:
            last_ref[...] = act[COLS:]

    edges = heard_edges(heard_ref, place_ref[0])
    activate(heard_sums(heard_ref), edges, state_ref, prior_ref, vectors_ref, keep, rows)
    tiles = convolve(rows, weight_ref, wide)
    rest = folded(tiles[1])
    for to in range(4):
        out_ref[to, 0:LANES] = tiles[0]
        out_ref[to, LANES:] = rest


def shard_lanes(shape, dim):
    lane = lax.broadcasted_iota(jnp.int32, shape, dim)
    inner = lane & (LANES - 1)
    part = (inner * 3277) >> 16
    within = inner - MEMBERS * part
    second = lane >= LANES
    used = part < jnp.where(second, 2, 6)
    return part + jnp.where(second, 6, 0), within, used


def conv_own_kernel(
    place_ref,
    stats_ref,
    heard_ref,
    state_ref,
    prior_ref,
    weight_ref,
    vectors_ref,
    out_ref,
    told_ref,
    rows,
    wide,
):
    a = place_ref[1]
    activate(
        jnp.sum(stats_ref[...], axis=0),
        heard_edges(heard_ref, place_ref[0]),
        state_ref,
        prior_ref,
        vectors_ref,
        lambda t, act: None,
        rows,
    )
    tiles = convolve(rows, weight_ref, wide)
    for t in range(4):
        mine = slice(t * ROWS, (t + 1) * ROWS)
        out_ref[t, 0:ROWS] = tiles[0][mine]
        out_ref[t, ROWS:] = folded(tiles[1][mine])
    part, within, used = shard_lanes((CHANNELS, 256), 1)
    channel = lax.broadcasted_iota(jnp.int32, (CHANNELS, 256), 0)
    select = used & (channel == 4 * MEMBERS * part + MEMBERS * a + within)
    select = jnp.where(select, 1.0, 0.0).astype(BF16)
    part, _, used = shard_lanes((LANES, 256), 1)
    group = lax.broadcasted_iota(jnp.int32, (LANES, 256), 0)
    holds = jnp.where(used & (group == 4 * part + a), 1.0, 0.0).astype(BF16)
    state = state_ref[...].reshape(QUAD_ROWS, CHANNELS)
    hidden = picked(state, select) + (
        jnp.concatenate(tiles, axis=1) + picked(eight([vectors_ref[5:6]], CHANNELS), select)[0:1]
    )
    sums = eight(
        [jnp.sum(hidden, axis=0, keepdims=True), jnp.sum(hidden * hidden, axis=0, keepdims=True)],
        256,
    )
    told = picked(sums, holds, NT)[0:4]
    told_ref[...] = jnp.broadcast_to(told[None], told_ref.shape)


def insert_kernel(conv_ref, stats_ref, out_ref):
    sums = jnp.sum(stats_ref[...], axis=0)
    for to in range(4):
        out_ref[to, 0:48] = conv_ref[to]
        out_ref[to, 48:] = eight([sums], LANES)


def assembled(conv_ref, count):
    lane = lax.broadcasted_iota(jnp.int32, (count, LANES), 1)
    tiles = [jnp.zeros((count, LANES), F32) for _ in range(5)]
    for t in range(4):
        rest = conv_ref[t, count : count + count // 2]
        sources = (
            conv_ref[t, 0:count],
            jnp.concatenate([rest, pltpu.roll(rest, 64, 1)], axis=0),
        )
        for part in range(8):
            source, at = divmod(part, 6)
            at *= MEMBERS
            tile, to = divmod(4 * MEMBERS * part + MEMBERS * t, LANES)
            turn = (to - at) % LANES
            block = sources[source]
            if turn:
                block = pltpu.roll(block, turn, 1)
            kept = (lane >= to) & (lane < to + MEMBERS)
            tiles[tile] = jnp.where(kept, block, tiles[tile])
            if to + MEMBERS > LANES:
                kept = lane < to + MEMBERS - LANES
                tiles[tile + 1] = jnp.where(kept, block, tiles[tile + 1])
    return jnp.concatenate(tiles, axis=1)


def hidden_kernel(
    place_ref, conv_ref, state_ref, vectors_ref, first_ref, last_ref, hidden_ref, told_ref
):
    state = state_ref[...].reshape(QUAD_ROWS, CHANNELS)
    hidden = state + (assembled(conv_ref, QUAD_ROWS) + vectors_ref[4:5])
    hidden_ref[...] = hidden.reshape(hidden_ref.shape)
    tell_sums_and_edges(hidden, place_ref[0], first_ref[...], last_ref[...], told_ref)


def project(hidden, mean, scale, vectors_ref, query_ref, keyvalue_ref):
    normed = ((hidden - mean) * scale * vectors_ref[2:3] + vectors_ref[3:4]).astype(BF16)
    query = dot(normed, query_ref[...]).astype(BF16)
    return query, dot(normed, keyvalue_ref[...]).astype(BF16)


def project_kernel(
    heard_ref, hidden_ref, vectors_ref, query_ref, keyvalue_ref, asked_ref, fresh_ref
):
    mean, scale = spread_sums(heard_sums(heard_ref), group_matrix())
    hidden = hidden_ref[...].reshape(QUAD_ROWS, CHANNELS)
    asked, fresh = project(hidden, mean, scale, vectors_ref, query_ref, keyvalue_ref)
    asked_ref[...] = asked
    fresh_ref[...] = fresh


def attend(query, fresh, patch, y, kv_ref, turned):
    count = query.shape[0]
    lane = lax.broadcasted_iota(jnp.int32, (count, LANES), 1)
    low = lane < HEAD_DIM

    block = lax.broadcasted_iota(jnp.int32, (count, POSITIONS), 1) >> 5
    replaced = (block ^ turned) == 4 * y + patch
    if count == ROWS:
        theirs = None
    else:
        theirs = (lax.broadcasted_iota(jnp.int32, (count, count), 1) >> 5) == patch
    tiles = [jnp.zeros((count, LANES), F32) for _ in range(3)]
    for h in range(HEADS):
        at = LANES * (h // 2)
        own = low if h % 2 == 0 else ~low
        asked = jnp.where(own, query[:, at : at + LANES].astype(F32), 0.0).astype(BF16)
        old = dot(asked, kv_ref[:, at : at + LANES], NT) * HEAD_DIM ** (-0.5)
        old = jnp.where(replaced, -jnp.inf, old)
        new = dot(asked, fresh[:, at : at + LANES], NT) * HEAD_DIM ** (-0.5)
        if theirs is not None:
            new = jnp.where(theirs, new, -jnp.inf)
        peak = jnp.maximum(
            jnp.max(old, axis=1, keepdims=True), jnp.max(new, axis=1, keepdims=True)
        )
        old = jnp.exp(old - peak)
        new = jnp.exp(new - peak)
        total = jnp.sum(old, axis=1, keepdims=True) + jnp.sum(new, axis=1, keepdims=True)
        at = LANES * ((HEADS + h) // 2)
        summed = dot(old.astype(BF16), kv_ref[:, at : at + LANES])
        summed += dot(new.astype(BF16), fresh[:, at : at + LANES])
        summed = pltpu.roll(summed / total, HEAD_DIM, 1)
        tiles[h // 2] = jnp.where(own, summed, tiles[h // 2])
    return jnp.concatenate(tiles, axis=1)[:, :WIDTH].astype(BF16)


def attend_quad_kernel(
    place_ref, asked_ref, fresh_ref, hidden_ref, out_ref, kv_ref, state_ref, told_ref
):
    turned = 4 * (place_ref[0] & 1)
    patch = lax.broadcasted_iota(jnp.int32, (QUAD_ROWS, 1), 0) >> 5
    attended = attend(asked_ref[...], fresh_ref[...], patch, place_ref[0], kv_ref, turned)
    result = hidden_ref[...].reshape(QUAD_ROWS, CHANNELS) + dot(attended, out_ref[...])
    state_ref[...] = result.reshape(state_ref.shape)
    tell_sums(result, group_matrix(), told_ref)


def attend_own_kernel(
    place_ref,
    conv_ref,
    state_ref,
    vectors_ref,
    query_ref,
    keyvalue_ref,
    out_ref,
    kv_ref,
    result_ref,
):
    a = place_ref[1]
    earlier = state_ref[a]
    hidden = earlier + (assembled(conv_ref, ROWS) + vectors_ref[5:6])
    sums = jnp.zeros((8, LANES), F32)
    for t in range(4):
        sums += conv_ref[t, 48:56]
    mean, scale = spread_sums(sums, group_matrix())
    query, fresh = project(hidden, mean, scale, vectors_ref, query_ref, keyvalue_ref)
    attended = attend(query, fresh, a, place_ref[0], kv_ref, 0)
    result_ref[0] = earlier
    result_ref[1] = hidden + dot(attended, out_ref[...])


VMEM = pl.BlockSpec(memory_space=pltpu.VMEM)
SMEM = pl.BlockSpec(memory_space=pltpu.SMEM)


def call(kernel, name, out_shapes, args, scalars=0, scratch=(), flops=0):
    return pl.pallas_call(
        kernel,
        name=name,
        out_shape=[jax.ShapeDtypeStruct(s, t) for s, t in out_shapes],
        in_specs=[SMEM] * scalars + [VMEM] * (len(args) - scalars),
        out_specs=[VMEM] * len(out_shapes),
        scratch_shapes=list(scratch),
        cost_estimate=pl.CostEstimate(flops=flops, bytes_accessed=1 << 20, transcendentals=0),
        compiler_params=pltpu.CompilerParams(vmem_limit_bytes=20 << 20),
    )(*args)


def to_all(value, axes):
    return lax.all_to_all(value, axes, 0, 0, tiled=True)


def per_device(
    field,
    stale_conv_in,
    stale_keys,
    stale_values,
    norm1_gain,
    norm1_bias,
    conv_weight,
    conv_bias,
    time_embed,
    norm2_gain,
    norm2_bias,
    w_query,
    w_keyvalue,
    w_out,
):
    quad = (4, ROWS, CHANNELS)
    line = (COLS, CHANNELS)
    stats8 = ((8, 4, LANES), F32)
    told8 = ((8, 6 * COLS, LANES), BF16)
    y = 2 * lax.axis_index("yh") + lax.axis_index("yl")
    a = 2 * lax.axis_index("zh") + lax.axis_index("core")
    place = jnp.stack([y, a]).astype(jnp.int32)

    slices = conv_weight.transpose(0, 1, 3, 2).reshape(9 * MEMBERS, CHANNELS)
    weights = lax.all_gather(slices, Y, axis=0, tiled=False)

    own = field.reshape(ROWS, CHANNELS)
    (packed,) = call(
        pack_kernel,
        "pack",
        [((4, 4 * ROWS, CHANNELS), BF16)],
        (own, stale_conv_in.reshape(ROWS, CHANNELS), stale_keys, stale_values),
    )
    vectors = jnp.stack(
        [
            norm1_gain,
            norm1_bias,
            norm2_gain,
            norm2_bias,
            conv_bias + time_embed[0],
            conv_bias + time_embed[1],
            jnp.zeros_like(conv_bias),
            jnp.zeros_like(conv_bias),
        ]
    )
    w_query = jnp.pad(w_query, ((0, 0), (0, 3 * LANES - WIDTH)))
    packed, vectors, w_query, place = lax.optimization_barrier(
        (to_all(packed, QUAD), vectors, w_query, place)
    )
    state, kv, prior, told = call(
        unpack_kernel,
        "unpack",
        [(quad, F32), (quad, BF16), (quad, BF16), told8],
        (place, packed, own),
        scalars=1,
    )
    kv = kv.reshape(QUAD_ROWS, CHANNELS)
    told, partner = lax.optimization_barrier(
        (to_all(told, Y), lax.ppermute(kv, "yl", [(0, 1), (1, 0)]))
    )
    pair = jnp.concatenate([kv, partner], axis=0)
    old = lax.all_gather(pair, "yh", axis=0, tiled=True)
    buffers = [pltpu.VMEM((4, 64, CHANNELS), BF16), pltpu.VMEM((256, 256), F32)]

    conv, prior, first, last = call(
        conv_quad_kernel,
        "conv0",
        [((4, LANES + 64, LANES), F32), (quad, BF16), (line, BF16), (line, BF16)],
        (place, told, state, prior, weights, vectors),
        scalars=1,
        scratch=buffers,
        flops=1 << 30,
    )
    hidden, told = call(
        hidden_kernel,
        "hidden0",
        [(quad, F32), told8],
        (place, to_all(conv, QUAD), state, vectors, first, last),
        scalars=1,
        flops=1 << 28,
    )
    heard = to_all(told, Y)
    asked, fresh = call(
        project_kernel,
        "project0",
        [((QUAD_ROWS, 3 * LANES), BF16), ((QUAD_ROWS, CHANNELS), BF16)],
        (heard, hidden, vectors, w_query, w_keyvalue),
        flops=1 << 28,
    )
    kv = lax.all_gather(fresh, Y, axis=0, tiled=True)
    state, stats = call(
        attend_quad_kernel,
        "attend0",
        [(quad, F32), stats8],
        (place, asked, fresh, hidden, w_out, old),
        scalars=1,
        flops=1 << 30,
    )
    conv, stats = call(
        conv_own_kernel,
        "conv1",
        [((4, ROWS + ROWS // 2, LANES), F32), stats8],
        (place, to_all(stats, Y), heard, state, prior, weights, vectors),
        scalars=1,
        scratch=buffers,
        flops=1 << 30,
    )
    (conv,) = call(
        insert_kernel,
        "insert1",
        [((4, 56, LANES), F32)],
        (conv, to_all(stats, Y)),
        flops=1 << 24,
    )
    (out,) = call(
        attend_own_kernel,
        "attend1",
        [((2, ROWS, CHANNELS), F32)],
        (place, to_all(conv, QUAD), state, vectors, w_query, w_keyvalue, w_out, kv),
        scalars=1,
        flops=1 << 30,
    )
    return out.reshape(2, 2, COLS, CHANNELS)


def solution(mesh):
    torus = Mesh(
        mesh.devices.reshape(mesh.shape["req"], 4, 2, 2, 2), REQ_PATCH
    )
    placed = (
        P(REQ_PATCH, None, None),
        P(REQ_PATCH, None, None),
        P(REQ_PATCH, None),
        P(REQ_PATCH, None),
        P(),
        P(),
        P(None, None, None, PATCH),
        P(),
        P("req", None),
        P(),
        P(),
        P(),
        P(),
        P(),
    )
    return jax.shard_map(
        per_device,
        mesh=torus,
        in_specs=placed,
        out_specs=P(None, REQ_PATCH, None, None),
        check_vma=False,
    )
```

```python
import functools

import jax
import jax.numpy as jnp
from jax import lax
from jax.experimental import pallas as pl
from jax.experimental.pallas import tpu as pltpu
from jax.sharding import Mesh
from jax.sharding import PartitionSpec as P

GROUPS = 32
HEADS = 5
HEAD_DIM = 64
WIDTH = HEADS * HEAD_DIM
CHANNELS = 640
MEMBERS = CHANNELS // GROUPS
COLS = 16
ROWS = 32
LANES = 128
QUAD_ROWS = 4 * ROWS
POSITIONS = 1024
EPS = 1e-05

Y = ("yh", "yl")
QUAD = ("zh", "core")
REQ_PATCH = ("req", "yh", "yl", "zh", "core")
PATCH = ("yh", "yl", "zh", "core")

F32 = jnp.float32
BF16 = jnp.bfloat16

NN = (((1,), (0,)), ((), ()))
NT = (((1,), (1,)), ((), ()))


def dot(a, b, dims=NN):
    return lax.dot_general(a, b, dims, preferred_element_type=F32)


def thirds(x):
    high = x.astype(BF16)
    rest = x - high.astype(F32)
    middle = rest.astype(BF16)
    low = (rest - middle.astype(F32)).astype(BF16)
    return high, middle, low


def picked(x, zero_one, dims=NN):
    rows = x.shape[0]
    stacked = jnp.concatenate([t.astype(F32) for t in thirds(x)], axis=0).astype(BF16)
    out = dot(stacked, zero_one, dims)
    return out[:rows] + out[rows : 2 * rows] + out[2 * rows :]


def group_matrix():
    channel = lax.broadcasted_iota(jnp.int32, (CHANNELS, LANES), 0)
    first = lax.broadcasted_iota(jnp.int32, (CHANNELS, LANES), 1) * MEMBERS
    return jnp.where((channel >= first) & (channel < first + MEMBERS), 1.0, 0.0).astype(BF16)


def eight(rows, lanes):
    have = sum(r.shape[0] for r in rows)
    return jnp.concatenate([*rows, jnp.zeros((8 - have, lanes), F32)], axis=0)


def tell_sums(x, groups, stats_ref):
    sums = eight(
        [jnp.sum(x, axis=0, keepdims=True), jnp.sum(x * x, axis=0, keepdims=True)], CHANNELS
    )
    told = picked(sums, groups)[0:4]
    stats_ref[...] = jnp.broadcast_to(told[None], stats_ref.shape)


def mean_and_scale(stats_ref, groups):
    return spread_sums(jnp.sum(stats_ref[...], axis=0), groups)


def spread_sums(sums, groups):
    number = POSITIONS * MEMBERS
    mean = sums[0:1] * (1.0 / number)
    variance = sums[1:2] * (1.0 / number) - mean * mean
    spread = picked(eight([mean, lax.rsqrt(variance + EPS)], LANES), groups, NT)
    return spread[0:1], spread[1:2]


def tell_sums_and_edges(x, y, first, last, out_ref):
    sums = eight(
        [jnp.sum(x, axis=0, keepdims=True), jnp.sum(x * x, axis=0, keepdims=True)], CHANNELS
    )
    terms = [t.astype(F32)[0:2] for t in thirds(picked(sums, group_matrix()))]
    told = jnp.concatenate([*terms, jnp.zeros((10, LANES), F32)], axis=0).astype(BF16)
    for to in range(8):
        out_ref[to, 0:COLS] = told
        edge = jnp.where(y + 1 == to, last.astype(F32), first.astype(F32)).astype(BF16)
        for k in range(5):
            out_ref[to, COLS * (k + 1) : COLS * (k + 2)] = edge[:, LANES * k : LANES * (k + 1)]


def heard_sums(heard_ref):
    terms = jnp.sum(heard_ref[:, 0:COLS].astype(F32), axis=0)
    return terms[0:2] + terms[2:4] + terms[4:6]


def heard_edge(heard_ref, sender, exists):
    row = jnp.concatenate(
        [heard_ref[sender, COLS * (k + 1) : COLS * (k + 2)] for k in range(5)], axis=1
    )
    return jnp.where(exists, row.astype(F32), 0.0).astype(BF16)


def heard_edges(heard_ref, y):
    return heard_edge(heard_ref, (y - 1) & 7, y > 0), heard_edge(heard_ref, (y + 1) & 7, y < 7)


def pack_kernel(field_ref, stale_ref, keys_ref, values_ref, packed_ref):
    high, middle, _ = thirds(field_ref[...])
    both = jnp.concatenate(
        [keys_ref[...].astype(F32), values_ref[...].astype(F32)], axis=1
    ).astype(BF16)
    for to in range(4):
        packed_ref[to, 0:ROWS] = high
        packed_ref[to, ROWS : 2 * ROWS] = middle
        packed_ref[to, 2 * ROWS : 3 * ROWS] = stale_ref[...]
        packed_ref[to, 3 * ROWS :] = both


def unpack_kernel(place_ref, packed_ref, field_ref, state_ref, kv_ref, prior_ref, told_ref):
    for t in range(4):
        state_ref[t] = packed_ref[t, 0:ROWS].astype(F32) + packed_ref[t, ROWS : 2 * ROWS].astype(F32)
        prior_ref[t] = packed_ref[t, 2 * ROWS : 3 * ROWS]
        kv_ref[t] = packed_ref[t, 3 * ROWS :]
    state_ref[place_ref[1]] = field_ref[...]
    tell_sums_and_edges(
        state_ref[...].reshape(QUAD_ROWS, CHANNELS),
        place_ref[0],
        prior_ref[0, :COLS],
        prior_ref[3, COLS:],
        told_ref,
    )


def activate(sums, edges, state_ref, prior_ref, vectors_ref, keep, rows):
    mean, scale = spread_sums(sums, group_matrix())
    above, below = edges
    for t in range(4):
        value = (state_ref[t] - mean) * scale * vectors_ref[0:1] + vectors_ref[1:2]
        act = (value * (1.0 / (1.0 + jnp.exp(-value)))).astype(BF16)
        rows[t, COLS : 3 * COLS] = act
        keep(t, act)
        rows[t, 0:COLS] = above if t == 0 else prior_ref[t - 1, COLS:]
        rows[t, 3 * COLS :] = below if t == 3 else prior_ref[t + 1, :COLS]


def convolve(rows, weight_ref, wide):
    window = rows[...].reshape(4 * 64, CHANNELS)
    wide[...] = jnp.zeros(wide.shape, F32)
    col = lax.broadcasted_iota(jnp.int32, (LANES, LANES), 0) & (COLS - 1)
    lane = lax.broadcasted_iota(jnp.int32, (LANES, LANES), 1)
    tiles = [jnp.zeros((LANES, LANES), F32), jnp.zeros((LANES, LANES), F32)]
    for part in range(8):
        wide[:, 0 : 9 * MEMBERS] = dot(window, weight_ref[part], NT)
        whole = wide[...].reshape(4, 64, 256)
        lines = [
            whole[:, COLS * r : COLS * r + 2 * COLS].reshape(LANES, 256) for r in range(3)
        ]
        total = (
            lines[0][:, :LANES]
            + pltpu.roll(lines[1][:, :LANES], LANES - 3 * MEMBERS, 1)
            + pltpu.roll(lines[2], 256 - 6 * MEMBERS, 1)[:, :LANES]
        )
        left = jnp.where(col > 0, pltpu.roll(total, 1, 0), 0.0)
        centre = pltpu.roll(total, LANES - MEMBERS, 1)
        right = pltpu.roll(total, LANES - 2 * MEMBERS, 1)
        right = jnp.where(col < COLS - 1, pltpu.roll(right, LANES - 1, 0), 0.0)
        made = left + centre + right
        tile, at = divmod(part, 6)
        at *= MEMBERS
        if at:
            made = pltpu.roll(made, at, 1)
        kept = (lane >= at) & (lane < at + MEMBERS)
        tiles[tile] = jnp.where(kept, made, tiles[tile])
    return tiles


def folded(tile):
    half = tile.shape[0] // 2
    lane = lax.broadcasted_iota(jnp.int32, (half, LANES), 1)
    return jnp.where(lane < 64, tile[:half], pltpu.roll(tile[half:], 64, 1))


def conv_quad_kernel(
    place_ref,
    heard_ref,
    state_ref,
    prior_ref,
    weight_ref,
    vectors_ref,
    out_ref,
    act_ref,
    first_ref,
    last_ref,
    rows,
    wide,
):
    def keep(t, act):
        act_ref[t] = act
        if t == 0:
            first_ref[...] = act[:COLS]
        if t == 3:
            last_ref[...] = act[COLS:]

    edges = heard_edges(heard_ref, place_ref[0])
    activate(heard_sums(heard_ref), edges, state_ref, prior_ref, vectors_ref, keep, rows)
    tiles = convolve(rows, weight_ref, wide)
    rest = folded(tiles[1])
    for to in range(4):
        out_ref[to, 0:LANES] = tiles[0]
        out_ref[to, LANES:] = rest


def shard_lanes(shape, dim):
    lane = lax.broadcasted_iota(jnp.int32, shape, dim)
    inner = lane & (LANES - 1)
    part = (inner * 3277) >> 16
    within = inner - MEMBERS * part
    second = lane >= LANES
    used = part < jnp.where(second, 2, 6)
    return part + jnp.where(second, 6, 0), within, used


def conv_own_kernel(
    place_ref,
    stats_ref,
    above_ref,
    below_ref,
    state_ref,
    prior_ref,
    weight_ref,
    vectors_ref,
    out_ref,
    told_ref,
    rows,
    wide,
):
    a = place_ref[1]
    activate(
        jnp.sum(stats_ref[...], axis=0),
        (above_ref[...], below_ref[...]),
        state_ref,
        prior_ref,
        vectors_ref,
        lambda t, act: None,
        rows,
    )
    tiles = convolve(rows, weight_ref, wide)
    for t in range(4):
        mine = slice(t * ROWS, (t + 1) * ROWS)
        out_ref[t, 0:ROWS] = tiles[0][mine]
        out_ref[t, ROWS:] = folded(tiles[1][mine])
    part, within, used = shard_lanes((CHANNELS, 256), 1)
    channel = lax.broadcasted_iota(jnp.int32, (CHANNELS, 256), 0)
    select = used & (channel == 4 * MEMBERS * part + MEMBERS * a + within)
    select = jnp.where(select, 1.0, 0.0).astype(BF16)
    part, _, used = shard_lanes((LANES, 256), 1)
    group = lax.broadcasted_iota(jnp.int32, (LANES, 256), 0)
    holds = jnp.where(used & (group == 4 * part + a), 1.0, 0.0).astype(BF16)
    state = state_ref[...].reshape(QUAD_ROWS, CHANNELS)
    hidden = picked(state, select) + (
        jnp.concatenate(tiles, axis=1) + picked(eight([vectors_ref[5:6]], CHANNELS), select)[0:1]
    )
    sums = eight(
        [jnp.sum(hidden, axis=0, keepdims=True), jnp.sum(hidden * hidden, axis=0, keepdims=True)],
        256,
    )
    told = picked(sums, holds, NT)[0:4]
    told_ref[...] = jnp.broadcast_to(told[None], told_ref.shape)


def insert_kernel(conv_ref, stats_ref, out_ref):
    sums = jnp.sum(stats_ref[...], axis=0)
    for to in range(4):
        out_ref[to, 0:48] = conv_ref[to]
        out_ref[to, 48:] = eight([sums], LANES)


def assembled(conv_ref, count):
    lane = lax.broadcasted_iota(jnp.int32, (count, LANES), 1)
    tiles = [jnp.zeros((count, LANES), F32) for _ in range(5)]
    for t in range(4):
        rest = conv_ref[t, count : count + count // 2]
        sources = (
            conv_ref[t, 0:count],
            jnp.concatenate([rest, pltpu.roll(rest, 64, 1)], axis=0),
        )
        for part in range(8):
            source, at = divmod(part, 6)
            at *= MEMBERS
            tile, to = divmod(4 * MEMBERS * part + MEMBERS * t, LANES)
            turn = (to - at) % LANES
            block = sources[source]
            if turn:
                block = pltpu.roll(block, turn, 1)
            kept = (lane >= to) & (lane < to + MEMBERS)
            tiles[tile] = jnp.where(kept, block, tiles[tile])
            if to + MEMBERS > LANES:
                kept = lane < to + MEMBERS - LANES
                tiles[tile + 1] = jnp.where(kept, block, tiles[tile + 1])
    return jnp.concatenate(tiles, axis=1)


def hidden_kernel(conv_ref, state_ref, vectors_ref, hidden_ref, stats_ref):
    state = state_ref[...].reshape(QUAD_ROWS, CHANNELS)
    hidden = state + (assembled(conv_ref, QUAD_ROWS) + vectors_ref[4:5])
    hidden_ref[...] = hidden.reshape(hidden_ref.shape)
    tell_sums(hidden, group_matrix(), stats_ref)


def project(hidden, mean, scale, vectors_ref, query_ref, keyvalue_ref):
    normed = ((hidden - mean) * scale * vectors_ref[2:3] + vectors_ref[3:4]).astype(BF16)
    query = dot(normed, query_ref[...]).astype(BF16)
    return query, dot(normed, keyvalue_ref[...]).astype(BF16)


def project_kernel(
    stats_ref, hidden_ref, vectors_ref, query_ref, keyvalue_ref, asked_ref, fresh_ref
):
    mean, scale = mean_and_scale(stats_ref, group_matrix())
    hidden = hidden_ref[...].reshape(QUAD_ROWS, CHANNELS)
    asked, fresh = project(hidden, mean, scale, vectors_ref, query_ref, keyvalue_ref)
    asked_ref[...] = asked
    fresh_ref[...] = fresh


def attend(query, fresh, patch, y, kv_ref):
    count = query.shape[0]
    lane = lax.broadcasted_iota(jnp.int32, (count, LANES), 1)
    low = lane < HEAD_DIM

    block = lax.broadcasted_iota(jnp.int32, (count, POSITIONS), 1) >> 5
    replaced = block == 4 * y + patch
    if count == ROWS:
        theirs = None
    else:
        theirs = (lax.broadcasted_iota(jnp.int32, (count, count), 1) >> 5) == patch
    tiles = [jnp.zeros((count, LANES), F32) for _ in range(3)]
    for h in range(HEADS):
        at = LANES * (h // 2)
        own = low if h % 2 == 0 else ~low
        asked = jnp.where(own, query[:, at : at + LANES].astype(F32), 0.0).astype(BF16)
        old = dot(asked, kv_ref[:, at : at + LANES], NT) * HEAD_DIM ** (-0.5)
        old = jnp.where(replaced, -jnp.inf, old)
        new = dot(asked, fresh[:, at : at + LANES], NT) * HEAD_DIM ** (-0.5)
        if theirs is not None:
            new = jnp.where(theirs, new, -jnp.inf)
        peak = jnp.maximum(
            jnp.max(old, axis=1, keepdims=True), jnp.max(new, axis=1, keepdims=True)
        )
        old = jnp.exp(old - peak)
        new = jnp.exp(new - peak)
        total = jnp.sum(old, axis=1, keepdims=True) + jnp.sum(new, axis=1, keepdims=True)
        at = LANES * ((HEADS + h) // 2)
        summed = dot(old.astype(BF16), kv_ref[:, at : at + LANES])
        summed += dot(new.astype(BF16), fresh[:, at : at + LANES])
        summed = pltpu.roll(summed / total, HEAD_DIM, 1)
        tiles[h // 2] = jnp.where(own, summed, tiles[h // 2])
    return jnp.concatenate(tiles, axis=1)[:, :WIDTH].astype(BF16)


def attend_quad_kernel(
    place_ref, asked_ref, fresh_ref, hidden_ref, out_ref, kv_ref, state_ref, told_ref
):
    patch = lax.broadcasted_iota(jnp.int32, (QUAD_ROWS, 1), 0) >> 5
    attended = attend(asked_ref[...], fresh_ref[...], patch, place_ref[0], kv_ref)
    result = hidden_ref[...].reshape(QUAD_ROWS, CHANNELS) + dot(attended, out_ref[...])
    state_ref[...] = result.reshape(state_ref.shape)
    tell_sums(result, group_matrix(), told_ref)


def attend_own_kernel(
    place_ref,
    conv_ref,
    state_ref,
    vectors_ref,
    query_ref,
    keyvalue_ref,
    out_ref,
    kv_ref,
    result_ref,
):
    a = place_ref[1]
    earlier = state_ref[a]
    hidden = earlier + (assembled(conv_ref, ROWS) + vectors_ref[5:6])
    sums = jnp.zeros((8, LANES), F32)
    for t in range(4):
        sums += conv_ref[t, 48:56]
    mean, scale = spread_sums(sums, group_matrix())
    query, fresh = project(hidden, mean, scale, vectors_ref, query_ref, keyvalue_ref)
    attended = attend(query, fresh, a, place_ref[0], kv_ref)
    result_ref[0] = earlier
    result_ref[1] = hidden + dot(attended, out_ref[...])


VMEM = pl.BlockSpec(memory_space=pltpu.VMEM)
SMEM = pl.BlockSpec(memory_space=pltpu.SMEM)


def call(kernel, name, out_shapes, args, scalars=0, scratch=(), flops=0):
    return pl.pallas_call(
        kernel,
        name=name,
        out_shape=[jax.ShapeDtypeStruct(s, t) for s, t in out_shapes],
        in_specs=[SMEM] * scalars + [VMEM] * (len(args) - scalars),
        out_specs=[VMEM] * len(out_shapes),
        scratch_shapes=list(scratch),
        cost_estimate=pl.CostEstimate(flops=flops, bytes_accessed=1 << 20, transcendentals=0),
        compiler_params=pltpu.CompilerParams(vmem_limit_bytes=20 << 20),
    )(*args)


def to_all(value, axes):
    return lax.all_to_all(value, axes, 0, 0, tiled=True)


def per_device(
    field,
    stale_conv_in,
    stale_keys,
    stale_values,
    norm1_gain,
    norm1_bias,
    conv_weight,
    conv_bias,
    time_embed,
    norm2_gain,
    norm2_bias,
    w_query,
    w_keyvalue,
    w_out,
):
    quad = (4, ROWS, CHANNELS)
    line = (COLS, CHANNELS)
    stats8 = ((8, 4, LANES), F32)
    told8 = ((8, 6 * COLS, LANES), BF16)
    y = 2 * lax.axis_index("yh") + lax.axis_index("yl")
    a = 2 * lax.axis_index("zh") + lax.axis_index("core")
    place = jnp.stack([y, a]).astype(jnp.int32)

    slices = conv_weight.transpose(0, 1, 3, 2).reshape(9 * MEMBERS, CHANNELS)
    weights = lax.all_gather(slices, Y, axis=0, tiled=False)

    own = field.reshape(ROWS, CHANNELS)
    (packed,) = call(
        pack_kernel,
        "pack",
        [((4, 4 * ROWS, CHANNELS), BF16)],
        (own, stale_conv_in.reshape(ROWS, CHANNELS), stale_keys, stale_values),
    )
    vectors = jnp.stack(
        [
            norm1_gain,
            norm1_bias,
            norm2_gain,
            norm2_bias,
            conv_bias + time_embed[0],
            conv_bias + time_embed[1],
            jnp.zeros_like(conv_bias),
            jnp.zeros_like(conv_bias),
        ]
    )
    w_query = jnp.pad(w_query, ((0, 0), (0, 3 * LANES - WIDTH)))
    packed, vectors, w_query, place = lax.optimization_barrier(
        (to_all(packed, QUAD), vectors, w_query, place)
    )
    state, kv, prior, told = call(
        unpack_kernel,
        "unpack",
        [(quad, F32), (quad, BF16), (quad, BF16), told8],
        (place, packed, own),
        scalars=1,
    )
    kv = kv.reshape(QUAD_ROWS, CHANNELS)
    old = lax.all_gather(kv, Y, axis=0, tiled=True)
    buffers = [pltpu.VMEM((4, 64, CHANNELS), BF16), pltpu.VMEM((256, 256), F32)]

    conv, prior, first, last = call(
        conv_quad_kernel,
        "conv0",
        [((4, LANES + 64, LANES), F32), (quad, BF16), (line, BF16), (line, BF16)],
        (place, to_all(told, Y), state, prior, weights, vectors),
        scalars=1,
        scratch=buffers,
        flops=1 << 30,
    )
    hidden, stats = call(
        hidden_kernel,
        "hidden0",
        [(quad, F32), stats8],
        (to_all(conv, QUAD), state, vectors),
        flops=1 << 28,
    )
    up = [(i, i + 1) for i in range(7)]
    down = [(i + 1, i) for i in range(7)]
    last, first, hidden, stats = lax.optimization_barrier((last, first, hidden, stats))
    stats, above, below = lax.optimization_barrier(
        (to_all(stats, Y), lax.ppermute(last, Y, up), lax.ppermute(first, Y, down))
    )
    asked, fresh = call(
        project_kernel,
        "project0",
        [((QUAD_ROWS, 3 * LANES), BF16), ((QUAD_ROWS, CHANNELS), BF16)],
        (stats, hidden, vectors, w_query, w_keyvalue),
        flops=1 << 28,
    )
    kv = lax.all_gather(fresh, Y, axis=0, tiled=True)
    state, stats = call(
        attend_quad_kernel,
        "attend0",
        [(quad, F32), stats8],
        (place, asked, fresh, hidden, w_out, old),
        scalars=1,
        flops=1 << 30,
    )
    conv, stats = call(
        conv_own_kernel,
        "conv1",
        [((4, ROWS + ROWS // 2, LANES), F32), stats8],
        (place, to_all(stats, Y), above, below, state, prior, weights, vectors),
        scalars=1,
        scratch=buffers,
        flops=1 << 30,
    )
    (conv,) = call(
        insert_kernel,
        "insert1",
        [((4, 56, LANES), F32)],
        (conv, to_all(stats, Y)),
        flops=1 << 24,
    )
    (out,) = call(
        attend_own_kernel,
        "attend1",
        [((2, ROWS, CHANNELS), F32)],
        (place, to_all(conv, QUAD), state, vectors, w_query, w_keyvalue, w_out, kv),
        scalars=1,
        flops=1 << 30,
    )
    return out.reshape(2, 2, COLS, CHANNELS)


def solution(mesh):
    torus = Mesh(
        mesh.devices.reshape(mesh.shape["req"], 4, 2, 2, 2), REQ_PATCH
    )
    placed = (
        P(REQ_PATCH, None, None),
        P(REQ_PATCH, None, None),
        P(REQ_PATCH, None),
        P(REQ_PATCH, None),
        P(),
        P(),
        P(None, None, None, PATCH),
        P(),
        P("req", None),
        P(),
        P(),
        P(),
        P(),
        P(),
    )
    return jax.shard_map(
        per_device,
        mesh=torus,
        in_specs=placed,
        out_specs=P(None, REQ_PATCH, None, None),
        check_vma=False,
    )
```

```python
import functools

import jax
import jax.numpy as jnp
from jax import lax
from jax.experimental import pallas as pl
from jax.experimental.pallas import tpu as pltpu
from jax.sharding import Mesh
from jax.sharding import PartitionSpec as P

GROUPS = 32
HEADS = 5
HEAD_DIM = 64
WIDTH = HEADS * HEAD_DIM
CHANNELS = 640
MEMBERS = CHANNELS // GROUPS
COLS = 16
ROWS = 32
LANES = 128
QUAD_ROWS = 4 * ROWS
POSITIONS = 1024
EPS = 1e-05

Y = ("yh", "yl")
QUAD = ("zh", "core")
REQ_PATCH = ("req", "yh", "yl", "zh", "core")
PATCH = ("yh", "yl", "zh", "core")

F32 = jnp.float32
BF16 = jnp.bfloat16

NN = (((1,), (0,)), ((), ()))
NT = (((1,), (1,)), ((), ()))


def dot(a, b, dims=NN):
    return lax.dot_general(a, b, dims, preferred_element_type=F32)


def thirds(x):
    high = x.astype(BF16)
    rest = x - high.astype(F32)
    middle = rest.astype(BF16)
    low = (rest - middle.astype(F32)).astype(BF16)
    return high, middle, low


def picked(x, zero_one, dims=NN):
    rows = x.shape[0]
    stacked = jnp.concatenate([t.astype(F32) for t in thirds(x)], axis=0).astype(BF16)
    out = dot(stacked, zero_one, dims)
    return out[:rows] + out[rows : 2 * rows] + out[2 * rows :]


def group_matrix():
    channel = lax.broadcasted_iota(jnp.int32, (CHANNELS, LANES), 0)
    first = lax.broadcasted_iota(jnp.int32, (CHANNELS, LANES), 1) * MEMBERS
    return jnp.where((channel >= first) & (channel < first + MEMBERS), 1.0, 0.0).astype(BF16)


def eight(rows, lanes):
    have = sum(r.shape[0] for r in rows)
    return jnp.concatenate([*rows, jnp.zeros((8 - have, lanes), F32)], axis=0)


def tell_sums(x, groups, stats_ref):
    sums = eight(
        [jnp.sum(x, axis=0, keepdims=True), jnp.sum(x * x, axis=0, keepdims=True)], CHANNELS
    )
    told = picked(sums, groups)[0:4]
    stats_ref[...] = jnp.broadcast_to(told[None], stats_ref.shape)


def mean_and_scale(stats_ref, groups):
    return spread_sums(jnp.sum(stats_ref[...], axis=0), groups)


def spread_sums(sums, groups):
    number = POSITIONS * MEMBERS
    mean = sums[0:1] * (1.0 / number)
    variance = sums[1:2] * (1.0 / number) - mean * mean
    spread = picked(eight([mean, lax.rsqrt(variance + EPS)], LANES), groups, NT)
    return spread[0:1], spread[1:2]


def pack_kernel(field_ref, stale_ref, packed_ref):
    high, middle, _ = thirds(field_ref[...])
    for to in range(4):
        packed_ref[to, 0:ROWS] = high
        packed_ref[to, ROWS : 2 * ROWS] = middle
        packed_ref[to, 2 * ROWS :] = stale_ref[...]


def unpack_kernel(
    place_ref, packed_ref, field_ref, state_ref, prior_ref, first_ref, last_ref, stats_ref
):
    for t in range(4):
        state_ref[t] = packed_ref[t, 0:ROWS].astype(F32) + packed_ref[t, ROWS : 2 * ROWS].astype(F32)
        prior_ref[t] = packed_ref[t, 2 * ROWS :]
    state_ref[place_ref[1]] = field_ref[...]
    first_ref[...] = prior_ref[0, :COLS]
    last_ref[...] = prior_ref[3, COLS:]
    tell_sums(state_ref[...].reshape(QUAD_ROWS, CHANNELS), group_matrix(), stats_ref)


def activate(sums, edges, state_ref, prior_ref, vectors_ref, keep, rows):
    mean, scale = spread_sums(sums, group_matrix())
    above, below = edges
    for t in range(4):
        value = (state_ref[t] - mean) * scale * vectors_ref[0:1] + vectors_ref[1:2]
        act = (value * (1.0 / (1.0 + jnp.exp(-value)))).astype(BF16)
        rows[t, COLS : 3 * COLS] = act
        keep(t, act)
        rows[t, 0:COLS] = above if t == 0 else prior_ref[t - 1, COLS:]
        rows[t, 3 * COLS :] = below if t == 3 else prior_ref[t + 1, :COLS]


def convolve(rows, weight_ref, wide):
    window = rows[...].reshape(4 * 64, CHANNELS)
    wide[...] = jnp.zeros(wide.shape, F32)
    col = lax.broadcasted_iota(jnp.int32, (LANES, LANES), 0) & (COLS - 1)
    lane = lax.broadcasted_iota(jnp.int32, (LANES, LANES), 1)
    tiles = [jnp.zeros((LANES, LANES), F32), jnp.zeros((LANES, LANES), F32)]
    for part in range(8):
        wide[:, 0 : 9 * MEMBERS] = dot(window, weight_ref[part, ROWS:], NT)
        whole = wide[...].reshape(4, 64, 256)
        lines = [
            whole[:, COLS * r : COLS * r + 2 * COLS].reshape(LANES, 256) for r in range(3)
        ]
        total = (
            lines[0][:, :LANES]
            + pltpu.roll(lines[1][:, :LANES], LANES - 3 * MEMBERS, 1)
            + pltpu.roll(lines[2], 256 - 6 * MEMBERS, 1)[:, :LANES]
        )
        left = jnp.where(col > 0, pltpu.roll(total, 1, 0), 0.0)
        centre = pltpu.roll(total, LANES - MEMBERS, 1)
        right = pltpu.roll(total, LANES - 2 * MEMBERS, 1)
        right = jnp.where(col < COLS - 1, pltpu.roll(right, LANES - 1, 0), 0.0)
        made = left + centre + right
        tile, at = divmod(part, 6)
        at *= MEMBERS
        if at:
            made = pltpu.roll(made, at, 1)
        kept = (lane >= at) & (lane < at + MEMBERS)
        tiles[tile] = jnp.where(kept, made, tiles[tile])
    return tiles


def folded(tile):
    half = tile.shape[0] // 2
    lane = lax.broadcasted_iota(jnp.int32, (half, LANES), 1)
    return jnp.where(lane < 64, tile[:half], pltpu.roll(tile[half:], 64, 1))


def conv_quad_kernel(
    stats_ref,
    above_ref,
    below_ref,
    state_ref,
    prior_ref,
    weight_ref,
    vectors_ref,
    out_ref,
    act_ref,
    first_ref,
    last_ref,
    rows,
    wide,
):
    def keep(t, act):
        act_ref[t] = act
        if t == 0:
            first_ref[...] = act[:COLS]
        if t == 3:
            last_ref[...] = act[COLS:]

    edges = (above_ref[...], below_ref[...])
    sums = jnp.sum(stats_ref[...], axis=0)
    activate(sums, edges, state_ref, prior_ref, vectors_ref, keep, rows)
    tiles = convolve(rows, weight_ref, wide)
    rest = folded(tiles[1])
    for to in range(4):
        out_ref[to, 0:LANES] = tiles[0]
        out_ref[to, LANES:] = rest


def shard_lanes(shape, dim):
    lane = lax.broadcasted_iota(jnp.int32, shape, dim)
    inner = lane & (LANES - 1)
    part = (inner * 3277) >> 16
    within = inner - MEMBERS * part
    second = lane >= LANES
    used = part < jnp.where(second, 2, 6)
    return part + jnp.where(second, 6, 0), within, used


def conv_own_kernel(
    place_ref,
    stats_ref,
    above_ref,
    below_ref,
    state_ref,
    prior_ref,
    weight_ref,
    vectors_ref,
    out_ref,
    told_ref,
    rows,
    wide,
):
    a = place_ref[1]
    activate(
        jnp.sum(stats_ref[...], axis=0),
        (above_ref[...], below_ref[...]),
        state_ref,
        prior_ref,
        vectors_ref,
        lambda t, act: None,
        rows,
    )
    tiles = convolve(rows, weight_ref, wide)
    for t in range(4):
        mine = slice(t * ROWS, (t + 1) * ROWS)
        out_ref[t, 0:ROWS] = tiles[0][mine]
        out_ref[t, ROWS:] = folded(tiles[1][mine])
    part, within, used = shard_lanes((CHANNELS, 256), 1)
    channel = lax.broadcasted_iota(jnp.int32, (CHANNELS, 256), 0)
    select = used & (channel == 4 * MEMBERS * part + MEMBERS * a + within)
    select = jnp.where(select, 1.0, 0.0).astype(BF16)
    part, _, used = shard_lanes((LANES, 256), 1)
    group = lax.broadcasted_iota(jnp.int32, (LANES, 256), 0)
    holds = jnp.where(used & (group == 4 * part + a), 1.0, 0.0).astype(BF16)
    state = state_ref[...].reshape(QUAD_ROWS, CHANNELS)
    hidden = picked(state, select) + (
        jnp.concatenate(tiles, axis=1) + picked(eight([vectors_ref[5:6]], CHANNELS), select)[0:1]
    )
    sums = eight(
        [jnp.sum(hidden, axis=0, keepdims=True), jnp.sum(hidden * hidden, axis=0, keepdims=True)],
        256,
    )
    told = picked(sums, holds, NT)[0:4]
    told_ref[...] = jnp.broadcast_to(told[None], told_ref.shape)


def insert_kernel(conv_ref, stats_ref, out_ref):
    sums = jnp.sum(stats_ref[...], axis=0)
    for to in range(4):
        out_ref[to, 0:48] = conv_ref[to]
        out_ref[to, 48:] = eight([sums], LANES)


def assembled(conv_ref, count):
    lane = lax.broadcasted_iota(jnp.int32, (count, LANES), 1)
    tiles = [jnp.zeros((count, LANES), F32) for _ in range(5)]
    for t in range(4):
        rest = conv_ref[t, count : count + count // 2]
        sources = (
            conv_ref[t, 0:count],
            jnp.concatenate([rest, pltpu.roll(rest, 64, 1)], axis=0),
        )
        for part in range(8):
            source, at = divmod(part, 6)
            at *= MEMBERS
            tile, to = divmod(4 * MEMBERS * part + MEMBERS * t, LANES)
            turn = (to - at) % LANES
            block = sources[source]
            if turn:
                block = pltpu.roll(block, turn, 1)
            kept = (lane >= to) & (lane < to + MEMBERS)
            tiles[tile] = jnp.where(kept, block, tiles[tile])
            if to + MEMBERS > LANES:
                kept = lane < to + MEMBERS - LANES
                tiles[tile + 1] = jnp.where(kept, block, tiles[tile + 1])
    return jnp.concatenate(tiles, axis=1)


def hidden_kernel(conv_ref, state_ref, vectors_ref, hidden_ref, stats_ref):
    state = state_ref[...].reshape(QUAD_ROWS, CHANNELS)
    hidden = state + (assembled(conv_ref, QUAD_ROWS) + vectors_ref[4:5])
    hidden_ref[...] = hidden.reshape(hidden_ref.shape)
    tell_sums(hidden, group_matrix(), stats_ref)


def project(hidden, mean, scale, vectors_ref, query_ref, keyvalue_ref):
    normed = ((hidden - mean) * scale * vectors_ref[2:3] + vectors_ref[3:4]).astype(BF16)
    query = dot(normed, query_ref[...]).astype(BF16)
    return query, dot(normed, keyvalue_ref[...]).astype(BF16)


def project_kernel(
    stats_ref, hidden_ref, vectors_ref, query_ref, keyvalue_ref, asked_ref, fresh_ref
):
    mean, scale = mean_and_scale(stats_ref, group_matrix())
    hidden = hidden_ref[...].reshape(QUAD_ROWS, CHANNELS)
    asked, fresh = project(hidden, mean, scale, vectors_ref, query_ref, keyvalue_ref)
    asked_ref[...] = asked
    fresh_ref[...] = fresh


def attend(query, fresh, patch, y, kvs):
    count = query.shape[0]
    lane = lax.broadcasted_iota(jnp.int32, (count, LANES), 1)
    low = lane < HEAD_DIM

    replaced = []
    for ref, step, first in kvs:
        block = lax.broadcasted_iota(jnp.int32, (count, ref.shape[0]), 1) >> 5
        replaced.append(step * block + first == 4 * y + patch)
    if count == ROWS:
        theirs = None
    else:
        theirs = (lax.broadcasted_iota(jnp.int32, (count, count), 1) >> 5) == patch
    tiles = [jnp.zeros((count, LANES), F32) for _ in range(3)]
    for h in range(HEADS):
        at = LANES * (h // 2)
        own = low if h % 2 == 0 else ~low
        asked = jnp.where(own, query[:, at : at + LANES].astype(F32), 0.0).astype(BF16)
        olds = [dot(asked, ref[:, at : at + LANES], NT) * HEAD_DIM ** (-0.5) for ref, _, _ in kvs]
        olds = [jnp.where(r, -jnp.inf, old) for r, old in zip(replaced, olds)]
        new = dot(asked, fresh[:, at : at + LANES], NT) * HEAD_DIM ** (-0.5)
        if theirs is not None:
            new = jnp.where(theirs, new, -jnp.inf)
        peak = functools.reduce(
            jnp.maximum, [jnp.max(e, axis=1, keepdims=True) for e in (*olds, new)]
        )
        olds = [jnp.exp(old - peak) for old in olds]
        new = jnp.exp(new - peak)
        total = sum(jnp.sum(e, axis=1, keepdims=True) for e in (*olds, new))
        at = LANES * ((HEADS + h) // 2)
        summed = sum(
            dot(old.astype(BF16), ref[:, at : at + LANES]) for old, (ref, _, _) in zip(olds, kvs)
        )
        summed += dot(new.astype(BF16), fresh[:, at : at + LANES])
        summed = pltpu.roll(summed / total, HEAD_DIM, 1)
        tiles[h // 2] = jnp.where(own, summed, tiles[h // 2])
    return jnp.concatenate(tiles, axis=1)[:, :WIDTH].astype(BF16)


def attend_quad_kernel(
    place_ref,
    asked_ref,
    fresh_ref,
    hidden_ref,
    out_ref,
    own_ref,
    beside_ref,
    across_ref,
    corner_ref,
    state_ref,
    told_ref,
):
    a = place_ref[1]
    kvs = [(r, 4, a ^ k) for k, r in enumerate((own_ref, beside_ref, across_ref, corner_ref))]
    patch = lax.broadcasted_iota(jnp.int32, (QUAD_ROWS, 1), 0) >> 5
    attended = attend(asked_ref[...], fresh_ref[...], patch, place_ref[0], kvs)
    result = hidden_ref[...].reshape(QUAD_ROWS, CHANNELS) + dot(attended, out_ref[...])
    state_ref[...] = result.reshape(state_ref.shape)
    tell_sums(result, group_matrix(), told_ref)


def attend_own_kernel(
    place_ref,
    conv_ref,
    state_ref,
    vectors_ref,
    query_ref,
    keyvalue_ref,
    out_ref,
    kv_ref,
    result_ref,
):
    a = place_ref[1]
    earlier = state_ref[a]
    hidden = earlier + (assembled(conv_ref, ROWS) + vectors_ref[5:6])
    sums = jnp.zeros((8, LANES), F32)
    for t in range(4):
        sums += conv_ref[t, 48:56]
    mean, scale = spread_sums(sums, group_matrix())
    query, fresh = project(hidden, mean, scale, vectors_ref, query_ref, keyvalue_ref)
    attended = attend(query, fresh, a, place_ref[0], ((kv_ref, 1, 0),))
    result_ref[0] = earlier
    result_ref[1] = hidden + dot(attended, out_ref[...])


VMEM = pl.BlockSpec(memory_space=pltpu.VMEM)
SMEM = pl.BlockSpec(memory_space=pltpu.SMEM)


def call(kernel, name, out_shapes, args, scalars=0, scratch=(), flops=0):
    return pl.pallas_call(
        kernel,
        name=name,
        out_shape=[jax.ShapeDtypeStruct(s, t) for s, t in out_shapes],
        in_specs=[SMEM] * scalars + [VMEM] * (len(args) - scalars),
        out_specs=[VMEM] * len(out_shapes),
        scratch_shapes=list(scratch),
        cost_estimate=pl.CostEstimate(flops=flops, bytes_accessed=1 << 20, transcendentals=0),
        compiler_params=pltpu.CompilerParams(vmem_limit_bytes=20 << 20),
    )(*args)


def to_all(value, axes):
    return lax.all_to_all(value, axes, 0, 0, tiled=True)


def per_device(
    field,
    stale_conv_in,
    stale_keys,
    stale_values,
    norm1_gain,
    norm1_bias,
    conv_weight,
    conv_bias,
    time_embed,
    norm2_gain,
    norm2_bias,
    w_query,
    w_keyvalue,
    w_out,
):
    quad = (4, ROWS, CHANNELS)
    line = (COLS, CHANNELS)
    stats8 = ((8, 4, LANES), F32)
    y = 2 * lax.axis_index("yh") + lax.axis_index("yl")
    a = 2 * lax.axis_index("zh") + lax.axis_index("core")
    place = jnp.stack([y, a]).astype(jnp.int32)

    slices = conv_weight.transpose(0, 1, 3, 2).reshape(9 * MEMBERS, CHANNELS)
    stale_kv = jnp.concatenate([stale_keys, stale_values], axis=1)
    weights = lax.all_gather(jnp.concatenate([stale_kv, slices], axis=0), Y, axis=0, tiled=False)

    own = field.reshape(ROWS, CHANNELS)
    (packed,) = call(
        pack_kernel,
        "pack",
        [((4, 3 * ROWS, CHANNELS), BF16)],
        (own, stale_conv_in.reshape(ROWS, CHANNELS)),
    )
    vectors = jnp.stack(
        [
            norm1_gain,
            norm1_bias,
            norm2_gain,
            norm2_bias,
            conv_bias + time_embed[0],
            conv_bias + time_embed[1],
            jnp.zeros_like(conv_bias),
            jnp.zeros_like(conv_bias),
        ]
    )
    w_query = jnp.pad(w_query, ((0, 0), (0, 3 * LANES - WIDTH)))
    packed, vectors, w_query, place = lax.optimization_barrier(
        (to_all(packed, QUAD), vectors, w_query, place)
    )
    state, prior, first, last, stats = call(
        unpack_kernel,
        "unpack",
        [(quad, F32), (quad, BF16), (line, BF16), (line, BF16), stats8],
        (place, packed, own),
        scalars=1,
    )
    buffers = [pltpu.VMEM((4, 64, CHANNELS), BF16), pltpu.VMEM((256, 256), F32)]
    up = [(i, i + 1) for i in range(7)]
    down = [(i + 1, i) for i in range(7)]
    swapped = lambda v, axis: lax.ppermute(v, axis, [(0, 1), (1, 0)])
    above = lax.ppermute(last, Y, up)
    below = lax.ppermute(first, Y, down)

    conv, prior, first, last = call(
        conv_quad_kernel,
        "conv0",
        [((4, LANES + 64, LANES), F32), (quad, BF16), (line, BF16), (line, BF16)],
        (to_all(stats, Y), above, below, state, prior, weights, vectors),
        scratch=buffers,
        flops=1 << 30,
    )
    conv, old = lax.optimization_barrier((conv, weights[:, :ROWS].reshape(8 * ROWS, CHANNELS)))
    across = swapped(old, "zh")
    conv, beside = lax.optimization_barrier((to_all(conv, QUAD), swapped(old, "core")))
    hidden, stats = call(
        hidden_kernel,
        "hidden0",
        [(quad, F32), stats8],
        (conv, state, vectors),
        flops=1 << 28,
    )
    last, first, hidden, stats = lax.optimization_barrier((last, first, hidden, stats))
    stats, above, below, across = lax.optimization_barrier(
        (to_all(stats, Y), lax.ppermute(last, Y, up), lax.ppermute(first, Y, down), across)
    )
    asked, fresh = call(
        project_kernel,
        "project0",
        [((QUAD_ROWS, 3 * LANES), BF16), ((QUAD_ROWS, CHANNELS), BF16)],
        (stats, hidden, vectors, w_query, w_keyvalue),
        flops=1 << 28,
    )
    kv = lax.all_gather(fresh, Y, axis=0, tiled=True)
    state, stats = call(
        attend_quad_kernel,
        "attend0",
        [(quad, F32), stats8],
        (place, asked, fresh, hidden, w_out, old, beside, across, swapped(across, "core")),
        scalars=1,
        flops=1 << 30,
    )
    conv, stats = call(
        conv_own_kernel,
        "conv1",
        [((4, ROWS + ROWS // 2, LANES), F32), stats8],
        (place, to_all(stats, Y), above, below, state, prior, weights, vectors),
        scalars=1,
        scratch=buffers,
        flops=1 << 30,
    )
    (conv,) = call(
        insert_kernel,
        "insert1",
        [((4, 56, LANES), F32)],
        (conv, to_all(stats, Y)),
        flops=1 << 24,
    )
    (out,) = call(
        attend_own_kernel,
        "attend1",
        [((2, ROWS, CHANNELS), F32)],
        (place, to_all(conv, QUAD), state, vectors, w_query, w_keyvalue, w_out, kv),
        scalars=1,
        flops=1 << 30,
    )
    return out.reshape(2, 2, COLS, CHANNELS)


def solution(mesh):
    torus = Mesh(
        mesh.devices.reshape(mesh.shape["req"], 4, 2, 2, 2), REQ_PATCH
    )
    placed = (
        P(REQ_PATCH, None, None),
        P(REQ_PATCH, None, None),
        P(REQ_PATCH, None),
        P(REQ_PATCH, None),
        P(),
        P(),
        P(None, None, None, PATCH),
        P(),
        P("req", None),
        P(),
        P(),
        P(),
        P(),
        P(),
    )
    return jax.shard_map(
        per_device,
        mesh=torus,
        in_specs=placed,
        out_specs=P(None, REQ_PATCH, None, None),
        check_vma=False,
    )
```

```python
import functools

import jax
import jax.numpy as jnp
from jax import lax
from jax.experimental import pallas as pl
from jax.experimental.pallas import tpu as pltpu
from jax.sharding import Mesh
from jax.sharding import PartitionSpec as P

GROUPS = 32
HEADS = 5
HEAD_DIM = 64
WIDTH = HEADS * HEAD_DIM
CHANNELS = 640
MEMBERS = CHANNELS // GROUPS
COLS = 16
ROWS = 32
LANES = 128
QUAD_ROWS = 4 * ROWS
POSITIONS = 1024
EPS = 1e-05

Y = ("yh", "yl")
QUAD = ("zh", "core")
REQ_PATCH = ("req", "yh", "yl", "zh", "core")
PATCH = ("yh", "yl", "zh", "core")

F32 = jnp.float32
BF16 = jnp.bfloat16

NN = (((1,), (0,)), ((), ()))
NT = (((1,), (1,)), ((), ()))


def dot(a, b, dims=NN):
    return lax.dot_general(a, b, dims, preferred_element_type=F32)


def thirds(x):
    high = x.astype(BF16)
    rest = x - high.astype(F32)
    middle = rest.astype(BF16)
    low = (rest - middle.astype(F32)).astype(BF16)
    return high, middle, low


def picked(x, zero_one, dims=NN):
    rows = x.shape[0]
    stacked = jnp.concatenate([t.astype(F32) for t in thirds(x)], axis=0).astype(BF16)
    out = dot(stacked, zero_one, dims)
    return out[:rows] + out[rows : 2 * rows] + out[2 * rows :]


def group_matrix():
    channel = lax.broadcasted_iota(jnp.int32, (CHANNELS, LANES), 0)
    first = lax.broadcasted_iota(jnp.int32, (CHANNELS, LANES), 1) * MEMBERS
    return jnp.where((channel >= first) & (channel < first + MEMBERS), 1.0, 0.0).astype(BF16)


def eight(rows, lanes):
    have = sum(r.shape[0] for r in rows)
    return jnp.concatenate([*rows, jnp.zeros((8 - have, lanes), F32)], axis=0)


def tell_sums(x, groups, stats_ref):
    sums = eight(
        [jnp.sum(x, axis=0, keepdims=True), jnp.sum(x * x, axis=0, keepdims=True)], CHANNELS
    )
    told = picked(sums, groups)[0:4]
    stats_ref[...] = jnp.broadcast_to(told[None], stats_ref.shape)


def mean_and_scale(stats_ref, groups):
    return spread_sums(jnp.sum(stats_ref[...], axis=0), groups)


def spread_sums(sums, groups):
    number = POSITIONS * MEMBERS
    mean = sums[0:1] * (1.0 / number)
    variance = sums[1:2] * (1.0 / number) - mean * mean
    spread = picked(eight([mean, lax.rsqrt(variance + EPS)], LANES), groups, NT)
    return spread[0:1], spread[1:2]


def pack_kernel(field_ref, stale_ref, keys_ref, values_ref, packed_ref):
    high, middle, _ = thirds(field_ref[...])
    both = jnp.concatenate(
        [keys_ref[...].astype(F32), values_ref[...].astype(F32)], axis=1
    ).astype(BF16)
    for to in range(4):
        packed_ref[to, 0:ROWS] = high
        packed_ref[to, ROWS : 2 * ROWS] = middle
        packed_ref[to, 2 * ROWS : 3 * ROWS] = stale_ref[...]
        packed_ref[to, 3 * ROWS :] = both


def unpack_kernel(
    place_ref,
    packed_ref,
    field_ref,
    state_ref,
    kv_ref,
    prior_ref,
    first_ref,
    last_ref,
    stats_ref,
):
    for t in range(4):
        state_ref[t] = packed_ref[t, 0:ROWS].astype(F32) + packed_ref[t, ROWS : 2 * ROWS].astype(F32)
        prior_ref[t] = packed_ref[t, 2 * ROWS : 3 * ROWS]
        kv_ref[t] = packed_ref[t, 3 * ROWS :]
    state_ref[place_ref[1]] = field_ref[...]
    first_ref[...] = prior_ref[0, :COLS]
    last_ref[...] = prior_ref[3, COLS:]
    tell_sums(state_ref[...].reshape(QUAD_ROWS, CHANNELS), group_matrix(), stats_ref)


def activate(sums, edges, state_ref, prior_ref, vectors_ref, keep, rows):
    mean, scale = spread_sums(sums, group_matrix())
    above, below = edges
    for t in range(4):
        value = (state_ref[t] - mean) * scale * vectors_ref[0:1] + vectors_ref[1:2]
        act = (value * (1.0 / (1.0 + jnp.exp(-value)))).astype(BF16)
        rows[t, COLS : 3 * COLS] = act
        keep(t, act)
        rows[t, 0:COLS] = above if t == 0 else prior_ref[t - 1, COLS:]
        rows[t, 3 * COLS :] = below if t == 3 else prior_ref[t + 1, :COLS]


def convolve(rows, weight_ref, wide):
    window = rows[...].reshape(4 * 64, CHANNELS)
    wide[...] = jnp.zeros(wide.shape, F32)
    col = lax.broadcasted_iota(jnp.int32, (LANES, LANES), 0) & (COLS - 1)
    lane = lax.broadcasted_iota(jnp.int32, (LANES, LANES), 1)
    tiles = [jnp.zeros((LANES, LANES), F32), jnp.zeros((LANES, LANES), F32)]
    for part in range(8):
        wide[:, 0 : 9 * MEMBERS] = dot(window, weight_ref[part], NT)
        whole = wide[...].reshape(4, 64, 256)
        lines = [
            whole[:, COLS * r : COLS * r + 2 * COLS].reshape(LANES, 256) for r in range(3)
        ]
        total = (
            lines[0][:, :LANES]
            + pltpu.roll(lines[1][:, :LANES], LANES - 3 * MEMBERS, 1)
            + pltpu.roll(lines[2], 256 - 6 * MEMBERS, 1)[:, :LANES]
        )
        left = jnp.where(col > 0, pltpu.roll(total, 1, 0), 0.0)
        centre = pltpu.roll(total, LANES - MEMBERS, 1)
        right = pltpu.roll(total, LANES - 2 * MEMBERS, 1)
        right = jnp.where(col < COLS - 1, pltpu.roll(right, LANES - 1, 0), 0.0)
        made = left + centre + right
        tile, at = divmod(part, 6)
        at *= MEMBERS
        if at:
            made = pltpu.roll(made, at, 1)
        kept = (lane >= at) & (lane < at + MEMBERS)
        tiles[tile] = jnp.where(kept, made, tiles[tile])
    return tiles


def folded(tile):
    half = tile.shape[0] // 2
    lane = lax.broadcasted_iota(jnp.int32, (half, LANES), 1)
    return jnp.where(lane < 64, tile[:half], pltpu.roll(tile[half:], 64, 1))


def conv_quad_kernel(
    stats_ref,
    above_ref,
    below_ref,
    state_ref,
    prior_ref,
    weight_ref,
    vectors_ref,
    out_ref,
    act_ref,
    first_ref,
    last_ref,
    rows,
    wide,
):
    def keep(t, act):
        act_ref[t] = act
        if t == 0:
            first_ref[...] = act[:COLS]
        if t == 3:
            last_ref[...] = act[COLS:]

    edges = (above_ref[...], below_ref[...])
    sums = jnp.sum(stats_ref[...], axis=0)
    activate(sums, edges, state_ref, prior_ref, vectors_ref, keep, rows)
    tiles = convolve(rows, weight_ref, wide)
    rest = folded(tiles[1])
    for to in range(4):
        out_ref[to, 0:LANES] = tiles[0]
        out_ref[to, LANES:] = rest


def shard_lanes(shape, dim):
    lane = lax.broadcasted_iota(jnp.int32, shape, dim)
    inner = lane & (LANES - 1)
    part = (inner * 3277) >> 16
    within = inner - MEMBERS * part
    second = lane >= LANES
    used = part < jnp.where(second, 2, 6)
    return part + jnp.where(second, 6, 0), within, used


def conv_own_kernel(
    place_ref,
    stats_ref,
    above_ref,
    below_ref,
    state_ref,
    prior_ref,
    weight_ref,
    vectors_ref,
    out_ref,
    told_ref,
    rows,
    wide,
):
    a = place_ref[1]
    activate(
        jnp.sum(stats_ref[...], axis=0),
        (above_ref[...], below_ref[...]),
        state_ref,
        prior_ref,
        vectors_ref,
        lambda t, act: None,
        rows,
    )
    tiles = convolve(rows, weight_ref, wide)
    for t in range(4):
        mine = slice(t * ROWS, (t + 1) * ROWS)
        out_ref[t, 0:ROWS] = tiles[0][mine]
        out_ref[t, ROWS:] = folded(tiles[1][mine])
    part, within, used = shard_lanes((CHANNELS, 256), 1)
    channel = lax.broadcasted_iota(jnp.int32, (CHANNELS, 256), 0)
    select = used & (channel == 4 * MEMBERS * part + MEMBERS * a + within)
    select = jnp.where(select, 1.0, 0.0).astype(BF16)
    part, _, used = shard_lanes((LANES, 256), 1)
    group = lax.broadcasted_iota(jnp.int32, (LANES, 256), 0)
    holds = jnp.where(used & (group == 4 * part + a), 1.0, 0.0).astype(BF16)
    state = state_ref[...].reshape(QUAD_ROWS, CHANNELS)
    hidden = picked(state, select) + (
        jnp.concatenate(tiles, axis=1) + picked(eight([vectors_ref[5:6]], CHANNELS), select)[0:1]
    )
    sums = eight(
        [jnp.sum(hidden, axis=0, keepdims=True), jnp.sum(hidden * hidden, axis=0, keepdims=True)],
        256,
    )
    told = picked(sums, holds, NT)[0:4]
    told_ref[...] = jnp.broadcast_to(told[None], told_ref.shape)


def insert_kernel(conv_ref, stats_ref, out_ref):
    sums = jnp.sum(stats_ref[...], axis=0)
    for to in range(4):
        out_ref[to, 0:48] = conv_ref[to]
        out_ref[to, 48:] = eight([sums], LANES)


def assembled(conv_ref, count):
    lane = lax.broadcasted_iota(jnp.int32, (count, LANES), 1)
    tiles = [jnp.zeros((count, LANES), F32) for _ in range(5)]
    for t in range(4):
        rest = conv_ref[t, count : count + count // 2]
        sources = (
            conv_ref[t, 0:count],
            jnp.concatenate([rest, pltpu.roll(rest, 64, 1)], axis=0),
        )
        for part in range(8):
            source, at = divmod(part, 6)
            at *= MEMBERS
            tile, to = divmod(4 * MEMBERS * part + MEMBERS * t, LANES)
            turn = (to - at) % LANES
            block = sources[source]
            if turn:
                block = pltpu.roll(block, turn, 1)
            kept = (lane >= to) & (lane < to + MEMBERS)
            tiles[tile] = jnp.where(kept, block, tiles[tile])
            if to + MEMBERS > LANES:
                kept = lane < to + MEMBERS - LANES
                tiles[tile + 1] = jnp.where(kept, block, tiles[tile + 1])
    return jnp.concatenate(tiles, axis=1)


def hidden_kernel(conv_ref, state_ref, vectors_ref, hidden_ref, stats_ref):
    state = state_ref[...].reshape(QUAD_ROWS, CHANNELS)
    hidden = state + (assembled(conv_ref, QUAD_ROWS) + vectors_ref[4:5])
    hidden_ref[...] = hidden.reshape(hidden_ref.shape)
    tell_sums(hidden, group_matrix(), stats_ref)


def project(hidden, mean, scale, vectors_ref, query_ref, keyvalue_ref):
    normed = ((hidden - mean) * scale * vectors_ref[2:3] + vectors_ref[3:4]).astype(BF16)
    query = dot(normed, query_ref[...]).astype(BF16)
    return query, dot(normed, keyvalue_ref[...]).astype(BF16)


def project_kernel(
    stats_ref, hidden_ref, vectors_ref, query_ref, keyvalue_ref, asked_ref, fresh_ref
):
    mean, scale = mean_and_scale(stats_ref, group_matrix())
    hidden = hidden_ref[...].reshape(QUAD_ROWS, CHANNELS)
    asked, fresh = project(hidden, mean, scale, vectors_ref, query_ref, keyvalue_ref)
    asked_ref[...] = asked
    fresh_ref[...] = fresh


def attend(query, fresh, patch, y, kv_ref):
    count = query.shape[0]
    lane = lax.broadcasted_iota(jnp.int32, (count, LANES), 1)
    low = lane < HEAD_DIM

    block = lax.broadcasted_iota(jnp.int32, (count, POSITIONS), 1) >> 5
    replaced = block == 4 * y + patch
    if count == ROWS:
        theirs = None
    else:
        theirs = (lax.broadcasted_iota(jnp.int32, (count, count), 1) >> 5) == patch
    tiles = [jnp.zeros((count, LANES), F32) for _ in range(3)]
    for h in range(HEADS):
        at = LANES * (h // 2)
        own = low if h % 2 == 0 else ~low
        asked = jnp.where(own, query[:, at : at + LANES].astype(F32), 0.0).astype(BF16)
        old = dot(asked, kv_ref[:, at : at + LANES], NT) * HEAD_DIM ** (-0.5)
        old = jnp.where(replaced, -jnp.inf, old)
        new = dot(asked, fresh[:, at : at + LANES], NT) * HEAD_DIM ** (-0.5)
        if theirs is not None:
            new = jnp.where(theirs, new, -jnp.inf)
        peak = jnp.maximum(
            jnp.max(old, axis=1, keepdims=True), jnp.max(new, axis=1, keepdims=True)
        )
        old = jnp.exp(old - peak)
        new = jnp.exp(new - peak)
        total = jnp.sum(old, axis=1, keepdims=True) + jnp.sum(new, axis=1, keepdims=True)
        at = LANES * ((HEADS + h) // 2)
        summed = dot(old.astype(BF16), kv_ref[:, at : at + LANES])
        summed += dot(new.astype(BF16), fresh[:, at : at + LANES])
        summed = pltpu.roll(summed / total, HEAD_DIM, 1)
        tiles[h // 2] = jnp.where(own, summed, tiles[h // 2])
    return jnp.concatenate(tiles, axis=1)[:, :WIDTH].astype(BF16)


def attend_quad_kernel(
    place_ref, asked_ref, fresh_ref, hidden_ref, out_ref, kv_ref, state_ref, told_ref
):
    patch = lax.broadcasted_iota(jnp.int32, (QUAD_ROWS, 1), 0) >> 5
    attended = attend(asked_ref[...], fresh_ref[...], patch, place_ref[0], kv_ref)
    result = hidden_ref[...].reshape(QUAD_ROWS, CHANNELS) + dot(attended, out_ref[...])
    state_ref[...] = result.reshape(state_ref.shape)
    tell_sums(result, group_matrix(), told_ref)


def attend_own_kernel(
    place_ref,
    conv_ref,
    state_ref,
    vectors_ref,
    query_ref,
    keyvalue_ref,
    out_ref,
    kv_ref,
    result_ref,
):
    a = place_ref[1]
    earlier = state_ref[a]
    hidden = earlier + (assembled(conv_ref, ROWS) + vectors_ref[5:6])
    sums = jnp.zeros((8, LANES), F32)
    for t in range(4):
        sums += conv_ref[t, 48:56]
    mean, scale = spread_sums(sums, group_matrix())
    query, fresh = project(hidden, mean, scale, vectors_ref, query_ref, keyvalue_ref)
    attended = attend(query, fresh, a, place_ref[0], kv_ref)
    result_ref[0] = earlier
    result_ref[1] = hidden + dot(attended, out_ref[...])


VMEM = pl.BlockSpec(memory_space=pltpu.VMEM)
SMEM = pl.BlockSpec(memory_space=pltpu.SMEM)


def call(kernel, name, out_shapes, args, scalars=0, scratch=(), flops=0):
    return pl.pallas_call(
        kernel,
        name=name,
        out_shape=[jax.ShapeDtypeStruct(s, t) for s, t in out_shapes],
        in_specs=[SMEM] * scalars + [VMEM] * (len(args) - scalars),
        out_specs=[VMEM] * len(out_shapes),
        scratch_shapes=list(scratch),
        cost_estimate=pl.CostEstimate(flops=flops, bytes_accessed=1 << 20, transcendentals=0),
        compiler_params=pltpu.CompilerParams(vmem_limit_bytes=20 << 20),
    )(*args)


def to_all(value, axes):
    return lax.all_to_all(value, axes, 0, 0, tiled=True)


def per_device(
    field,
    stale_conv_in,
    stale_keys,
    stale_values,
    norm1_gain,
    norm1_bias,
    conv_weight,
    conv_bias,
    time_embed,
    norm2_gain,
    norm2_bias,
    w_query,
    w_keyvalue,
    w_out,
):
    quad = (4, ROWS, CHANNELS)
    line = (COLS, CHANNELS)
    stats8 = ((8, 4, LANES), F32)
    y = 2 * lax.axis_index("yh") + lax.axis_index("yl")
    a = 2 * lax.axis_index("zh") + lax.axis_index("core")
    place = jnp.stack([y, a]).astype(jnp.int32)

    slices = conv_weight.transpose(0, 1, 3, 2).reshape(9 * MEMBERS, CHANNELS)
    weights = lax.all_gather(slices, Y, axis=0, tiled=False)

    own = field.reshape(ROWS, CHANNELS)
    (packed,) = call(
        pack_kernel,
        "pack",
        [((4, 4 * ROWS, CHANNELS), BF16)],
        (own, stale_conv_in.reshape(ROWS, CHANNELS), stale_keys, stale_values),
    )
    vectors = jnp.stack(
        [
            norm1_gain,
            norm1_bias,
            norm2_gain,
            norm2_bias,
            conv_bias + time_embed[0],
            conv_bias + time_embed[1],
            jnp.zeros_like(conv_bias),
            jnp.zeros_like(conv_bias),
        ]
    )
    w_query = jnp.pad(w_query, ((0, 0), (0, 3 * LANES - WIDTH)))
    packed, vectors, w_query, place = lax.optimization_barrier(
        (to_all(packed, QUAD), vectors, w_query, place)
    )
    state, kv, prior, first, last, stats = call(
        unpack_kernel,
        "unpack",
        [(quad, F32), (quad, BF16), (quad, BF16), (line, BF16), (line, BF16), stats8],
        (place, packed, own),
        scalars=1,
    )
    kv = kv.reshape(QUAD_ROWS, CHANNELS)
    old = lax.all_gather(kv, Y, axis=0, tiled=True)
    up = [(i, i + 1) for i in range(7)]
    down = [(i + 1, i) for i in range(7)]
    above = lax.ppermute(last, Y, up)
    below = lax.ppermute(first, Y, down)
    buffers = [pltpu.VMEM((4, 64, CHANNELS), BF16), pltpu.VMEM((256, 256), F32)]

    conv, prior, first, last = call(
        conv_quad_kernel,
        "conv0",
        [((4, LANES + 64, LANES), F32), (quad, BF16), (line, BF16), (line, BF16)],
        (to_all(stats, Y), above, below, state, prior, weights, vectors),
        scratch=buffers,
        flops=1 << 30,
    )
    hidden, stats = call(
        hidden_kernel,
        "hidden0",
        [(quad, F32), stats8],
        (to_all(conv, QUAD), state, vectors),
        flops=1 << 28,
    )
    last, first, hidden, stats = lax.optimization_barrier((last, first, hidden, stats))
    stats, above, below = lax.optimization_barrier(
        (to_all(stats, Y), lax.ppermute(last, Y, up), lax.ppermute(first, Y, down))
    )
    asked, fresh = call(
        project_kernel,
        "project0",
        [((QUAD_ROWS, 3 * LANES), BF16), ((QUAD_ROWS, CHANNELS), BF16)],
        (stats, hidden, vectors, w_query, w_keyvalue),
        flops=1 << 28,
    )
    kv = lax.all_gather(fresh, Y, axis=0, tiled=True)
    state, stats = call(
        attend_quad_kernel,
        "attend0",
        [(quad, F32), stats8],
        (place, asked, fresh, hidden, w_out, old),
        scalars=1,
        flops=1 << 30,
    )
    conv, stats = call(
        conv_own_kernel,
        "conv1",
        [((4, ROWS + ROWS // 2, LANES), F32), stats8],
        (place, to_all(stats, Y), above, below, state, prior, weights, vectors),
        scalars=1,
        scratch=buffers,
        flops=1 << 30,
    )
    (conv,) = call(
        insert_kernel,
        "insert1",
        [((4, 56, LANES), F32)],
        (conv, to_all(stats, Y)),
        flops=1 << 24,
    )
    (out,) = call(
        attend_own_kernel,
        "attend1",
        [((2, ROWS, CHANNELS), F32)],
        (place, to_all(conv, QUAD), state, vectors, w_query, w_keyvalue, w_out, kv),
        scalars=1,
        flops=1 << 30,
    )
    return out.reshape(2, 2, COLS, CHANNELS)


def solution(mesh):
    torus = Mesh(
        mesh.devices.reshape(mesh.shape["req"], 4, 2, 2, 2), REQ_PATCH
    )
    placed = (
        P(REQ_PATCH, None, None),
        P(REQ_PATCH, None, None),
        P(REQ_PATCH, None),
        P(REQ_PATCH, None),
        P(),
        P(),
        P(None, None, None, PATCH),
        P(),
        P("req", None),
        P(),
        P(),
        P(),
        P(),
        P(),
    )
    return jax.shard_map(
        per_device,
        mesh=torus,
        in_specs=placed,
        out_specs=P(None, REQ_PATCH, None, None),
        check_vma=False,
    )
```

```python
import functools

import jax
import jax.numpy as jnp
from jax import lax
from jax.experimental import pallas as pl
from jax.experimental.pallas import tpu as pltpu
from jax.sharding import Mesh
from jax.sharding import PartitionSpec as P

GROUPS = 32
HEADS = 5
HEAD_DIM = 64
WIDTH = HEADS * HEAD_DIM
CHANNELS = 640
MEMBERS = CHANNELS // GROUPS
COLS = 16
ROWS = 32
LANES = 128
QUAD_ROWS = 4 * ROWS
POSITIONS = 1024
EPS = 1e-05

Y = ("yh", "yl")
QUAD = ("zh", "core")
REQ_PATCH = ("req", "yh", "yl", "zh", "core")
PATCH = ("yh", "yl", "zh", "core")

F32 = jnp.float32
BF16 = jnp.bfloat16

NN = (((1,), (0,)), ((), ()))
NT = (((1,), (1,)), ((), ()))


def dot(a, b, dims=NN):
    return lax.dot_general(a, b, dims, preferred_element_type=F32)


def thirds(x):
    high = x.astype(BF16)
    rest = x - high.astype(F32)
    middle = rest.astype(BF16)
    low = (rest - middle.astype(F32)).astype(BF16)
    return high, middle, low


def picked(x, zero_one, dims=NN):
    rows = x.shape[0]
    stacked = jnp.concatenate([t.astype(F32) for t in thirds(x)], axis=0).astype(BF16)
    out = dot(stacked, zero_one, dims)
    return out[:rows] + out[rows : 2 * rows] + out[2 * rows :]


def group_matrix():
    channel = lax.broadcasted_iota(jnp.int32, (CHANNELS, LANES), 0)
    first = lax.broadcasted_iota(jnp.int32, (CHANNELS, LANES), 1) * MEMBERS
    return jnp.where((channel >= first) & (channel < first + MEMBERS), 1.0, 0.0).astype(BF16)


def eight(rows, lanes):
    have = sum(r.shape[0] for r in rows)
    return jnp.concatenate([*rows, jnp.zeros((8 - have, lanes), F32)], axis=0)


def tell_sums(x, groups, stats_ref):
    sums = eight(
        [jnp.sum(x, axis=0, keepdims=True), jnp.sum(x * x, axis=0, keepdims=True)], CHANNELS
    )
    told = picked(sums, groups)[0:4]
    stats_ref[...] = jnp.broadcast_to(told[None], stats_ref.shape)


def mean_and_scale(stats_ref, groups):
    return spread_sums(jnp.sum(stats_ref[...], axis=0), groups)


def spread_sums(sums, groups):
    number = POSITIONS * MEMBERS
    mean = sums[0:1] * (1.0 / number)
    variance = sums[1:2] * (1.0 / number) - mean * mean
    spread = picked(eight([mean, lax.rsqrt(variance + EPS)], LANES), groups, NT)
    return spread[0:1], spread[1:2]


def pack_kernel(field_ref, stale_ref, keys_ref, values_ref, packed_ref):
    high, middle, _ = thirds(field_ref[...])
    both = jnp.concatenate(
        [keys_ref[...].astype(F32), values_ref[...].astype(F32)], axis=1
    ).astype(BF16)
    for to in range(4):
        packed_ref[to, 0:ROWS] = high
        packed_ref[to, ROWS : 2 * ROWS] = middle
        packed_ref[to, 2 * ROWS : 3 * ROWS] = stale_ref[...]
        packed_ref[to, 3 * ROWS :] = both


def unpack_kernel(
    place_ref,
    packed_ref,
    field_ref,
    state_ref,
    kv_ref,
    prior_ref,
    first_ref,
    last_ref,
    stats_ref,
):
    for t in range(4):
        state_ref[t] = packed_ref[t, 0:ROWS].astype(F32) + packed_ref[t, ROWS : 2 * ROWS].astype(F32)
        prior_ref[t] = packed_ref[t, 2 * ROWS : 3 * ROWS]
        kv_ref[t] = packed_ref[t, 3 * ROWS :]
    state_ref[place_ref[1]] = field_ref[...]
    first_ref[...] = prior_ref[0, :COLS]
    last_ref[...] = prior_ref[3, COLS:]
    tell_sums(state_ref[...].reshape(QUAD_ROWS, CHANNELS), group_matrix(), stats_ref)


def activate(sums, edges, state_ref, prior_ref, vectors_ref, keep, rows):
    mean, scale = spread_sums(sums, group_matrix())
    above, below = edges
    for t in range(4):
        value = (state_ref[t] - mean) * scale * vectors_ref[0:1] + vectors_ref[1:2]
        act = (value * (1.0 / (1.0 + jnp.exp(-value)))).astype(BF16)
        rows[t, COLS : 3 * COLS] = act
        keep(t, act)
        rows[t, 0:COLS] = above if t == 0 else prior_ref[t - 1, COLS:]
        rows[t, 3 * COLS :] = below if t == 3 else prior_ref[t + 1, :COLS]


def convolve(rows, weight_ref, wide):
    window = rows[...].reshape(4 * 64, CHANNELS)
    wide[...] = jnp.zeros(wide.shape, F32)
    col = lax.broadcasted_iota(jnp.int32, (LANES, LANES), 0) & (COLS - 1)
    lane = lax.broadcasted_iota(jnp.int32, (LANES, LANES), 1)
    tiles = [jnp.zeros((LANES, LANES), F32), jnp.zeros((LANES, LANES), F32)]
    for part in range(8):
        wide[:, 0 : 9 * MEMBERS] = dot(window, weight_ref[part], NT)
        whole = wide[...].reshape(4, 64, 256)
        lines = [
            whole[:, COLS * r : COLS * r + 2 * COLS].reshape(LANES, 256) for r in range(3)
        ]
        total = (
            lines[0][:, :LANES]
            + pltpu.roll(lines[1][:, :LANES], LANES - 3 * MEMBERS, 1)
            + pltpu.roll(lines[2], 256 - 6 * MEMBERS, 1)[:, :LANES]
        )
        left = jnp.where(col > 0, pltpu.roll(total, 1, 0), 0.0)
        centre = pltpu.roll(total, LANES - MEMBERS, 1)
        right = pltpu.roll(total, LANES - 2 * MEMBERS, 1)
        right = jnp.where(col < COLS - 1, pltpu.roll(right, LANES - 1, 0), 0.0)
        made = left + centre + right
        tile, at = divmod(part, 6)
        at *= MEMBERS
        if at:
            made = pltpu.roll(made, at, 1)
        kept = (lane >= at) & (lane < at + MEMBERS)
        tiles[tile] = jnp.where(kept, made, tiles[tile])
    return tiles


def folded(tile):
    half = tile.shape[0] // 2
    lane = lax.broadcasted_iota(jnp.int32, (half, LANES), 1)
    return jnp.where(lane < 64, tile[:half], pltpu.roll(tile[half:], 64, 1))


def conv_quad_kernel(
    stats_ref,
    above_ref,
    below_ref,
    state_ref,
    prior_ref,
    weight_ref,
    vectors_ref,
    out_ref,
    act_ref,
    first_ref,
    last_ref,
    rows,
    wide,
):
    def keep(t, act):
        act_ref[t] = act
        if t == 0:
            first_ref[...] = act[:COLS]
        if t == 3:
            last_ref[...] = act[COLS:]

    edges = (above_ref[...], below_ref[...])
    sums = jnp.sum(stats_ref[...], axis=0)
    activate(sums, edges, state_ref, prior_ref, vectors_ref, keep, rows)
    tiles = convolve(rows, weight_ref, wide)
    rest = folded(tiles[1])
    for to in range(4):
        out_ref[to, 0:LANES] = tiles[0]
        out_ref[to, LANES:] = rest


def shard_lanes(shape, dim):
    lane = lax.broadcasted_iota(jnp.int32, shape, dim)
    inner = lane & (LANES - 1)
    part = (inner * 3277) >> 16
    within = inner - MEMBERS * part
    second = lane >= LANES
    used = part < jnp.where(second, 2, 6)
    return part + jnp.where(second, 6, 0), within, used


def conv_own_kernel(
    place_ref,
    stats_ref,
    above_ref,
    below_ref,
    state_ref,
    prior_ref,
    weight_ref,
    vectors_ref,
    out_ref,
    told_ref,
    rows,
    wide,
):
    a = place_ref[1]
    activate(
        jnp.sum(stats_ref[...], axis=0),
        (above_ref[...], below_ref[...]),
        state_ref,
        prior_ref,
        vectors_ref,
        lambda t, act: None,
        rows,
    )
    tiles = convolve(rows, weight_ref, wide)
    for t in range(4):
        mine = slice(t * ROWS, (t + 1) * ROWS)
        out_ref[t, 0:ROWS] = tiles[0][mine]
        out_ref[t, ROWS:] = folded(tiles[1][mine])
    part, within, used = shard_lanes((CHANNELS, 256), 1)
    channel = lax.broadcasted_iota(jnp.int32, (CHANNELS, 256), 0)
    select = used & (channel == 4 * MEMBERS * part + MEMBERS * a + within)
    select = jnp.where(select, 1.0, 0.0).astype(BF16)
    part, _, used = shard_lanes((LANES, 256), 1)
    group = lax.broadcasted_iota(jnp.int32, (LANES, 256), 0)
    holds = jnp.where(used & (group == 4 * part + a), 1.0, 0.0).astype(BF16)
    state = state_ref[...].reshape(QUAD_ROWS, CHANNELS)
    hidden = picked(state, select) + (
        jnp.concatenate(tiles, axis=1) + picked(eight([vectors_ref[5:6]], CHANNELS), select)[0:1]
    )
    sums = eight(
        [jnp.sum(hidden, axis=0, keepdims=True), jnp.sum(hidden * hidden, axis=0, keepdims=True)],
        256,
    )
    told = picked(sums, holds, NT)[0:4]
    told_ref[...] = jnp.broadcast_to(told[None], told_ref.shape)


def insert_kernel(conv_ref, stats_ref, out_ref):
    sums = jnp.sum(stats_ref[...], axis=0)
    for to in range(4):
        out_ref[to, 0:48] = conv_ref[to]
        out_ref[to, 48:] = eight([sums], LANES)


def assembled(conv_ref, count):
    lane = lax.broadcasted_iota(jnp.int32, (count, LANES), 1)
    tiles = [jnp.zeros((count, LANES), F32) for _ in range(5)]
    for t in range(4):
        rest = conv_ref[t, count : count + count // 2]
        sources = (
            conv_ref[t, 0:count],
            jnp.concatenate([rest, pltpu.roll(rest, 64, 1)], axis=0),
        )
        for part in range(8):
            source, at = divmod(part, 6)
            at *= MEMBERS
            tile, to = divmod(4 * MEMBERS * part + MEMBERS * t, LANES)
            turn = (to - at) % LANES
            block = sources[source]
            if turn:
                block = pltpu.roll(block, turn, 1)
            kept = (lane >= to) & (lane < to + MEMBERS)
            tiles[tile] = jnp.where(kept, block, tiles[tile])
            if to + MEMBERS > LANES:
                kept = lane < to + MEMBERS - LANES
                tiles[tile + 1] = jnp.where(kept, block, tiles[tile + 1])
    return jnp.concatenate(tiles, axis=1)


def hidden_kernel(conv_ref, state_ref, vectors_ref, hidden_ref, stats_ref):
    state = state_ref[...].reshape(QUAD_ROWS, CHANNELS)
    hidden = state + (assembled(conv_ref, QUAD_ROWS) + vectors_ref[4:5])
    hidden_ref[...] = hidden.reshape(hidden_ref.shape)
    tell_sums(hidden, group_matrix(), stats_ref)


def project(hidden, mean, scale, vectors_ref, query_ref, keyvalue_ref):
    normed = ((hidden - mean) * scale * vectors_ref[2:3] + vectors_ref[3:4]).astype(BF16)
    query = dot(normed, query_ref[...]).astype(BF16)
    return query, dot(normed, keyvalue_ref[...]).astype(BF16)


def project_kernel(
    stats_ref, hidden_ref, vectors_ref, query_ref, keyvalue_ref, asked_ref, fresh_ref
):
    mean, scale = mean_and_scale(stats_ref, group_matrix())
    hidden = hidden_ref[...].reshape(QUAD_ROWS, CHANNELS)
    asked, fresh = project(hidden, mean, scale, vectors_ref, query_ref, keyvalue_ref)
    asked_ref[...] = asked
    fresh_ref[...] = fresh


def attend(query, fresh, patch, y, kv_ref):
    count = query.shape[0]
    lane = lax.broadcasted_iota(jnp.int32, (count, LANES), 1)
    low = lane < HEAD_DIM

    block = lax.broadcasted_iota(jnp.int32, (count, POSITIONS), 1) >> 5
    replaced = block == 4 * y + patch
    if count == ROWS:
        theirs = None
    else:
        theirs = (lax.broadcasted_iota(jnp.int32, (count, count), 1) >> 5) == patch
    tiles = [jnp.zeros((count, LANES), F32) for _ in range(3)]
    for h in range(HEADS):
        at = LANES * (h // 2)
        own = low if h % 2 == 0 else ~low
        asked = jnp.where(own, query[:, at : at + LANES].astype(F32), 0.0).astype(BF16)
        old = dot(asked, kv_ref[:, at : at + LANES], NT) * HEAD_DIM ** (-0.5)
        old = jnp.where(replaced, -jnp.inf, old)
        new = dot(asked, fresh[:, at : at + LANES], NT) * HEAD_DIM ** (-0.5)
        if theirs is not None:
            new = jnp.where(theirs, new, -jnp.inf)
        peak = jnp.maximum(
            jnp.max(old, axis=1, keepdims=True), jnp.max(new, axis=1, keepdims=True)
        )
        old = jnp.exp(old - peak)
        new = jnp.exp(new - peak)
        total = jnp.sum(old, axis=1, keepdims=True) + jnp.sum(new, axis=1, keepdims=True)
        at = LANES * ((HEADS + h) // 2)
        summed = dot(old.astype(BF16), kv_ref[:, at : at + LANES])
        summed += dot(new.astype(BF16), fresh[:, at : at + LANES])
        summed = pltpu.roll(summed / total, HEAD_DIM, 1)
        tiles[h // 2] = jnp.where(own, summed, tiles[h // 2])
    return jnp.concatenate(tiles, axis=1)[:, :WIDTH].astype(BF16)


def attend_quad_kernel(
    place_ref, asked_ref, fresh_ref, hidden_ref, out_ref, kv_ref, state_ref, told_ref
):
    patch = lax.broadcasted_iota(jnp.int32, (QUAD_ROWS, 1), 0) >> 5
    attended = attend(asked_ref[...], fresh_ref[...], patch, place_ref[0], kv_ref)
    result = hidden_ref[...].reshape(QUAD_ROWS, CHANNELS) + dot(attended, out_ref[...])
    state_ref[...] = result.reshape(state_ref.shape)
    tell_sums(result, group_matrix(), told_ref)


def project_own_kernel(
    place_ref,
    conv_ref,
    state_ref,
    vectors_ref,
    query_ref,
    keyvalue_ref,
    hidden_ref,
    asked_ref,
    fresh_ref,
):
    hidden = state_ref[place_ref[1]] + (assembled(conv_ref, ROWS) + vectors_ref[5:6])
    sums = jnp.zeros((8, LANES), F32)
    for t in range(4):
        sums += conv_ref[t, 48:56]
    mean, scale = spread_sums(sums, group_matrix())
    asked, fresh = project(hidden, mean, scale, vectors_ref, query_ref, keyvalue_ref)
    hidden_ref[...] = hidden
    asked_ref[...] = asked
    fresh_ref[...] = fresh


def attend_own_kernel(
    place_ref, asked_ref, fresh_ref, hidden_ref, state_ref, out_ref, kv_ref, result_ref
):
    a = place_ref[1]
    attended = attend(asked_ref[...], fresh_ref[...], a, place_ref[0], kv_ref)
    result_ref[0] = state_ref[a]
    result_ref[1] = hidden_ref[...] + dot(attended, out_ref[...])


VMEM = pl.BlockSpec(memory_space=pltpu.VMEM)
SMEM = pl.BlockSpec(memory_space=pltpu.SMEM)


def call(kernel, name, out_shapes, args, scalars=0, scratch=(), flops=0):
    return pl.pallas_call(
        kernel,
        name=name,
        out_shape=[jax.ShapeDtypeStruct(s, t) for s, t in out_shapes],
        in_specs=[SMEM] * scalars + [VMEM] * (len(args) - scalars),
        out_specs=[VMEM] * len(out_shapes),
        scratch_shapes=list(scratch),
        cost_estimate=pl.CostEstimate(flops=flops, bytes_accessed=1 << 20, transcendentals=0),
        compiler_params=pltpu.CompilerParams(vmem_limit_bytes=20 << 20),
    )(*args)


def to_all(value, axes):
    return lax.all_to_all(value, axes, 0, 0, tiled=True)


def per_device(
    field,
    stale_conv_in,
    stale_keys,
    stale_values,
    norm1_gain,
    norm1_bias,
    conv_weight,
    conv_bias,
    time_embed,
    norm2_gain,
    norm2_bias,
    w_query,
    w_keyvalue,
    w_out,
):
    quad = (4, ROWS, CHANNELS)
    line = (COLS, CHANNELS)
    stats8 = ((8, 4, LANES), F32)
    y = 2 * lax.axis_index("yh") + lax.axis_index("yl")
    a = 2 * lax.axis_index("zh") + lax.axis_index("core")
    place = jnp.stack([y, a]).astype(jnp.int32)

    slices = conv_weight.transpose(0, 1, 3, 2).reshape(9 * MEMBERS, CHANNELS)
    weights = lax.all_gather(slices, Y, axis=0, tiled=False)

    own = field.reshape(ROWS, CHANNELS)
    (packed,) = call(
        pack_kernel,
        "pack",
        [((4, 4 * ROWS, CHANNELS), BF16)],
        (own, stale_conv_in.reshape(ROWS, CHANNELS), stale_keys, stale_values),
    )
    vectors = jnp.stack(
        [
            norm1_gain,
            norm1_bias,
            norm2_gain,
            norm2_bias,
            conv_bias + time_embed[0],
            conv_bias + time_embed[1],
            jnp.zeros_like(conv_bias),
            jnp.zeros_like(conv_bias),
        ]
    )
    w_query = jnp.pad(w_query, ((0, 0), (0, 3 * LANES - WIDTH)))
    packed, vectors, w_query, place = lax.optimization_barrier(
        (to_all(packed, QUAD), vectors, w_query, place)
    )
    state, kv, prior, first, last, stats = call(
        unpack_kernel,
        "unpack",
        [(quad, F32), (quad, BF16), (quad, BF16), (line, BF16), (line, BF16), stats8],
        (place, packed, own),
        scalars=1,
    )
    kv = kv.reshape(QUAD_ROWS, CHANNELS)
    old = lax.all_gather(kv, Y, axis=0, tiled=True)
    up = [(i, i + 1) for i in range(7)]
    down = [(i + 1, i) for i in range(7)]
    above = lax.ppermute(last, Y, up)
    below = lax.ppermute(first, Y, down)
    buffers = [pltpu.VMEM((4, 64, CHANNELS), BF16), pltpu.VMEM((256, 256), F32)]

    conv, prior, first, last = call(
        conv_quad_kernel,
        "conv0",
        [((4, LANES + 64, LANES), F32), (quad, BF16), (line, BF16), (line, BF16)],
        (to_all(stats, Y), above, below, state, prior, weights, vectors),
        scratch=buffers,
        flops=1 << 30,
    )
    hidden, stats = call(
        hidden_kernel,
        "hidden0",
        [(quad, F32), stats8],
        (to_all(conv, QUAD), state, vectors),
        flops=1 << 28,
    )
    last, first, hidden, stats = lax.optimization_barrier((last, first, hidden, stats))
    stats, above, below = lax.optimization_barrier(
        (to_all(stats, Y), lax.ppermute(last, Y, up), lax.ppermute(first, Y, down))
    )
    asked, fresh = call(
        project_kernel,
        "project0",
        [((QUAD_ROWS, 3 * LANES), BF16), ((QUAD_ROWS, CHANNELS), BF16)],
        (stats, hidden, vectors, w_query, w_keyvalue),
        flops=1 << 28,
    )
    kv = lax.all_gather(fresh, Y, axis=0, tiled=True)
    state, stats = call(
        attend_quad_kernel,
        "attend0",
        [(quad, F32), stats8],
        (place, asked, fresh, hidden, w_out, old),
        scalars=1,
        flops=1 << 30,
    )
    conv, stats = call(
        conv_own_kernel,
        "conv1",
        [((4, ROWS + ROWS // 2, LANES), F32), stats8],
        (place, to_all(stats, Y), above, below, state, prior, weights, vectors),
        scalars=1,
        scratch=buffers,
        flops=1 << 30,
    )
    (conv,) = call(
        insert_kernel,
        "insert1",
        [((4, 56, LANES), F32)],
        (conv, to_all(stats, Y)),
        flops=1 << 24,
    )
    conv, kv = lax.optimization_barrier((to_all(conv, QUAD), kv))
    hidden, asked, fresh = call(
        project_own_kernel,
        "project1",
        [((ROWS, CHANNELS), F32), ((ROWS, 3 * LANES), BF16), ((ROWS, CHANNELS), BF16)],
        (place, conv, state, vectors, w_query, w_keyvalue),
        scalars=1,
        flops=1 << 30,
    )
    (out,) = call(
        attend_own_kernel,
        "attend1",
        [((2, ROWS, CHANNELS), F32)],
        (place, asked, fresh, hidden, state, w_out, kv),
        scalars=1,
        flops=1 << 30,
    )
    return out.reshape(2, 2, COLS, CHANNELS)


def solution(mesh):
    torus = Mesh(
        mesh.devices.reshape(mesh.shape["req"], 4, 2, 2, 2), REQ_PATCH
    )
    placed = (
        P(REQ_PATCH, None, None),
        P(REQ_PATCH, None, None),
        P(REQ_PATCH, None),
        P(REQ_PATCH, None),
        P(),
        P(),
        P(None, None, None, PATCH),
        P(),
        P("req", None),
        P(),
        P(),
        P(),
        P(),
        P(),
    )
    return jax.shard_map(
        per_device,
        mesh=torus,
        in_specs=placed,
        out_specs=P(None, REQ_PATCH, None, None),
        check_vma=False,
    )
```

```python
import functools

import jax
import jax.numpy as jnp
from jax import lax
from jax.experimental import pallas as pl
from jax.experimental.pallas import tpu as pltpu
from jax.sharding import Mesh
from jax.sharding import PartitionSpec as P

GROUPS = 32
HEADS = 5
HEAD_DIM = 64
WIDTH = HEADS * HEAD_DIM
CHANNELS = 640
MEMBERS = CHANNELS // GROUPS
COLS = 16
ROWS = 32
LANES = 128
QUAD_ROWS = 4 * ROWS
POSITIONS = 1024
EPS = 1e-05

Y = ("yh", "yl")
QUAD = ("zh", "core")
REQ_PATCH = ("req", "yh", "yl", "zh", "core")
PATCH = ("yh", "yl", "zh", "core")

F32 = jnp.float32
BF16 = jnp.bfloat16

NN = (((1,), (0,)), ((), ()))
NT = (((1,), (1,)), ((), ()))


def dot(a, b, dims=NN):
    return lax.dot_general(a, b, dims, preferred_element_type=F32)


def thirds(x):
    high = x.astype(BF16)
    rest = x - high.astype(F32)
    middle = rest.astype(BF16)
    low = (rest - middle.astype(F32)).astype(BF16)
    return high, middle, low


def picked(x, zero_one, dims=NN):
    rows = x.shape[0]
    stacked = jnp.concatenate([t.astype(F32) for t in thirds(x)], axis=0).astype(BF16)
    out = dot(stacked, zero_one, dims)
    return out[:rows] + out[rows : 2 * rows] + out[2 * rows :]


def group_matrix():
    channel = lax.broadcasted_iota(jnp.int32, (CHANNELS, LANES), 0)
    first = lax.broadcasted_iota(jnp.int32, (CHANNELS, LANES), 1) * MEMBERS
    return jnp.where((channel >= first) & (channel < first + MEMBERS), 1.0, 0.0).astype(BF16)


def eight(rows, lanes):
    have = sum(r.shape[0] for r in rows)
    return jnp.concatenate([*rows, jnp.zeros((8 - have, lanes), F32)], axis=0)


def tell_sums(x, groups, stats_ref):
    sums = eight(
        [jnp.sum(x, axis=0, keepdims=True), jnp.sum(x * x, axis=0, keepdims=True)], CHANNELS
    )
    told = picked(sums, groups)[0:4]
    stats_ref[...] = jnp.broadcast_to(told[None], stats_ref.shape)


def mean_and_scale(stats_ref, groups):
    return spread_sums(jnp.sum(stats_ref[...], axis=0), groups)


def spread_sums(sums, groups):
    number = POSITIONS * MEMBERS
    mean = sums[0:1] * (1.0 / number)
    variance = sums[1:2] * (1.0 / number) - mean * mean
    spread = picked(eight([mean, lax.rsqrt(variance + EPS)], LANES), groups, NT)
    return spread[0:1], spread[1:2]


def pack_kernel(field_ref, stale_ref, keys_ref, values_ref, packed_ref):
    high, middle, _ = thirds(field_ref[...])
    both = jnp.concatenate(
        [keys_ref[...].astype(F32), values_ref[...].astype(F32)], axis=1
    ).astype(BF16)
    for to in range(4):
        packed_ref[to, 0:ROWS] = high
        packed_ref[to, ROWS : 2 * ROWS] = middle
        packed_ref[to, 2 * ROWS : 3 * ROWS] = stale_ref[...]
        packed_ref[to, 3 * ROWS :] = both


def unpack_kernel(
    place_ref,
    packed_ref,
    field_ref,
    state_ref,
    kv_ref,
    prior_ref,
    first_ref,
    last_ref,
    stats_ref,
):
    for t in range(4):
        state_ref[t] = packed_ref[t, 0:ROWS].astype(F32) + packed_ref[t, ROWS : 2 * ROWS].astype(F32)
        prior_ref[t] = packed_ref[t, 2 * ROWS : 3 * ROWS]
        kv_ref[t] = packed_ref[t, 3 * ROWS :]
    state_ref[place_ref[1]] = field_ref[...]
    first_ref[...] = prior_ref[0, :COLS]
    last_ref[...] = prior_ref[3, COLS:]
    tell_sums(state_ref[...].reshape(QUAD_ROWS, CHANNELS), group_matrix(), stats_ref)


def activate(sums, edges, state_ref, prior_ref, vectors_ref, keep, rows):
    mean, scale = spread_sums(sums, group_matrix())
    above, below = edges
    for t in range(4):
        value = (state_ref[t] - mean) * scale * vectors_ref[0:1] + vectors_ref[1:2]
        act = (value * (1.0 / (1.0 + jnp.exp(-value)))).astype(BF16)
        rows[t, COLS : 3 * COLS] = act
        keep(t, act)
        rows[t, 0:COLS] = above if t == 0 else prior_ref[t - 1, COLS:]
        rows[t, 3 * COLS :] = below if t == 3 else prior_ref[t + 1, :COLS]


def convolve(rows, weight_ref, wide):
    window = rows[...].reshape(4 * 64, CHANNELS)
    wide[...] = jnp.zeros(wide.shape, F32)
    col = lax.broadcasted_iota(jnp.int32, (LANES, LANES), 0) & (COLS - 1)
    lane = lax.broadcasted_iota(jnp.int32, (LANES, LANES), 1)
    tiles = [jnp.zeros((LANES, LANES), F32), jnp.zeros((LANES, LANES), F32)]
    for part in range(8):
        wide[:, 0 : 9 * MEMBERS] = dot(window, weight_ref[part], NT)
        whole = wide[...].reshape(4, 64, 256)
        lines = [
            whole[:, COLS * r : COLS * r + 2 * COLS].reshape(LANES, 256) for r in range(3)
        ]
        total = (
            lines[0][:, :LANES]
            + pltpu.roll(lines[1][:, :LANES], LANES - 3 * MEMBERS, 1)
            + pltpu.roll(lines[2], 256 - 6 * MEMBERS, 1)[:, :LANES]
        )
        left = jnp.where(col > 0, pltpu.roll(total, 1, 0), 0.0)
        centre = pltpu.roll(total, LANES - MEMBERS, 1)
        right = pltpu.roll(total, LANES - 2 * MEMBERS, 1)
        right = jnp.where(col < COLS - 1, pltpu.roll(right, LANES - 1, 0), 0.0)
        made = left + centre + right
        tile, at = divmod(part, 6)
        at *= MEMBERS
        if at:
            made = pltpu.roll(made, at, 1)
        kept = (lane >= at) & (lane < at + MEMBERS)
        tiles[tile] = jnp.where(kept, made, tiles[tile])
    return tiles


def folded(tile):
    half = tile.shape[0] // 2
    lane = lax.broadcasted_iota(jnp.int32, (half, LANES), 1)
    return jnp.where(lane < 64, tile[:half], pltpu.roll(tile[half:], 64, 1))


def conv_quad_kernel(
    stats_ref,
    above_ref,
    below_ref,
    state_ref,
    prior_ref,
    weight_ref,
    vectors_ref,
    out_ref,
    act_ref,
    first_ref,
    last_ref,
    rows,
    wide,
):
    def keep(t, act):
        act_ref[t] = act
        if t == 0:
            first_ref[...] = act[:COLS]
        if t == 3:
            last_ref[...] = act[COLS:]

    edges = (above_ref[...], below_ref[...])
    sums = jnp.sum(stats_ref[...], axis=0)
    activate(sums, edges, state_ref, prior_ref, vectors_ref, keep, rows)
    tiles = convolve(rows, weight_ref, wide)
    rest = folded(tiles[1])
    for to in range(4):
        out_ref[to, 0:LANES] = tiles[0]
        out_ref[to, LANES:] = rest


def shard_lanes(shape, dim):
    lane = lax.broadcasted_iota(jnp.int32, shape, dim)
    inner = lane & (LANES - 1)
    part = (inner * 3277) >> 16
    within = inner - MEMBERS * part
    second = lane >= LANES
    used = part < jnp.where(second, 2, 6)
    return part + jnp.where(second, 6, 0), within, used


def conv_own_kernel(
    place_ref,
    stats_ref,
    above_ref,
    below_ref,
    state_ref,
    prior_ref,
    weight_ref,
    vectors_ref,
    out_ref,
    told_ref,
    rows,
    wide,
):
    a = place_ref[1]
    activate(
        jnp.sum(stats_ref[...], axis=0),
        (above_ref[...], below_ref[...]),
        state_ref,
        prior_ref,
        vectors_ref,
        lambda t, act: None,
        rows,
    )
    tiles = convolve(rows, weight_ref, wide)
    for t in range(4):
        mine = slice(t * ROWS, (t + 1) * ROWS)
        out_ref[t, 0:ROWS] = tiles[0][mine]
        out_ref[t, ROWS:] = folded(tiles[1][mine])
    part, within, used = shard_lanes((CHANNELS, 256), 1)
    channel = lax.broadcasted_iota(jnp.int32, (CHANNELS, 256), 0)
    select = used & (channel == 4 * MEMBERS * part + MEMBERS * a + within)
    select = jnp.where(select, 1.0, 0.0).astype(BF16)
    part, _, used = shard_lanes((LANES, 256), 1)
    group = lax.broadcasted_iota(jnp.int32, (LANES, 256), 0)
    holds = jnp.where(used & (group == 4 * part + a), 1.0, 0.0).astype(BF16)
    state = state_ref[...].reshape(QUAD_ROWS, CHANNELS)
    hidden = picked(state, select) + (
        jnp.concatenate(tiles, axis=1) + picked(eight([vectors_ref[5:6]], CHANNELS), select)[0:1]
    )
    sums = eight(
        [jnp.sum(hidden, axis=0, keepdims=True), jnp.sum(hidden * hidden, axis=0, keepdims=True)],
        256,
    )
    told = picked(sums, holds, NT)[0:4]
    told_ref[...] = jnp.broadcast_to(told[None], told_ref.shape)


def insert_kernel(conv_ref, stats_ref, out_ref):
    sums = jnp.sum(stats_ref[...], axis=0)
    for to in range(4):
        out_ref[to, 0:48] = conv_ref[to]
        out_ref[to, 48:] = eight([sums], LANES)


def assembled(conv_ref, count):
    lane = lax.broadcasted_iota(jnp.int32, (count, LANES), 1)
    tiles = [jnp.zeros((count, LANES), F32) for _ in range(5)]
    for t in range(4):
        rest = conv_ref[t, count : count + count // 2]
        sources = (
            conv_ref[t, 0:count],
            jnp.concatenate([rest, pltpu.roll(rest, 64, 1)], axis=0),
        )
        for part in range(8):
            source, at = divmod(part, 6)
            at *= MEMBERS
            tile, to = divmod(4 * MEMBERS * part + MEMBERS * t, LANES)
            turn = (to - at) % LANES
            block = sources[source]
            if turn:
                block = pltpu.roll(block, turn, 1)
            kept = (lane >= to) & (lane < to + MEMBERS)
            tiles[tile] = jnp.where(kept, block, tiles[tile])
            if to + MEMBERS > LANES:
                kept = lane < to + MEMBERS - LANES
                tiles[tile + 1] = jnp.where(kept, block, tiles[tile + 1])
    return jnp.concatenate(tiles, axis=1)


def hidden_kernel(conv_ref, state_ref, vectors_ref, hidden_ref, stats_ref):
    state = state_ref[...].reshape(QUAD_ROWS, CHANNELS)
    hidden = state + (assembled(conv_ref, QUAD_ROWS) + vectors_ref[4:5])
    hidden_ref[...] = hidden.reshape(hidden_ref.shape)
    tell_sums(hidden, group_matrix(), stats_ref)


def project(hidden, mean, scale, vectors_ref, query_ref, keyvalue_ref):
    normed = ((hidden - mean) * scale * vectors_ref[2:3] + vectors_ref[3:4]).astype(BF16)
    query = dot(normed, query_ref[...]).astype(BF16)
    return query, dot(normed, keyvalue_ref[...]).astype(BF16)


def project_kernel(
    stats_ref, hidden_ref, vectors_ref, query_ref, keyvalue_ref, asked_ref, fresh_ref
):
    mean, scale = mean_and_scale(stats_ref, group_matrix())
    hidden = hidden_ref[...].reshape(QUAD_ROWS, CHANNELS)
    asked, fresh = project(hidden, mean, scale, vectors_ref, query_ref, keyvalue_ref)
    asked_ref[...] = asked
    fresh_ref[...] = fresh


def attend(query, fresh, patch, y, kv_ref):
    count = query.shape[0]
    lane = lax.broadcasted_iota(jnp.int32, (count, LANES), 1)
    low = lane < HEAD_DIM

    block = lax.broadcasted_iota(jnp.int32, (count, POSITIONS), 1) >> 5
    replaced = block == 4 * y + patch
    if count == ROWS:
        theirs = None
    else:
        theirs = (lax.broadcasted_iota(jnp.int32, (count, count), 1) >> 5) == patch
    tiles = [jnp.zeros((count, LANES), F32) for _ in range(3)]
    for h in range(HEADS):
        at = LANES * (h // 2)
        own = low if h % 2 == 0 else ~low
        asked = jnp.where(own, query[:, at : at + LANES].astype(F32), 0.0).astype(BF16)
        old = dot(asked, kv_ref[:, at : at + LANES], NT) * HEAD_DIM ** (-0.5)
        old = jnp.where(replaced, -jnp.inf, old)
        new = dot(asked, fresh[:, at : at + LANES], NT) * HEAD_DIM ** (-0.5)
        if theirs is not None:
            new = jnp.where(theirs, new, -jnp.inf)
        peak = jnp.maximum(
            jnp.max(old, axis=1, keepdims=True), jnp.max(new, axis=1, keepdims=True)
        )
        old = jnp.exp(old - peak)
        new = jnp.exp(new - peak)
        total = jnp.sum(old, axis=1, keepdims=True) + jnp.sum(new, axis=1, keepdims=True)
        at = LANES * ((HEADS + h) // 2)
        summed = dot(old.astype(BF16), kv_ref[:, at : at + LANES])
        summed += dot(new.astype(BF16), fresh[:, at : at + LANES])
        summed = pltpu.roll(summed / total, HEAD_DIM, 1)
        tiles[h // 2] = jnp.where(own, summed, tiles[h // 2])
    return jnp.concatenate(tiles, axis=1)[:, :WIDTH].astype(BF16)


def attend_quad_kernel(
    place_ref, asked_ref, fresh_ref, hidden_ref, out_ref, kv_ref, state_ref, told_ref
):
    patch = lax.broadcasted_iota(jnp.int32, (QUAD_ROWS, 1), 0) >> 5
    attended = attend(asked_ref[...], fresh_ref[...], patch, place_ref[0], kv_ref)
    result = hidden_ref[...].reshape(QUAD_ROWS, CHANNELS) + dot(attended, out_ref[...])
    state_ref[...] = result.reshape(state_ref.shape)
    tell_sums(result, group_matrix(), told_ref)


def project_own_kernel(
    place_ref,
    conv_ref,
    state_ref,
    vectors_ref,
    query_ref,
    keyvalue_ref,
    hidden_ref,
    asked_ref,
    fresh_ref,
):
    hidden = state_ref[place_ref[1]] + (assembled(conv_ref, ROWS) + vectors_ref[5:6])
    sums = jnp.zeros((8, LANES), F32)
    for t in range(4):
        sums += conv_ref[t, 48:56]
    mean, scale = spread_sums(sums, group_matrix())
    asked, fresh = project(hidden, mean, scale, vectors_ref, query_ref, keyvalue_ref)
    hidden_ref[...] = hidden
    asked_ref[...] = asked
    fresh_ref[...] = fresh


def attend_own_kernel(
    place_ref, asked_ref, fresh_ref, hidden_ref, state_ref, out_ref, kv_ref, result_ref
):
    a = place_ref[1]
    lane = lax.broadcasted_iota(jnp.int32, (ROWS, 3 * LANES), 1)
    query = asked_ref[...].astype(F32)
    heads = jnp.concatenate(
        [jnp.where(lane >> 6 == h, query, 0.0) for h in range(HEADS)], axis=0
    ).astype(BF16)
    low, high = slice(0, 3 * LANES), slice(2 * LANES, 5 * LANES)
    old = dot(heads, kv_ref[:, low], NT) * HEAD_DIM ** (-0.5)
    block = lax.broadcasted_iota(jnp.int32, old.shape, 1) >> 5
    old = jnp.where(block == 4 * place_ref[0] + a, -jnp.inf, old)
    new = dot(heads, fresh_ref[:, low], NT) * HEAD_DIM ** (-0.5)
    peak = jnp.maximum(jnp.max(old, axis=1, keepdims=True), jnp.max(new, axis=1, keepdims=True))
    old = jnp.exp(old - peak)
    new = jnp.exp(new - peak)
    total = jnp.sum(old, axis=1, keepdims=True) + jnp.sum(new, axis=1, keepdims=True)
    summed = dot(old.astype(BF16), kv_ref[:, high]) + dot(new.astype(BF16), fresh_ref[:, high])
    summed = summed / total
    attended = jnp.zeros((ROWS, 3 * LANES), F32)
    for h in range(HEADS):
        mine = summed[h * ROWS : (h + 1) * ROWS]
        attended = jnp.where(lane >> 6 == h + 1, mine, attended)
    attended = pltpu.roll(attended, 3 * LANES - HEAD_DIM, 1)[:, :WIDTH].astype(BF16)
    result_ref[0] = state_ref[a]
    result_ref[1] = hidden_ref[...] + dot(attended, out_ref[...])


VMEM = pl.BlockSpec(memory_space=pltpu.VMEM)
SMEM = pl.BlockSpec(memory_space=pltpu.SMEM)


def call(kernel, name, out_shapes, args, scalars=0, scratch=(), flops=0):
    return pl.pallas_call(
        kernel,
        name=name,
        out_shape=[jax.ShapeDtypeStruct(s, t) for s, t in out_shapes],
        in_specs=[SMEM] * scalars + [VMEM] * (len(args) - scalars),
        out_specs=[VMEM] * len(out_shapes),
        scratch_shapes=list(scratch),
        cost_estimate=pl.CostEstimate(flops=flops, bytes_accessed=1 << 20, transcendentals=0),
        compiler_params=pltpu.CompilerParams(vmem_limit_bytes=20 << 20),
    )(*args)


def to_all(value, axes):
    return lax.all_to_all(value, axes, 0, 0, tiled=True)


def per_device(
    field,
    stale_conv_in,
    stale_keys,
    stale_values,
    norm1_gain,
    norm1_bias,
    conv_weight,
    conv_bias,
    time_embed,
    norm2_gain,
    norm2_bias,
    w_query,
    w_keyvalue,
    w_out,
):
    quad = (4, ROWS, CHANNELS)
    line = (COLS, CHANNELS)
    stats8 = ((8, 4, LANES), F32)
    y = 2 * lax.axis_index("yh") + lax.axis_index("yl")
    a = 2 * lax.axis_index("zh") + lax.axis_index("core")
    place = jnp.stack([y, a]).astype(jnp.int32)

    slices = conv_weight.transpose(0, 1, 3, 2).reshape(9 * MEMBERS, CHANNELS)
    weights = lax.all_gather(slices, Y, axis=0, tiled=False)

    own = field.reshape(ROWS, CHANNELS)
    (packed,) = call(
        pack_kernel,
        "pack",
        [((4, 4 * ROWS, CHANNELS), BF16)],
        (own, stale_conv_in.reshape(ROWS, CHANNELS), stale_keys, stale_values),
    )
    vectors = jnp.stack(
        [
            norm1_gain,
            norm1_bias,
            norm2_gain,
            norm2_bias,
            conv_bias + time_embed[0],
            conv_bias + time_embed[1],
            jnp.zeros_like(conv_bias),
            jnp.zeros_like(conv_bias),
        ]
    )
    w_query = jnp.pad(w_query, ((0, 0), (0, 3 * LANES - WIDTH)))
    packed, vectors, w_query, place = lax.optimization_barrier(
        (to_all(packed, QUAD), vectors, w_query, place)
    )
    state, kv, prior, first, last, stats = call(
        unpack_kernel,
        "unpack",
        [(quad, F32), (quad, BF16), (quad, BF16), (line, BF16), (line, BF16), stats8],
        (place, packed, own),
        scalars=1,
    )
    kv = kv.reshape(QUAD_ROWS, CHANNELS)
    old = lax.all_gather(kv, Y, axis=0, tiled=True)
    up = [(i, i + 1) for i in range(7)]
    down = [(i + 1, i) for i in range(7)]
    above = lax.ppermute(last, Y, up)
    below = lax.ppermute(first, Y, down)
    buffers = [pltpu.VMEM((4, 64, CHANNELS), BF16), pltpu.VMEM((256, 256), F32)]

    conv, prior, first, last = call(
        conv_quad_kernel,
        "conv0",
        [((4, LANES + 64, LANES), F32), (quad, BF16), (line, BF16), (line, BF16)],
        (to_all(stats, Y), above, below, state, prior, weights, vectors),
        scratch=buffers,
        flops=1 << 30,
    )
    hidden, stats = call(
        hidden_kernel,
        "hidden0",
        [(quad, F32), stats8],
        (to_all(conv, QUAD), state, vectors),
        flops=1 << 28,
    )
    last, first, hidden, stats = lax.optimization_barrier((last, first, hidden, stats))
    stats, above, below = lax.optimization_barrier(
        (to_all(stats, Y), lax.ppermute(last, Y, up), lax.ppermute(first, Y, down))
    )
    asked, fresh = call(
        project_kernel,
        "project0",
        [((QUAD_ROWS, 3 * LANES), BF16), ((QUAD_ROWS, CHANNELS), BF16)],
        (stats, hidden, vectors, w_query, w_keyvalue),
        flops=1 << 28,
    )
    kv = lax.all_gather(fresh, Y, axis=0, tiled=True)
    state, stats = call(
        attend_quad_kernel,
        "attend0",
        [(quad, F32), stats8],
        (place, asked, fresh, hidden, w_out, old),
        scalars=1,
        flops=1 << 30,
    )
    conv, stats = call(
        conv_own_kernel,
        "conv1",
        [((4, ROWS + ROWS // 2, LANES), F32), stats8],
        (place, to_all(stats, Y), above, below, state, prior, weights, vectors),
        scalars=1,
        scratch=buffers,
        flops=1 << 30,
    )
    (conv,) = call(
        insert_kernel,
        "insert1",
        [((4, 56, LANES), F32)],
        (conv, to_all(stats, Y)),
        flops=1 << 24,
    )
    conv, kv = lax.optimization_barrier((to_all(conv, QUAD), kv))
    hidden, asked, fresh = call(
        project_own_kernel,
        "project1",
        [((ROWS, CHANNELS), F32), ((ROWS, 3 * LANES), BF16), ((ROWS, CHANNELS), BF16)],
        (place, conv, state, vectors, w_query, w_keyvalue),
        scalars=1,
        flops=1 << 30,
    )
    (out,) = call(
        attend_own_kernel,
        "attend1",
        [((2, ROWS, CHANNELS), F32)],
        (place, asked, fresh, hidden, state, w_out, kv),
        scalars=1,
        flops=1 << 30,
    )
    return out.reshape(2, 2, COLS, CHANNELS)


def solution(mesh):
    torus = Mesh(
        mesh.devices.reshape(mesh.shape["req"], 4, 2, 2, 2), REQ_PATCH
    )
    placed = (
        P(REQ_PATCH, None, None),
        P(REQ_PATCH, None, None),
        P(REQ_PATCH, None),
        P(REQ_PATCH, None),
        P(),
        P(),
        P(None, None, None, PATCH),
        P(),
        P("req", None),
        P(),
        P(),
        P(),
        P(),
        P(),
    )
    return jax.shard_map(
        per_device,
        mesh=torus,
        in_specs=placed,
        out_specs=P(None, REQ_PATCH, None, None),
        check_vma=False,
    )
```
